8 devices in a mesh: dp: 1 (over z), kv: 2 (over y), tp: 4 (over x, core).
Axes of the slice: x: 2, y: 2, z: 1, core: 2. Of those that a mesh axis runs over, the one named last changes fastest.
Arguments:
- x: bfloat16 [64, 2048], P('dp')
- ks_cache: bfloat16 [64, 8, 1024, 64], P('dp', 'tp', 'kv')
- vs_cache: bfloat16 [64, 8, 1024, 64], P('dp', 'tp', 'kv')
- seq_len: int32 [64], P('dp')
- kx_cache: bfloat16 [64, 8, 6404, 64], P('dp', 'tp', 'kv')
- vx_cache: bfloat16 [64, 8, 6404, 64], P('dp', 'tp', 'kv')
- tile_vis: int32 [64, 4], P('dp')
- attn_norm: bfloat16 [2048], replicated
- wq_self: bfloat16 [2048, 2048], P(None, 'tp')
- wk_self: bfloat16 [2048, 512], P(None, 'tp')
- wv_self: bfloat16 [2048, 512], P(None, 'tp')
- wo_self: bfloat16 [2048, 2048], P('tp')
- mlp_norm: bfloat16 [2048], replicated
- wg_self: bfloat16 [2048, 8192], P(None, 'tp')
- wu_self: bfloat16 [2048, 8192], P(None, 'tp')
- wd_self: bfloat16 [8192, 2048], P('tp')
- xattn_norm: bfloat16 [2048], replicated
- wq_cross: bfloat16 [2048, 2048], P(None, 'tp')
- q_norm: bfloat16 [64], replicated
- wo_cross: bfloat16 [2048, 2048], P('tp')
- cross_gates: float32 [2], replicated
- xmlp_norm: bfloat16 [2048], replicated
- wg_cross: bfloat16 [2048, 8192], P(None, 'tp')
- wu_cross: bfloat16 [2048, 8192], P(None, 'tp')
- wd_cross: bfloat16 [8192, 2048], P('tp')
Outputs:
- output 1: bfloat16 [64, 2048], P('dp')
- output 2: bfloat16 [64, 8, 64], P('dp', 'tp')
- output 3: bfloat16 [64, 8, 64], P('dp', 'tp')
All inputs are finite; a program needn't handle non-finite values.
Results may differ from the reference program's by a relative error of at most 0.0128287.
Values sent between devices are 32-bit elements.
A program may use at most 1 GiB of HBM per device.

```python
import math
import jax
import jax.numpy as jnp
from jax import lax

D = 2048
HEADS = 32
KV_HEADS = 8
HEAD = 64
FF = 8192
TILES = 4
TILE_TOK = 1601
BATCH = 64
CACHE_LEN = 1024
NORM_EPS = 1e-5
ROPE_THETA = 500000.0
MASK_VALUE = -1e30


def rope_freqs():
    freq_list = []
    for index in range(HEAD // 2):
        base_freq = 1.0 / (ROPE_THETA ** (2.0 * index / HEAD))
        wave_len = 2.0 * math.pi / base_freq
        if wave_len < 2048.0:
            freq_list.append(base_freq)
        elif wave_len > 8192.0:
            freq_list.append(base_freq / 8.0)
        else:
            smooth = (8192.0 / wave_len - 1.0) / 3.0
            freq_list.append((1.0 - smooth) * base_freq / 8.0 + smooth * base_freq)
    return jnp.array(freq_list, dtype=jnp.float32)


def rms_norm(hidden, gain):
    return hidden * lax.rsqrt(jnp.mean(hidden * hidden, axis=-1, keepdims=True) + NORM_EPS) * gain.astype(jnp.float32)


def apply_rope(tensor, cos_t, sin_t):
    half = tensor.shape[-1] // 2
    first = tensor[..., :half]
    second = tensor[..., half:]
    return jnp.concatenate([first * cos_t - second * sin_t, second * cos_t + first * sin_t], axis=-1)


def swiglu(hidden, gain, w_gate, w_up, w_down):
    h_norm = rms_norm(hidden, gain).astype(jnp.bfloat16)
    gate = jnp.dot(h_norm, w_gate, preferred_element_type=jnp.float32)
    upper = jnp.dot(h_norm, w_up, preferred_element_type=jnp.float32)
    hidden_act = (jax.nn.silu(gate) * upper).astype(jnp.bfloat16)
    return jnp.dot(hidden_act, w_down, preferred_element_type=jnp.float32)


def attend_row(query, keys, values, visible):
    scores = jnp.einsum('kgd,ktd->kgt', query.astype(jnp.float32), keys.astype(jnp.float32)) * HEAD ** -0.5
    scores = jnp.where(visible[None, None, :], scores, MASK_VALUE)
    top = jnp.max(scores, axis=-1, keepdims=True)
    weights = jnp.where(visible[None, None, :], jnp.exp(scores - top), 0.0)
    total = jnp.sum(weights, axis=-1, keepdims=True)
    out = jnp.einsum('kgt,ktd->kgd', weights, values.astype(jnp.float32))
    return (out / jnp.where(total > 0, total, 1.0)).reshape(-1).astype(jnp.bfloat16)


def setup_inputs(seed: int = 0, part: int = 0) -> dict:
    wkeys = jax.random.split(jax.random.key(seed), 20)
    pkeys = jax.random.split(jax.random.fold_in(jax.random.key(seed + 1), part), 16)

    def draw_matrix(key, rows, cols, factor=1.0):
        return (jax.random.normal(key, (rows, cols), jnp.float32) * (factor * rows ** -0.5)).astype(jnp.bfloat16)

    def draw_gain(key, size, spread):
        return (1.0 + spread * jax.random.normal(key, (size,), jnp.float32)).astype(jnp.bfloat16)

    blocks = 8
    x = jax.random.normal(pkeys[0], (BATCH, D), jnp.float32).astype(jnp.bfloat16)
    coarse_k = jax.random.normal(pkeys[1], (BATCH, KV_HEADS, blocks, 1, HEAD), jnp.float32)
    noise_k = jax.random.normal(pkeys[2], (BATCH, KV_HEADS, blocks, CACHE_LEN // blocks, HEAD), jnp.float32)
    ks_cache = (noise_k + coarse_k).reshape(BATCH, KV_HEADS, CACHE_LEN, HEAD).astype(jnp.bfloat16)
    coarse_v = jax.random.normal(pkeys[3], (BATCH, KV_HEADS, blocks, 1, HEAD), jnp.float32)
    noise_v = jax.random.normal(pkeys[4], (BATCH, KV_HEADS, blocks, CACHE_LEN // blocks, HEAD), jnp.float32)
    vs_cache = (0.6 * noise_v + coarse_v).reshape(BATCH, KV_HEADS, CACHE_LEN, HEAD).astype(jnp.bfloat16)
    tile_k = jax.random.normal(pkeys[5], (BATCH, KV_HEADS, TILES, 1, HEAD), jnp.float32)
    noise_kx = jax.random.normal(pkeys[6], (BATCH, KV_HEADS, TILES, TILE_TOK, HEAD), jnp.float32)
    kx_cache = (noise_kx + tile_k).reshape(BATCH, KV_HEADS, TILES * TILE_TOK, HEAD).astype(jnp.bfloat16)
    tile_v = jax.random.normal(pkeys[7], (BATCH, KV_HEADS, TILES, 1, HEAD), jnp.float32)
    noise_vx = jax.random.normal(pkeys[8], (BATCH, KV_HEADS, TILES, TILE_TOK, HEAD), jnp.float32)
    vx_cache = (0.6 * noise_vx + tile_v).reshape(BATCH, KV_HEADS, TILES * TILE_TOK, HEAD).astype(jnp.bfloat16)
    row_ids = jnp.arange(BATCH)
    kind = jax.random.randint(pkeys[9], (BATCH,), 0, 4)
    short_len = jax.random.randint(pkeys[10], (BATCH,), 0, 8)
    long_len = jax.random.randint(pkeys[11], (BATCH,), 0, CACHE_LEN)
    seq_len = jnp.where(row_ids == 0, CACHE_LEN - 1, jnp.where(kind == 0, short_len, long_len)).astype(jnp.int32)
    cols = jnp.arange(TILES)[None, :]
    forced = (cols == (row_ids % TILES)[:, None]) | (cols == ((row_ids + TILES // 2) % TILES)[:, None])
    coin = jax.random.randint(pkeys[12], (BATCH, TILES), 0, 2)
    dropped = (jax.random.randint(pkeys[13], (BATCH,), 0, 4) == 0) & (row_ids > 0)
    tile_vis = jnp.where(dropped[:, None], 0, jnp.where(forced, 1, coin)).astype(jnp.int32)
    gate_raw = jax.random.uniform(wkeys[16], (2,), jnp.float32, -1.0, 1.0)
    cross_gates = jnp.where(gate_raw < 0, -1.0, 1.0) * (0.3 + 1.7 * jnp.abs(gate_raw))
    return {
        'x': x,
        'ks_cache': ks_cache,
        'vs_cache': vs_cache,
        'seq_len': seq_len,
        'kx_cache': kx_cache,
        'vx_cache': vx_cache,
        'tile_vis': tile_vis,
        'attn_norm': draw_gain(wkeys[0], D, 0.35),
        'wq_self': draw_matrix(wkeys[1], D, HEADS * HEAD),
        'wk_self': draw_matrix(wkeys[2], D, KV_HEADS * HEAD),
        'wv_self': draw_matrix(wkeys[3], D, KV_HEADS * HEAD),
        'wo_self': draw_matrix(wkeys[4], HEADS * HEAD, D),
        'mlp_norm': draw_gain(wkeys[5], D, 0.2),
        'wg_self': draw_matrix(wkeys[6], D, FF),
        'wu_self': draw_matrix(wkeys[7], D, FF),
        'wd_self': draw_matrix(wkeys[8], FF, D),
        'xattn_norm': draw_gain(wkeys[9], D, 0.2),
        'wq_cross': draw_matrix(wkeys[10], D, HEADS * HEAD),
        'q_norm': draw_gain(wkeys[11], HEAD, 0.5),
        'wo_cross': draw_matrix(wkeys[12], HEADS * HEAD, D, factor=1.5),
        'cross_gates': cross_gates,
        'xmlp_norm': draw_gain(wkeys[13], D, 0.2),
        'wg_cross': draw_matrix(wkeys[14], D, FF),
        'wu_cross': draw_matrix(wkeys[15], D, FF),
        'wd_cross': draw_matrix(wkeys[17], FF, D, factor=1.5),
    }


def reference(x, ks_cache, vs_cache, seq_len, kx_cache, vx_cache, tile_vis, attn_norm, wq_self, wk_self, wv_self, wo_self, mlp_norm, wg_self, wu_self, wd_self, xattn_norm, wq_cross, q_norm, wo_cross, cross_gates, xmlp_norm, wg_cross, wu_cross, wd_cross):
    group = HEADS // KV_HEADS
    x_float = x.astype(jnp.float32)
    angles = seq_len.astype(jnp.float32)[:, None] * rope_freqs()[None, :]
    cos_t = jnp.cos(angles)[:, None, :]
    sin_t = jnp.sin(angles)[:, None, :]
    x_norm = rms_norm(x_float, attn_norm).astype(jnp.bfloat16)
    query = apply_rope(jnp.dot(x_norm, wq_self, preferred_element_type=jnp.float32).reshape(BATCH, HEADS, HEAD), cos_t, sin_t)
    query = query.astype(jnp.bfloat16).reshape(BATCH, KV_HEADS, group, HEAD)
    key_new = apply_rope(jnp.dot(x_norm, wk_self, preferred_element_type=jnp.float32).reshape(BATCH, KV_HEADS, HEAD), cos_t, sin_t).astype(jnp.bfloat16)
    val_new = jnp.dot(x_norm, wv_self, preferred_element_type=jnp.float32).astype(jnp.bfloat16).reshape(BATCH, KV_HEADS, HEAD)
    slot_ids = jnp.arange(CACHE_LEN)[None, :]
    slot_hit = (slot_ids == seq_len[:, None])[:, None, :, None]
    keys_full = jnp.where(slot_hit, key_new[:, :, None, :], ks_cache)
    values_full = jnp.where(slot_hit, val_new[:, :, None, :], vs_cache)
    visible_self = slot_ids <= seq_len[:, None]
    attn_self = lax.map(lambda row: attend_row(row[0], row[1], row[2], row[3]), (query, keys_full, values_full, visible_self))
    h_one = (x_float + jnp.dot(attn_self, wo_self, preferred_element_type=jnp.float32)).astype(jnp.bfloat16)
    h_one_f = h_one.astype(jnp.float32)
    h_two = (h_one_f + swiglu(h_one_f, mlp_norm, wg_self, wu_self, wd_self)).astype(jnp.bfloat16)
    h_two_f = h_two.astype(jnp.float32)
    cx_norm = rms_norm(h_two_f, xattn_norm).astype(jnp.bfloat16)
    query_x = jnp.dot(cx_norm, wq_cross, preferred_element_type=jnp.float32).reshape(BATCH, HEADS, HEAD)
    query_x = rms_norm(query_x, q_norm).astype(jnp.bfloat16).reshape(BATCH, KV_HEADS, group, HEAD)
    tile_on = tile_vis != 0
    visible_cross = jnp.broadcast_to(tile_on[:, :, None], (BATCH, TILES, TILE_TOK)).reshape(BATCH, TILES * TILE_TOK)
    attn_cross = lax.map(lambda row: attend_row(row[0], row[1], row[2], row[3]), (query_x, kx_cache, vx_cache, visible_cross))
    row_on = jnp.any(tile_on, axis=1).astype(jnp.float32)[:, None]
    gates = jnp.tanh(cross_gates)
    h_three = (h_two_f + gates[0] * row_on * jnp.dot(attn_cross, wo_cross, preferred_element_type=jnp.float32)).astype(jnp.bfloat16)
    h_three_f = h_three.astype(jnp.float32)
    h_four = (h_three_f + gates[1] * row_on * swiglu(h_three_f, xmlp_norm, wg_cross, wu_cross, wd_cross)).astype(jnp.bfloat16)
    return (h_four, key_new, val_new)
```

```python
import math
import jax
import jax.numpy as jnp
from jax import lax
from jax.experimental import pallas as pl
from jax.experimental.pallas import tpu as pltpu
from jax.sharding import PartitionSpec as P

NORM_EPS = 1e-5
ROPE_THETA = 500000.0
MASK_VALUE = -1e30
LANES = 128
SLOTS = 4
SCALE = 0.125


def rope_freqs(head_dim):
    freq_list = []
    for index in range(head_dim // 2):
        base_freq = 1.0 / (ROPE_THETA ** (2.0 * index / head_dim))
        wave_len = 2.0 * math.pi / base_freq
        if wave_len < 2048.0:
            freq_list.append(base_freq)
        elif wave_len > 8192.0:
            freq_list.append(base_freq / 8.0)
        else:
            smooth = (8192.0 / wave_len - 1.0) / 3.0
            freq_list.append((1.0 - smooth) * base_freq / 8.0 + smooth * base_freq)
    return jnp.array(freq_list, dtype=jnp.float32)


def rms_norm(hidden, gain):
    return hidden * lax.rsqrt(jnp.mean(hidden * hidden, axis=-1, keepdims=True) + NORM_EPS) * gain.astype(jnp.float32)


def apply_rope(tensor, cos_t, sin_t):
    half = tensor.shape[-1] // 2
    first = tensor[..., :half]
    second = tensor[..., half:]
    return jnp.concatenate([first * cos_t - second * sin_t, second * cos_t + first * sin_t], axis=-1)


def swiglu_part(h_norm, w_gate, w_up, w_down):
    gate = jnp.dot(h_norm, w_gate, preferred_element_type=jnp.float32)
    upper = jnp.dot(h_norm, w_up, preferred_element_type=jnp.float32)
    hidden_act = (jax.nn.silu(gate) * upper).astype(jnp.bfloat16)
    return jnp.dot(hidden_act, w_down, preferred_element_type=jnp.float32)


def self_partial(query, keys, values, visible, key_new, val_new, owner):
    score_scale = query.shape[-1] ** -0.5
    mask = visible[:, None, None, :]
    owner_mask = owner[:, None, None]
    scores = jnp.einsum('bkgd,bktd->bkgt', query, keys, preferred_element_type=jnp.float32) * score_scale
    scores = jnp.where(mask, scores, MASK_VALUE)
    new_score = jnp.einsum('clhe,cle->clh', query, key_new, preferred_element_type=jnp.float32) * score_scale
    new_score = jnp.where(owner_mask, new_score, MASK_VALUE)
    top = jnp.maximum(jnp.max(scores, axis=-1), new_score)
    probs = jnp.where(mask, jnp.exp(scores - top[..., None]), 0.0)
    new_prob = jnp.where(owner_mask, jnp.exp(new_score - top), 0.0)
    total = jnp.sum(probs, axis=-1) + new_prob
    out = jnp.einsum('bkgt,bktd->bkgd', probs.astype(jnp.bfloat16), values, preferred_element_type=jnp.float32) + new_prob[..., None] * val_new[:, :, None, :].astype(jnp.float32)
    return out, top, total


def cross_attention(query_bd, keys, values, tile_rows):
    rows, feat, tokens = keys.shape
    tiles = tile_rows.shape[0]
    half_tokens = tokens
    tile_tok = half_tokens // 2
    base_one = tile_tok // LANES * LANES
    width = tokens - base_one
    width_pad = width
    width_zero = min(width_pad, -(-tile_tok // LANES) * LANES)

    def kernel(tile_ref, q_ref, k_hbm, v_hbm, o_ref, m_ref, l_ref, list_ref, kbuf, vbuf, ksem, vsem):
        kv_index = lax.axis_index('kv')
        first_tile = kv_index * (tiles // 2)

        def add_zero(row, count):
            list_ref[count] = row
            return count + jnp.where(tile_ref[first_tile, row] != 0, 1, 0)

        def add_one(row, count):
            list_ref[count] = row
            return count + jnp.where(tile_ref[first_tile + 1, row] != 0, 1, 0)

        n_zero = lax.fori_loop(0, rows, add_zero, jnp.int32(0))
        list_ref[n_zero] = list_ref[jnp.maximum(n_zero - 1, 0)]
        pairs_zero = (n_zero + 1) // 2
        start_one = 2 * pairs_zero
        end_one = lax.fori_loop(0, rows, add_one, start_one)
        n_one = end_one - start_one
        list_ref[end_one] = list_ref[jnp.maximum(end_one - 1, 0)]
        pairs = pairs_zero + (n_one + 1) // 2

        def copies(index, is_one):
            slot = lax.rem(index, SLOTS)
            out = []
            for half in range(2):
                row = list_ref[2 * index + half]
                span = pl.ds(base_one, width) if is_one else pl.ds(0, width_zero)
                dest = pl.ds(0, width) if is_one else pl.ds(0, width_zero)
                for hbm, buf, sem in ((k_hbm, kbuf, ksem), (v_hbm, vbuf, vsem)):
                    out.append(pltpu.make_async_copy(
                        hbm.at[row, :, span], buf.at[slot, pl.ds(half * feat, feat), dest], sem.at[slot, half]))
            return out

        def start(index):
            @pl.when(index < pairs_zero)
            def _():
                for copy in copies(index, False):
                    copy.start()

            @pl.when((index >= pairs_zero) & (index < pairs))
            def _():
                for copy in copies(index, True):
                    copy.start()

        def wait(index):
            @pl.when(index < pairs_zero)
            def _():
                for copy in copies(index, False):
                    copy.wait()

            @pl.when(index >= pairs_zero)
            def _():
                for copy in copies(index, True):
                    copy.wait()

        for index in range(SLOTS - 1):
            start(jnp.int32(index))
        o_ref[...] = jnp.zeros_like(o_ref)
        l_ref[...] = jnp.zeros_like(l_ref)
        m_ref[...] = jnp.full_like(m_ref, MASK_VALUE)

        def step(index, carry):
            start(index + SLOTS - 1)
            wait(index)
            slot = lax.rem(index, SLOTS)
            row_a = list_ref[2 * index]
            row_b = list_ref[2 * index + 1]
            is_one = index >= pairs_zero
            low = jnp.where(is_one, tile_tok - base_one, 0)
            high = jnp.where(is_one, width, tile_tok)
            high_b = jnp.where(is_one, jnp.where(2 * index + 1 == end_one, 0, high), jnp.where(2 * index + 1 == n_zero, 0, high))
            q_a = q_ref[pl.ds(pl.multiple_of(row_a * 8, 8), 8), :]
            q_b = q_ref[pl.ds(pl.multiple_of(row_b * 8, 8), 8), :]
            zero = jnp.zeros_like(q_a)
            q_pair = jnp.concatenate([jnp.concatenate([q_a, zero], axis=1), jnp.concatenate([zero, q_b], axis=1)], axis=0).astype(jnp.bfloat16)
            scores = jnp.dot(q_pair, kbuf[slot], preferred_element_type=jnp.float32)
            lane = lax.broadcasted_iota(jnp.int32, scores.shape, 1)
            sub = lax.broadcasted_iota(jnp.int32, scores.shape, 0)
            visible = (lane >= low) & (lane < jnp.where(sub < 8, high, high_b))
            scores = jnp.where(visible, scores, MASK_VALUE)
            top = jnp.max(scores, axis=1, keepdims=True)
            probs = jnp.where(visible, jnp.exp((scores - top) * SCALE), 0.0)
            total = jnp.sum(probs, axis=1, keepdims=True)
            lane_v = lax.broadcasted_iota(jnp.int32, (2 * feat, width - width_zero), 1)
            tail = jnp.where(lane_v < jnp.where(is_one, width, 0), vbuf[slot, :, width_zero:], jnp.zeros((), jnp.bfloat16))
            vals = jnp.concatenate([vbuf[slot, :, :width_zero], tail], axis=1)
            out = lax.dot_general(probs.astype(jnp.bfloat16), vals, (((1,), (1,)), ((), ())), preferred_element_type=jnp.float32)
            for half, row in ((0, row_a), (1, row_b)):
                where = pl.ds(pl.multiple_of(row * 8, 8), 8)
                part = out[8 * half:8 * half + 8, feat * half:feat * half + feat]
                top_new = jnp.broadcast_to(top[8 * half:8 * half + 8] * SCALE, (8, feat))
                total_new = jnp.broadcast_to(total[8 * half:8 * half + 8], (8, feat))
                top_old = m_ref[where, :]
                best = jnp.maximum(top_old, top_new)
                w_old = jnp.exp(top_old - best)
                w_new = jnp.exp(top_new - best)
                m_ref[where, :] = best
                l_ref[where, :] = l_ref[where, :] * w_old + total_new * w_new
                o_ref[where, :] = o_ref[where, :] * w_old + part * w_new
            return carry

        lax.fori_loop(0, pairs, step, 0)

    flat = jax.ShapeDtypeStruct((rows * 8, feat), jnp.float32)
    return pl.pallas_call(
        kernel,
        out_shape=(flat, flat, flat),
        in_specs=[pl.BlockSpec(memory_space=pltpu.SMEM), pl.BlockSpec(memory_space=pltpu.VMEM),
                  pl.BlockSpec(memory_space=pl.ANY), pl.BlockSpec(memory_space=pl.ANY)],
        out_specs=(pl.BlockSpec(memory_space=pltpu.VMEM),) * 3,
        scratch_shapes=[pltpu.SMEM((2 * rows + 8,), jnp.int32),
                        pltpu.VMEM((SLOTS, 2 * feat, width_pad), jnp.bfloat16),
                        pltpu.VMEM((SLOTS, 2 * feat, width_pad), jnp.bfloat16),
                        pltpu.SemaphoreType.DMA((SLOTS, 2)), pltpu.SemaphoreType.DMA((SLOTS, 2))],
        compiler_params=pltpu.CompilerParams(vmem_limit_bytes=40 * 1024 * 1024),
        cost_estimate=pl.CostEstimate(flops=4 * 8 * feat * tokens * rows, bytes_accessed=2 * feat * tokens * rows, transcendentals=8 * tokens * rows),
        name='cross_attention',
    )(tile_rows, query_bd, keys, values)


def combine_partials(out, top, total):
    head_dim = out.shape[-1]
    packed = jnp.concatenate([out, top[..., None], total[..., None]], axis=-1)
    gathered = lax.all_gather(packed, 'kv', axis=0)
    tops = gathered[..., head_dim]
    best = jnp.max(tops, axis=0)
    weight = jnp.exp(tops - best[None])
    weight_sum = jnp.sum(gathered[..., head_dim + 1] * weight, axis=0)
    combined = jnp.sum(gathered[..., :head_dim] * weight[..., None], axis=0)
    return (combined / jnp.where(weight_sum > 0, weight_sum, 1.0)[..., None]).astype(jnp.bfloat16)


def solution(mesh):
    kv_size = mesh.shape['kv']
    rows_spec = P('dp', None)
    cache_spec = P('dp', 'tp', 'kv', None)
    new_spec = P('dp', 'tp', None)
    col_spec = P(None, 'tp')
    row_spec = P('tp', None)
    vec_spec = P(None)
    in_specs = (rows_spec, cache_spec, cache_spec, P('dp'), cache_spec, cache_spec, rows_spec,
                vec_spec, col_spec, col_spec, col_spec, row_spec, vec_spec, col_spec, col_spec, row_spec,
                vec_spec, col_spec, vec_spec, row_spec, vec_spec, vec_spec, col_spec, col_spec, row_spec)
    out_specs = (rows_spec, new_spec, new_spec)

    def device_step(x, ks_cache, vs_cache, seq_len, kx_cache, vx_cache, tile_vis, attn_norm, wq_self, wk_self, wv_self, wo_self, mlp_norm, wg_self, wu_self, wd_self, xattn_norm, wq_cross, q_norm, wo_cross, cross_gates, xmlp_norm, wg_cross, wu_cross, wd_cross):
        batch = x.shape[0]
        kv_local = ks_cache.shape[1]
        shard_len = ks_cache.shape[2]
        head_dim = ks_cache.shape[3]
        heads_local = wq_self.shape[1] // head_dim
        group = heads_local // kv_local
        tiles_local = tile_vis.shape[1] // kv_size
        tile_tok = kx_cache.shape[2] // tiles_local
        kv_index = lax.axis_index('kv')
        angles = seq_len.astype(jnp.float32)[:, None] * rope_freqs(head_dim)[None, :]
        cos_t = jnp.cos(angles)[:, None, :]
        sin_t = jnp.sin(angles)[:, None, :]
        x_float = x.astype(jnp.float32)
        x_norm = rms_norm(x_float, attn_norm).astype(jnp.bfloat16)
        query = apply_rope(jnp.dot(x_norm, wq_self, preferred_element_type=jnp.float32).reshape(batch, heads_local, head_dim), cos_t, sin_t)
        query = query.astype(jnp.bfloat16).reshape(batch, kv_local, group, head_dim)
        key_new = apply_rope(jnp.dot(x_norm, wk_self, preferred_element_type=jnp.float32).reshape(batch, kv_local, head_dim), cos_t, sin_t).astype(jnp.bfloat16)
        val_new = jnp.dot(x_norm, wv_self, preferred_element_type=jnp.float32).astype(jnp.bfloat16).reshape(batch, kv_local, head_dim)
        slot_ids = kv_index * shard_len + jnp.arange(shard_len)
        visible_self = slot_ids[None, :] < seq_len[:, None]
        owner = (seq_len // shard_len) == kv_index
        out, top, total = self_partial(query, ks_cache, vs_cache, visible_self, key_new, val_new, owner)
        attn_self = combine_partials(out, top, total).reshape(batch, heads_local * head_dim)
        proj_self = lax.psum(jnp.dot(attn_self, wo_self, preferred_element_type=jnp.float32), 'tp')
        h_one = (x_float + proj_self).astype(jnp.bfloat16)
        h_one_f = h_one.astype(jnp.float32)
        mlp_self = swiglu_part(rms_norm(h_one_f, mlp_norm).astype(jnp.bfloat16), wg_self, wu_self, wd_self)
        h_two = (h_one_f + lax.psum(mlp_self, 'tp')).astype(jnp.bfloat16)
        h_two_f = h_two.astype(jnp.float32)
        cx_norm = rms_norm(h_two_f, xattn_norm).astype(jnp.bfloat16)
        query_x = jnp.dot(cx_norm, wq_cross, preferred_element_type=jnp.float32).reshape(batch, heads_local, head_dim)
        query_x = rms_norm(query_x, q_norm).astype(jnp.bfloat16).reshape(batch, kv_local, group, head_dim)
        tile_on = tile_vis != 0
        tokens = kx_cache.shape[2]
        qf = query_x.astype(jnp.float32)
        zero = jnp.zeros_like(qf[:, :1])
        query_bd = jnp.concatenate([jnp.concatenate([qf[:, :1], zero], axis=-1), jnp.concatenate([zero, qf[:, 1:]], axis=-1)], axis=1)
        keys_t = jnp.swapaxes(kx_cache, 2, 3).reshape(batch, kv_local * head_dim, tokens)
        vals_t = jnp.swapaxes(vx_cache, 2, 3).reshape(batch, kv_local * head_dim, tokens)
        out_x, top_x, total_x = cross_attention(query_bd.reshape(batch * heads_local, 2 * head_dim), keys_t, vals_t, tile_vis.T)
        out_x = out_x.reshape(batch, kv_local, group, kv_local, head_dim)
        out_x = jnp.stack([out_x[:, 0, :, 0], out_x[:, 1, :, 1]], axis=1)
        top_x = top_x.reshape(batch, kv_local, group, -1)[..., 0]
        total_x = total_x.reshape(batch, kv_local, group, -1)[..., 0]
        attn_cross = combine_partials(out_x, top_x, total_x).reshape(batch, heads_local * head_dim)
        row_on = jnp.any(tile_on, axis=1).astype(jnp.float32)[:, None]
        gates = jnp.tanh(cross_gates)
        proj_cross = lax.psum(jnp.dot(attn_cross, wo_cross, preferred_element_type=jnp.float32), 'tp')
        h_three = (h_two_f + gates[0] * row_on * proj_cross).astype(jnp.bfloat16)
        h_three_f = h_three.astype(jnp.float32)
        mlp_cross = swiglu_part(rms_norm(h_three_f, xmlp_norm).astype(jnp.bfloat16), wg_cross, wu_cross, wd_cross)
        h_four = (h_three_f + gates[1] * row_on * lax.psum(mlp_cross, 'tp')).astype(jnp.bfloat16)
        return h_four, key_new, val_new

    return jax.shard_map(device_step, mesh=mesh, in_specs=in_specs, out_specs=out_specs, check_vma=False)
```

```python
import math
import jax
import jax.numpy as jnp
from jax import lax
from jax.experimental import pallas as pl
from jax.experimental.pallas import tpu as pltpu
from jax.sharding import PartitionSpec as P

NORM_EPS = 1e-5
ROPE_THETA = 500000.0
MASK_VALUE = -1e30
LANES = 128
SLOTS = 4
SCALE = 0.125


def rope_freqs(head_dim):
    freq_list = []
    for index in range(head_dim // 2):
        base_freq = 1.0 / (ROPE_THETA ** (2.0 * index / head_dim))
        wave_len = 2.0 * math.pi / base_freq
        if wave_len < 2048.0:
            freq_list.append(base_freq)
        elif wave_len > 8192.0:
            freq_list.append(base_freq / 8.0)
        else:
            smooth = (8192.0 / wave_len - 1.0) / 3.0
            freq_list.append((1.0 - smooth) * base_freq / 8.0 + smooth * base_freq)
    return jnp.array(freq_list, dtype=jnp.float32)


MESH_ID = pl.DeviceIdType.MESH
CHUNKS = 4
ANY = pl.BlockSpec(memory_space=pl.ANY)
VMEM = pl.BlockSpec(memory_space=pltpu.VMEM)
SMEM = pl.BlockSpec(memory_space=pltpu.SMEM)
GROUP_ROWS = 8
BIG_VMEM = 60 * 1024 * 1024


def neighbours():
    row = lax.axis_index('kv')
    place = lax.axis_index('tp')
    core = lax.rem(place, 2)
    return row, core, {'tp': place + 1 - 2 * core}, {'tp': lax.rem(place + 2, 4)}, {'kv': 1 - row}


def greet(barrier, peers):
    for peer in peers:
        pl.semaphore_signal(barrier, inc=1, device_id=peer, device_id_type=MESH_ID)


def remote(src, dst, sems, index, peer):
    return pltpu.make_async_remote_copy(src_ref=src, dst_ref=dst, send_sem=sems.at[(0,) + index], recv_sem=sems.at[(1,) + index],
                                        device_id=peer, device_id_type=MESH_ID)


def reduce_chips(produce, part, from_core, chip, from_chip, sems, core, other_core, other_chip):
    first, second = [], []
    for j in range(CHUNKS):
        block = produce(j)
        width = block.shape[1] // 2
        part[j, 0] = block[:, :width]
        part[j, 1] = block[:, width:]
        copy = remote(part.at[j, 1 - core], from_core.at[j], sems, (0, j), other_core)
        copy.start()
        first.append(copy)
    for j in range(CHUNKS):
        first[j].wait_recv()
        chip[j] = part[j, core] + from_core[j]
        copy = remote(chip.at[j], from_chip.at[j], sems, (1, j), other_chip)
        copy.start()
        second.append(copy)
    return first, second


def all_reduce(produce, part, from_core, chip, from_chip, total, sems, core, other_core, other_chip):
    first, second = reduce_chips(produce, part, from_core, chip, from_chip, sems, core, other_core, other_chip)
    third = []
    for j in range(CHUNKS):
        second[j].wait_recv()
        total[j, core] = chip[j] + from_chip[j]
        copy = remote(total.at[j, core], total.at[j, core], sems, (2, j), other_core)
        copy.start()
        third.append(copy)
    for copy in third:
        copy.wait_recv()
    return first + second + third


def norm_chunks(chunks, gains_ref, index):
    width = chunks[0].shape[1]
    square = sum(jnp.sum(c * c, axis=1, keepdims=True) for c in chunks)
    inv = lax.rsqrt(square / (width * len(chunks)) + NORM_EPS)
    return jnp.concatenate([(c * inv * gains_ref[index:index + 1, k * width:(k + 1) * width]).astype(jnp.bfloat16)
                            for k, c in enumerate(chunks)], axis=1)


def swiglu_hidden(u_ref, wg_ref, wu_ref, act_ref):
    block = 512
    for n in range(wg_ref.shape[1] // block):
        cols = pl.ds(n * block, block)
        gate = jnp.dot(u_ref[...], wg_ref[:, cols], preferred_element_type=jnp.float32)
        upper = jnp.dot(u_ref[...], wu_ref[:, cols], preferred_element_type=jnp.float32)
        act_ref[:, cols] = (jax.nn.silu(gate) * upper).astype(jnp.bfloat16)


def chunk_dot(lhs_ref, w_ref):
    block = w_ref.shape[1] // CHUNKS
    return lambda j: jnp.dot(lhs_ref[...], w_ref[:, j * block:(j + 1) * block], preferred_element_type=jnp.float32)


def half_lane(shape):
    return lax.broadcasted_iota(jnp.int32, shape, 1) < shape[1] // 2


def half_sums(value):
    low = half_lane(value.shape)
    return jnp.where(low, jnp.sum(jnp.where(low, value, 0.0), axis=1, keepdims=True),
                     jnp.sum(jnp.where(low, 0.0, value), axis=1, keepdims=True))


def by_group(columns, group):
    low = half_lane(columns[0].shape)
    out = []
    for g in range(group):
        a, b = columns[g // 2], columns[group // 2 + g // 2]
        if g % 2 == 0:
            out.append(jnp.where(low, a, pltpu.roll(b, b.shape[1] // 2, 1)))
        else:
            out.append(jnp.where(low, pltpu.roll(a, a.shape[1] // 2, 1), b))
    return out


def store_block_diagonal(ref, groups, lead=()):
    rows, lanes = groups[0].shape
    low = half_lane((rows, lanes))
    for g, value in enumerate(groups):
        ref[lead + (pl.ds(g, rows, stride=8), slice(None))] = jnp.where(low, value, 0.0)
        ref[lead + (pl.ds(4 + g, rows, stride=8), slice(None))] = jnp.where(low, 0.0, value)


def load_groups(ref, lead, rows, lanes, group):
    low = half_lane((rows, lanes))
    return [jnp.where(low, ref[lead, pl.ds(g, rows, stride=8), :], ref[lead, pl.ds(4 + g, rows, stride=8), :]) for g in range(group)]


def pack_partial(tx, outs, tops, totals):
    group = len(outs)
    lane = lax.rem(lax.broadcasted_iota(jnp.int32, outs[0].shape, 1), outs[0].shape[1] // 2)
    packed = jnp.zeros_like(outs[0])
    for g in range(group):
        tx[g] = outs[g]
        packed = jnp.where(lane == g, tops[g], packed)
        packed = jnp.where(lane == group + g, totals[g], packed)
    tx[group] = packed


def unpack_partial(rx, group):
    packed = rx[group]
    low = half_lane(packed.shape)
    middle = packed.shape[1] // 2

    def spread(k):
        return jnp.where(low, jnp.broadcast_to(packed[:, k:k + 1], packed.shape), jnp.broadcast_to(packed[:, middle + k:middle + k + 1], packed.shape))

    return [rx[g] for g in range(group)], [spread(g) for g in range(group)], [spread(group + g) for g in range(group)]


def merge(parts):
    best = parts[0][1]
    for _, top, _ in parts[1:]:
        best = jnp.maximum(best, top)
    out, total = 0.0, 0.0
    for value, top, count in parts:
        weight = jnp.exp(top - best)
        out = out + value * weight
        total = total + count * weight
    return out / jnp.where(total > 0, total, 1.0)


def load_projection(w_hbm, w_ref, sems, group, head_dim):
    out = []
    for g in range(group):
        for h in range(2):
            out.append(pltpu.make_async_copy(w_hbm.at[pl.ds((h * group + g) * head_dim, head_dim), :],
                                             w_ref.at[pl.ds((g * 2 + h) * head_dim, head_dim), :], sems.at[g * 2 + h]))
    return out


def self_layer(x, keys, values, seq_len, gains, wq, wk, wv, wo, wg, wu, wd, wqc, group):
    batch, width = x.shape
    feat = wk.shape[1]
    head_dim = feat // 2
    slots = keys.shape[1]
    mine = batch // 2
    ff = wg.shape[1]
    qcols = wq.shape[1]
    loads = batch // GROUP_ROWS
    chunk = width // CHUNKS // 2

    def kernel(seq_ref, x_ref, gains_ref, k_hbm, v_hbm, wq_hbm, wk_hbm, wv_hbm, wo_hbm, wg_hbm, wu_hbm, wd_hbm, wqc_hbm,
               kn_ref, vn_ref, qx_ref, h_ref,
               wq_ref, wk_ref, wv_ref, kbuf, vbuf, wo_ref, wg_ref, wu_ref, wd_ref, wqc_ref,
               seqf, qg_ref, knf, vnf, q3_ref, o_ref, m_ref, l_ref, tx, rx, att_ref, u_ref, act_ref,
               part, from_core, chip, from_chip, total, qtx, qrx,
               wsem, ksem, vsem, osem, red_sems, pair_sems):
        row, core, other_core, other_chip, other_row = neighbours()
        barrier = pltpu.get_barrier_semaphore()
        greet(barrier, (other_core, other_chip, other_row))

        def fetch(src, dst, index):
            copy = pltpu.make_async_copy(src, dst, wsem.at[index])
            copy.start()
            return copy

        c_q, c_k, c_v = fetch(wq_hbm, wq_ref, 0), fetch(wk_hbm, wk_ref, 1), fetch(wv_hbm, wv_ref, 2)

        def cache_copies(index):
            start = lax.rem((1 - row) * mine + index * GROUP_ROWS, batch)
            rows = pl.ds(pl.multiple_of(start * feat, GROUP_ROWS * feat), GROUP_ROWS * feat)
            return (pltpu.make_async_copy(k_hbm.at[rows, :], kbuf.at[rows, :], ksem.at[index]),
                    pltpu.make_async_copy(v_hbm.at[rows, :], vbuf.at[rows, :], vsem.at[index]))

        for index in range(loads):
            for copy in cache_copies(index):
                copy.start()
        c_o = load_projection(wo_hbm, wo_ref, osem, group, head_dim)
        for copy in c_o:
            copy.start()
        c_g, c_u, c_d = fetch(wg_hbm, wg_ref, 3), fetch(wu_hbm, wu_ref, 4), fetch(wd_hbm, wd_ref, 5)
        c_qc = fetch(wqc_hbm, wqc_ref, 6)

        for b in range(batch):
            seqf[b:b + 1, :] = jnp.full((1, feat), seq_ref[b].astype(jnp.float32))
        angles = seqf[...] * gains_ref[5:6, :feat]
        lane = lax.rem(lax.broadcasted_iota(jnp.int32, (batch, feat), 1), head_dim)
        first = lane < head_dim // 2
        cos_t = jnp.cos(angles)
        sin_t = jnp.where(first, -jnp.sin(angles), jnp.sin(angles))

        def rope(value):
            partner = jnp.where(first, pltpu.roll(value, feat - head_dim // 2, 1), pltpu.roll(value, head_dim // 2, 1))
            return (value * cos_t + partner * sin_t).astype(jnp.bfloat16).astype(jnp.float32)

        x_float = x_ref[...].astype(jnp.float32)
        inv = lax.rsqrt(jnp.mean(x_float * x_float, axis=1, keepdims=True) + NORM_EPS)
        x_norm = (x_float * inv * gains_ref[0:1, :]).astype(jnp.bfloat16)
        c_q.wait()
        query = jnp.dot(x_norm, wq_ref[...], preferred_element_type=jnp.float32)
        groups = by_group([rope(query[:, n * feat:(n + 1) * feat]) for n in range(qcols // feat)], group)
        for g in range(group):
            qg_ref[g] = groups[g]
        store_block_diagonal(q3_ref, groups)
        c_k.wait()
        key_new = rope(jnp.dot(x_norm, wk_ref[...], preferred_element_type=jnp.float32))
        c_v.wait()
        val_new = jnp.dot(x_norm, wv_ref[...], preferred_element_type=jnp.float32).astype(jnp.bfloat16)
        kn_ref[...] = key_new.astype(jnp.bfloat16)
        vn_ref[...] = val_new
        knf[...] = key_new
        vnf[...] = val_new.astype(jnp.float32)

        def attend(phase, start, local):
            q_a = q3_ref[pl.ds(pl.multiple_of(start * 8, 16), 8), :]
            q_b = q3_ref[pl.ds(pl.multiple_of(start * 8, 16) + 8, 8), :]
            zero = jnp.zeros_like(q_a)
            q_pair = jnp.concatenate([jnp.concatenate([q_a, zero], axis=1), jnp.concatenate([zero, q_b], axis=1)], axis=0).astype(jnp.bfloat16)
            rows = pl.ds(pl.multiple_of(start * feat, 2 * feat), 2 * feat)
            scores = jnp.dot(q_pair, kbuf[rows, :], preferred_element_type=jnp.float32)
            slot = lax.broadcasted_iota(jnp.int32, scores.shape, 1)
            sub = lax.broadcasted_iota(jnp.int32, scores.shape, 0)
            visible = slot < jnp.where(sub < 8, seq_ref[start], seq_ref[start + 1]) - row * slots
            scores = jnp.where(visible, scores, MASK_VALUE)
            top = jnp.max(scores, axis=1, keepdims=True)
            probs = jnp.where(visible, jnp.exp((scores - top) * SCALE), 0.0)
            count = jnp.sum(probs, axis=1, keepdims=True)
            out = lax.dot_general(probs.astype(jnp.bfloat16), vbuf[rows, :], (((1,), (1,)), ((), ())), preferred_element_type=jnp.float32)
            for half in range(2):
                where = pl.ds(pl.multiple_of(local * 8, 16) + 8 * half, 8)
                o_ref[phase, where, :] = out[8 * half:8 * half + 8, feat * half:feat * half + feat]
                m_ref[phase, where, :] = jnp.broadcast_to(top[8 * half:8 * half + 8] * SCALE, (8, feat))
                l_ref[phase, where, :] = jnp.broadcast_to(count[8 * half:8 * half + 8], (8, feat))

        def attend_half(phase):
            def body(index, carry):
                k_copy, v_copy = cache_copies(phase * (loads // 2) + index)
                k_copy.wait()
                v_copy.wait()
                start = lax.rem((1 - row) * mine + (phase * (loads // 2) + index) * GROUP_ROWS, batch)
                for p in range(GROUP_ROWS // 2):
                    attend(phase, start + 2 * p, index * GROUP_ROWS + 2 * p)
                return carry

            lax.fori_loop(0, loads // 2, body, 0)

        attend_half(0)
        pack_partial(tx, *(load_groups(ref, 0, mine, feat, group) for ref in (o_ref, m_ref, l_ref)))
        pl.semaphore_wait(barrier, 3)
        sent = remote(tx, rx, pair_sems, (0,), other_row)
        sent.start()
        attend_half(1)

        own = pl.ds(pl.multiple_of(row * mine, mine), mine)
        key_own, val_own = knf[own, :], vnf[own, :]
        outs, tops, counts = (load_groups(ref, 1, mine, feat, group) for ref in (o_ref, m_ref, l_ref))
        new_tops = [half_sums(qg_ref[g, own, :] * key_own) * SCALE for g in range(group)]
        sent.wait_recv()
        outs_p, tops_p, counts_p = unpack_partial(rx, group)
        for g in range(group):
            merged = merge(((outs[g], tops[g], counts[g]), (outs_p[g], tops_p[g], counts_p[g]), (val_own, new_tops[g], 1.0)))
            att_ref[:, g * feat:(g + 1) * feat] = merged.astype(jnp.bfloat16)
        for copy in c_o:
            copy.wait()
        pending = [sent]
        ends = (core, other_core, other_chip)
        pending += all_reduce(chunk_dot(att_ref, wo_ref), part.at[0], from_core.at[0], chip.at[0], from_chip.at[0], total.at[0], red_sems.at[0], *ends)
        cols = [slice(k * chunk, (k + 1) * chunk) for k in range(2 * CHUNKS)]
        hidden = [(x_ref[own, cols[k]].astype(jnp.float32) + total[0, k // 2, k % 2]).astype(jnp.bfloat16).astype(jnp.float32) for k in range(2 * CHUNKS)]
        for k in range(2 * CHUNKS):
            h_ref[k] = hidden[k]
        u_ref[...] = norm_chunks(hidden, gains_ref, 1)
        c_g.wait()
        c_u.wait()
        swiglu_hidden(u_ref, wg_ref, wu_ref, act_ref)
        c_d.wait()
        pending += all_reduce(chunk_dot(act_ref, wd_ref), part.at[1], from_core.at[1], chip.at[1], from_chip.at[1], total.at[1], red_sems.at[1], *ends)
        hidden = [(h_ref[k] + total[1, k // 2, k % 2]).astype(jnp.bfloat16).astype(jnp.float32) for k in range(2 * CHUNKS)]
        for k in range(2 * CHUNKS):
            h_ref[k] = hidden[k]
        u_ref[...] = norm_chunks(hidden, gains_ref, 2)
        c_qc.wait()
        query = jnp.dot(u_ref[...], wqc_ref[...], preferred_element_type=jnp.float32)
        groups = by_group([query[:, n * feat:(n + 1) * feat] for n in range(qcols // feat)], group)
        groups = [(v * lax.rsqrt(half_sums(v * v) / head_dim + NORM_EPS) * gains_ref[4:5, :feat]).astype(jnp.bfloat16).astype(jnp.float32) for v in groups]
        for g in range(group):
            qtx[g] = groups[g]
        sent = remote(qtx, qrx, pair_sems, (1,), other_row)
        sent.start()
        pending.append(sent)
        store_block_diagonal(qx_ref, groups, (row,))
        sent.wait_recv()
        store_block_diagonal(qx_ref, [qrx[g] for g in range(group)], (1 - row,))
        for copy in pending:
            copy.wait_send()

    bf16, f32 = jnp.bfloat16, jnp.float32
    chunk_shape = (2, CHUNKS, mine, chunk)
    return pl.pallas_call(
        kernel,
        out_shape=(jax.ShapeDtypeStruct((batch, feat), bf16), jax.ShapeDtypeStruct((batch, feat), bf16),
                   jax.ShapeDtypeStruct((2, mine * 8, feat), f32), jax.ShapeDtypeStruct((2 * CHUNKS, mine, chunk), f32)),
        in_specs=[SMEM, VMEM, VMEM] + [ANY] * 10,
        out_specs=(VMEM,) * 4,
        scratch_shapes=[pltpu.VMEM(wq.shape, bf16), pltpu.VMEM(wk.shape, bf16), pltpu.VMEM(wv.shape, bf16),
                        pltpu.VMEM(keys.shape, bf16), pltpu.VMEM(values.shape, bf16), pltpu.VMEM(wo.shape, bf16),
                        pltpu.VMEM(wg.shape, bf16), pltpu.VMEM(wu.shape, bf16), pltpu.VMEM(wd.shape, bf16), pltpu.VMEM(wqc.shape, bf16),
                        pltpu.VMEM((batch, feat), f32), pltpu.VMEM((group, batch, feat), f32), pltpu.VMEM((batch, feat), f32), pltpu.VMEM((batch, feat), f32),
                        pltpu.VMEM((batch * 8, feat), f32)] + [pltpu.VMEM((2, mine * 8, feat), f32)] * 3
                       + [pltpu.VMEM((group + 1, mine, feat), f32)] * 2
                       + [pltpu.VMEM((mine, group * feat), bf16), pltpu.VMEM((mine, width), bf16), pltpu.VMEM((mine, ff), bf16)]
                       + [pltpu.VMEM((2, CHUNKS, 2, mine, chunk), f32)] + [pltpu.VMEM(chunk_shape, f32)] * 3 + [pltpu.VMEM((2, CHUNKS, 2, mine, chunk), f32)]
                       + [pltpu.VMEM((group, mine, feat), f32)] * 2
                       + [pltpu.SemaphoreType.DMA((7,)), pltpu.SemaphoreType.DMA((loads,)), pltpu.SemaphoreType.DMA((loads,)), pltpu.SemaphoreType.DMA((2 * group,)),
                          pltpu.SemaphoreType.DMA((2, 2, 3, CHUNKS)), pltpu.SemaphoreType.DMA((2, 2))],
        compiler_params=pltpu.CompilerParams(vmem_limit_bytes=BIG_VMEM, collective_id=1, has_side_effects=True),
        cost_estimate=pl.CostEstimate(flops=2 * batch * width * (3 * ff + 3 * qcols), bytes_accessed=50 * 1024 * 1024, transcendentals=batch * 8 * slots),
        name='self_layer',
    )(seq_len, x, gains, keys, values, wq, wk, wv, wo, wg, wu, wd, wqc)


def cross_tail(outs_in, tops_in, totals_in, hidden_in, tile_rows, gates, gains, wo, wg, wu, wd, group):
    mine = hidden_in.shape[1]
    feat = outs_in.shape[2]
    head_dim = feat // 2
    width, ff = wg.shape
    tiles = tile_rows.shape[0]
    chunk = width // CHUNKS // 2

    def kernel(tile_ref, gate_ref, o_ref, m_ref, l_ref, h_ref, gains_ref, wo_hbm, wg_hbm, wu_hbm, wd_hbm, out_ref,
               wo_ref, wg_ref, wu_ref, wd_ref, on_ref, h3_ref, tx, rx, att_ref, u_ref, act_ref,
               part, from_core, chip, from_chip, total, final,
               wsem, osem, red_sems, pair_sems, far_sems):
        row, core, other_core, other_chip, other_row = neighbours()
        barrier = pltpu.get_barrier_semaphore()
        greet(barrier, (other_core, other_chip, other_row))
        c_o = load_projection(wo_hbm, wo_ref, osem, group, head_dim)
        for copy in c_o:
            copy.start()
        c_w = [pltpu.make_async_copy(src, dst, wsem.at[i]) for i, (src, dst) in enumerate(((wg_hbm, wg_ref), (wu_hbm, wu_ref), (wd_hbm, wd_ref)))]
        for copy in c_w:
            copy.start()
        pack_partial(tx, *(load_groups(ref, 1 - row, mine, feat, group) for ref in (o_ref, m_ref, l_ref)))
        pl.semaphore_wait(barrier, 3)
        sent = remote(tx, rx, pair_sems, (0,), other_row)
        sent.start()
        for r in range(mine):
            seen = tile_ref[0, row * mine + r]
            for t in range(1, tiles):
                seen = jnp.maximum(seen, tile_ref[t, row * mine + r])
            on_ref[r:r + 1, :] = jnp.full((1, chunk), jnp.where(seen != 0, 1.0, 0.0))
        gate_att = jnp.tanh(jnp.full((1, chunk), gate_ref[0]))
        gate_mlp = jnp.tanh(jnp.full((1, chunk), gate_ref[1]))
        outs, tops, counts = (load_groups(ref, row, mine, feat, group) for ref in (o_ref, m_ref, l_ref))
        sent.wait_recv()
        outs_p, tops_p, counts_p = unpack_partial(rx, group)
        for g in range(group):
            merged = merge(((outs[g], tops[g], counts[g]), (outs_p[g], tops_p[g], counts_p[g])))
            att_ref[:, g * feat:(g + 1) * feat] = merged.astype(jnp.bfloat16)
        for copy in c_o:
            copy.wait()
        pending = [sent]
        ends = (core, other_core, other_chip)
        pending += all_reduce(chunk_dot(att_ref, wo_ref), part.at[0], from_core.at[0], chip.at[0], from_chip.at[0], total, red_sems.at[0], *ends)
        hidden = [(h_ref[k] + gate_att * on_ref[...] * total[k // 2, k % 2]).astype(jnp.bfloat16).astype(jnp.float32) for k in range(2 * CHUNKS)]
        for k in range(2 * CHUNKS):
            h3_ref[k] = hidden[k]
        u_ref[...] = norm_chunks(hidden, gains_ref, 3)
        c_w[0].wait()
        c_w[1].wait()
        swiglu_hidden(u_ref, wg_ref, wu_ref, act_ref)
        c_w[2].wait()
        first, second = reduce_chips(chunk_dot(act_ref, wd_ref), part.at[1], from_core.at[1], chip.at[1], from_chip.at[1], red_sems.at[1], *ends)
        pending += first + second
        near, far, relay = [], [], []
        for j in range(CHUNKS):
            second[j].wait_recv()
            summed = chip[1, j] + from_chip[1, j]
            final[row, 2 * j + core] = (h3_ref[2 * j + core] + gate_mlp * on_ref[...] * summed).astype(jnp.bfloat16).astype(jnp.float32)
            piece = final.at[row, 2 * j + core]
            far.append(remote(piece, piece, far_sems, (0, j), other_row))
            far[j].start()
            near.append(remote(piece, piece, far_sems, (1, j), other_core))
            near[j].start()
        for j in range(CHUNKS):
            far[j].wait_recv()
            piece = final.at[1 - row, 2 * j + core]
            relay.append(remote(piece, piece, far_sems, (2, j), other_core))
            relay[j].start()
        for j in range(CHUNKS):
            near[j].wait_recv()
        for j in range(CHUNKS):
            relay[j].wait_recv()
        for half in range(2):
            for k in range(2 * CHUNKS):
                out_ref[half * mine:(half + 1) * mine, k * chunk:(k + 1) * chunk] = final[half, k].astype(jnp.bfloat16)
        for copy in pending + near + far + relay:
            copy.wait_send()

    bf16, f32 = jnp.bfloat16, jnp.float32
    chunk_shape = (2, CHUNKS, mine, chunk)
    return pl.pallas_call(
        kernel,
        out_shape=jax.ShapeDtypeStruct((2 * mine, width), bf16),
        in_specs=[SMEM, SMEM] + [VMEM] * 5 + [ANY] * 4,
        out_specs=VMEM,
        scratch_shapes=[pltpu.VMEM(wo.shape, bf16), pltpu.VMEM(wg.shape, bf16), pltpu.VMEM(wu.shape, bf16), pltpu.VMEM(wd.shape, bf16),
                        pltpu.VMEM((mine, chunk), f32), pltpu.VMEM((2 * CHUNKS, mine, chunk), f32)]
                       + [pltpu.VMEM((group + 1, mine, feat), f32)] * 2
                       + [pltpu.VMEM((mine, group * feat), bf16), pltpu.VMEM((mine, width), bf16), pltpu.VMEM((mine, ff), bf16)]
                       + [pltpu.VMEM((2, CHUNKS, 2, mine, chunk), f32)] + [pltpu.VMEM(chunk_shape, f32)] * 3 + [pltpu.VMEM((CHUNKS, 2, mine, chunk), f32)]
                       + [pltpu.VMEM((2, 2 * CHUNKS, mine, chunk), f32)]
                       + [pltpu.SemaphoreType.DMA((3,)), pltpu.SemaphoreType.DMA((2 * group,)),
                          pltpu.SemaphoreType.DMA((2, 2, 3, CHUNKS)), pltpu.SemaphoreType.DMA((2, 1)), pltpu.SemaphoreType.DMA((2, 3, CHUNKS))],
        compiler_params=pltpu.CompilerParams(vmem_limit_bytes=BIG_VMEM, collective_id=2, has_side_effects=True),
        cost_estimate=pl.CostEstimate(flops=4 * mine * width * 3 * ff, bytes_accessed=30 * 1024 * 1024, transcendentals=mine * ff),
        name='cross_tail',
    )(tile_rows, gates, outs_in, tops_in, totals_in, hidden_in, gains, wo, wg, wu, wd)


def cross_attention(query_bd, keys, values, tile_rows):
    rows, feat, tokens = keys.shape
    tiles = tile_rows.shape[0]
    half_tokens = tokens
    tile_tok = half_tokens // 2
    base_one = tile_tok // LANES * LANES
    width = tokens - base_one
    width_pad = width
    width_zero = min(width_pad, -(-tile_tok // LANES) * LANES)

    def kernel(tile_ref, q_ref, k_hbm, v_hbm, o_ref, m_ref, l_ref, list_ref, kbuf, vbuf, ksem, vsem):
        kv_index = lax.axis_index('kv')
        first_tile = kv_index * (tiles // 2)

        def add_zero(row, count):
            list_ref[count] = row
            return count + jnp.where(tile_ref[first_tile, row] != 0, 1, 0)

        def add_one(row, count):
            list_ref[count] = row
            return count + jnp.where(tile_ref[first_tile + 1, row] != 0, 1, 0)

        n_zero = lax.fori_loop(0, rows, add_zero, jnp.int32(0))
        list_ref[n_zero] = list_ref[jnp.maximum(n_zero - 1, 0)]
        pairs_zero = (n_zero + 1) // 2
        start_one = 2 * pairs_zero
        end_one = lax.fori_loop(0, rows, add_one, start_one)
        n_one = end_one - start_one
        list_ref[end_one] = list_ref[jnp.maximum(end_one - 1, 0)]
        pairs = pairs_zero + (n_one + 1) // 2

        def copies(index, is_one):
            slot = lax.rem(index, SLOTS)
            out = []
            for half in range(2):
                row = list_ref[2 * index + half]
                span = pl.ds(base_one, width) if is_one else pl.ds(0, width_zero)
                dest = pl.ds(0, width) if is_one else pl.ds(0, width_zero)
                for hbm, buf, sem in ((k_hbm, kbuf, ksem), (v_hbm, vbuf, vsem)):
                    out.append(pltpu.make_async_copy(
                        hbm.at[row, :, span], buf.at[slot, pl.ds(half * feat, feat), dest], sem.at[slot, half]))
            return out

        def start(index):
            @pl.when(index < pairs_zero)
            def _():
                for copy in copies(index, False):
                    copy.start()

            @pl.when((index >= pairs_zero) & (index < pairs))
            def _():
                for copy in copies(index, True):
                    copy.start()

        def wait(index):
            @pl.when(index < pairs_zero)
            def _():
                for copy in copies(index, False):
                    copy.wait()

            @pl.when(index >= pairs_zero)
            def _():
                for copy in copies(index, True):
                    copy.wait()

        for index in range(SLOTS - 1):
            start(jnp.int32(index))
        o_ref[...] = jnp.zeros_like(o_ref)
        l_ref[...] = jnp.zeros_like(l_ref)
        m_ref[...] = jnp.full_like(m_ref, MASK_VALUE)

        def step(index, carry):
            start(index + SLOTS - 1)
            wait(index)
            slot = lax.rem(index, SLOTS)
            row_a = list_ref[2 * index]
            row_b = list_ref[2 * index + 1]
            is_one = index >= pairs_zero
            low = jnp.where(is_one, tile_tok - base_one, 0)
            high = jnp.where(is_one, width, tile_tok)
            high_b = jnp.where(is_one, jnp.where(2 * index + 1 == end_one, 0, high), jnp.where(2 * index + 1 == n_zero, 0, high))
            q_a = q_ref[pl.ds(pl.multiple_of(row_a * 8, 8), 8), :]
            q_b = q_ref[pl.ds(pl.multiple_of(row_b * 8, 8), 8), :]
            zero = jnp.zeros_like(q_a)
            q_pair = jnp.concatenate([jnp.concatenate([q_a, zero], axis=1), jnp.concatenate([zero, q_b], axis=1)], axis=0).astype(jnp.bfloat16)
            scores = jnp.dot(q_pair, kbuf[slot], preferred_element_type=jnp.float32)
            lane = lax.broadcasted_iota(jnp.int32, scores.shape, 1)
            sub = lax.broadcasted_iota(jnp.int32, scores.shape, 0)
            visible = (lane >= low) & (lane < jnp.where(sub < 8, high, high_b))
            scores = jnp.where(visible, scores, MASK_VALUE)
            top = jnp.max(scores, axis=1, keepdims=True)
            probs = jnp.where(visible, jnp.exp((scores - top) * SCALE), 0.0)
            total = jnp.sum(probs, axis=1, keepdims=True)
            lane_v = lax.broadcasted_iota(jnp.int32, (2 * feat, width - width_zero), 1)
            tail = jnp.where(lane_v < jnp.where(is_one, width, 0), vbuf[slot, :, width_zero:], jnp.zeros((), jnp.bfloat16))
            vals = jnp.concatenate([vbuf[slot, :, :width_zero], tail], axis=1)
            out = lax.dot_general(probs.astype(jnp.bfloat16), vals, (((1,), (1,)), ((), ())), preferred_element_type=jnp.float32)
            for half, row in ((0, row_a), (1, row_b)):
                where = pl.ds(pl.multiple_of(row * 8, 8), 8)
                part = out[8 * half:8 * half + 8, feat * half:feat * half + feat]
                top_new = jnp.broadcast_to(top[8 * half:8 * half + 8] * SCALE, (8, feat))
                total_new = jnp.broadcast_to(total[8 * half:8 * half + 8], (8, feat))
                top_old = m_ref[where, :]
                best = jnp.maximum(top_old, top_new)
                w_old = jnp.exp(top_old - best)
                w_new = jnp.exp(top_new - best)
                m_ref[where, :] = best
                l_ref[where, :] = l_ref[where, :] * w_old + total_new * w_new
                o_ref[where, :] = o_ref[where, :] * w_old + part * w_new
            return carry

        lax.fori_loop(0, pairs, step, 0)

    flat = jax.ShapeDtypeStruct((rows * 8, feat), jnp.float32)
    return pl.pallas_call(
        kernel,
        out_shape=(flat, flat, flat),
        in_specs=[pl.BlockSpec(memory_space=pltpu.SMEM), pl.BlockSpec(memory_space=pltpu.VMEM),
                  pl.BlockSpec(memory_space=pl.ANY), pl.BlockSpec(memory_space=pl.ANY)],
        out_specs=(pl.BlockSpec(memory_space=pltpu.VMEM),) * 3,
        scratch_shapes=[pltpu.SMEM((2 * rows + 8,), jnp.int32),
                        pltpu.VMEM((SLOTS, 2 * feat, width_pad), jnp.bfloat16),
                        pltpu.VMEM((SLOTS, 2 * feat, width_pad), jnp.bfloat16),
                        pltpu.SemaphoreType.DMA((SLOTS, 2)), pltpu.SemaphoreType.DMA((SLOTS, 2))],
        compiler_params=pltpu.CompilerParams(vmem_limit_bytes=40 * 1024 * 1024),
        cost_estimate=pl.CostEstimate(flops=4 * 8 * feat * tokens * rows, bytes_accessed=2 * feat * tokens * rows, transcendentals=8 * tokens * rows),
        name='cross_attention',
    )(tile_rows, query_bd, keys, values)


def solution(mesh):
    rows_spec = P('dp', None)
    cache_spec = P('dp', 'tp', 'kv', None)
    new_spec = P('dp', 'tp', None)
    col_spec = P(None, 'tp')
    row_spec = P('tp', None)
    vec_spec = P(None)
    in_specs = (rows_spec, cache_spec, cache_spec, P('dp'), cache_spec, cache_spec, rows_spec,
                vec_spec, col_spec, col_spec, col_spec, row_spec, vec_spec, col_spec, col_spec, row_spec,
                vec_spec, col_spec, vec_spec, row_spec, vec_spec, vec_spec, col_spec, col_spec, row_spec)
    out_specs = (rows_spec, new_spec, new_spec)

    def device_step(x, ks_cache, vs_cache, seq_len, kx_cache, vx_cache, tile_vis, attn_norm, wq_self, wk_self, wv_self, wo_self, mlp_norm, wg_self, wu_self, wd_self, xattn_norm, wq_cross, q_norm, wo_cross, cross_gates, xmlp_norm, wg_cross, wu_cross, wd_cross):
        batch, width = x.shape
        kv_local, slots, head_dim = ks_cache.shape[1:]
        feat = kv_local * head_dim
        group = wq_self.shape[1] // feat
        tokens = kx_cache.shape[2]
        rows = [attn_norm, mlp_norm, xattn_norm, xmlp_norm, jnp.tile(q_norm, width // head_dim)]
        gains = jnp.stack([r.astype(jnp.float32) for r in rows] + [jnp.tile(rope_freqs(head_dim), 2 * width // head_dim)] + [jnp.zeros((width,), jnp.float32)] * 2)

        def token_minor(cache):
            return jnp.swapaxes(cache, 2, 3).reshape(batch, feat, cache.shape[2])

        key_new, val_new, query_x, h_two = self_layer(
            x, token_minor(ks_cache).reshape(batch * feat, slots), token_minor(vs_cache).reshape(batch * feat, slots), seq_len, gains,
            wq_self, wk_self, wv_self, wo_self, wg_self, wu_self, wd_self, wq_cross, group)
        tile_rows = tile_vis.T
        parts = cross_attention(query_x.reshape(batch * 8, feat), token_minor(kx_cache), token_minor(vx_cache), tile_rows)
        parts = [p.reshape(2, batch * 4, feat) for p in parts]
        h_four = cross_tail(*parts, h_two, tile_rows, cross_gates, gains, wo_cross, wg_cross, wu_cross, wd_cross, group)
        return h_four, key_new.reshape(batch, kv_local, head_dim), val_new.reshape(batch, kv_local, head_dim)

    return jax.shard_map(device_step, mesh=mesh, in_specs=in_specs, out_specs=out_specs, check_vma=False)
```

```python
import functools
import math
import jax
import jax.numpy as jnp
from jax import lax
from jax.experimental import pallas as pl
from jax.experimental.pallas import tpu as pltpu
from jax.sharding import PartitionSpec as P

NORM_EPS = 1e-5
ROPE_THETA = 500000.0
MASK_VALUE = -1e30
LANES = 128
SLOTS = 5
SCALE = 0.125


def rope_freqs(head_dim):
    freq_list = []
    for index in range(head_dim // 2):
        base_freq = 1.0 / (ROPE_THETA ** (2.0 * index / head_dim))
        wave_len = 2.0 * math.pi / base_freq
        if wave_len < 2048.0:
            freq_list.append(base_freq)
        elif wave_len > 8192.0:
            freq_list.append(base_freq / 8.0)
        else:
            smooth = (8192.0 / wave_len - 1.0) / 3.0
            freq_list.append((1.0 - smooth) * base_freq / 8.0 + smooth * base_freq)
    return jnp.array(freq_list, dtype=jnp.float32)


MESH_ID = pl.DeviceIdType.MESH
CHUNKS = 4
ANY = pl.BlockSpec(memory_space=pl.ANY)
VMEM = pl.BlockSpec(memory_space=pltpu.VMEM)
SMEM = pl.BlockSpec(memory_space=pltpu.SMEM)
GROUP_ROWS = 8


def in_hbm(*arrays):
    return [pltpu.with_memory_space_constraint(a, pltpu.HBM) for a in arrays]


def neighbours():
    row = lax.axis_index('kv')
    place = lax.axis_index('tp')
    core = lax.rem(place, 2)
    return row, core, {'tp': place + 1 - 2 * core}, {'tp': lax.rem(place + 2, 4)}, {'kv': 1 - row}


def greet(barrier, peers):
    for peer in peers:
        pl.semaphore_signal(barrier, inc=1, device_id=peer, device_id_type=MESH_ID)


def remote(src, dst, sems, index, peer):
    return pltpu.make_async_remote_copy(src_ref=src, dst_ref=dst, send_sem=sems.at[(0,) + index], recv_sem=sems.at[(1,) + index],
                                        device_id=peer, device_id_type=MESH_ID)


def reduce_chips(produce, part, from_core, chip, from_chip, sems, core, other_core, other_chip):
    first, second = [], []
    for j in range(CHUNKS):
        block = produce(j)
        width = block.shape[1] // 2
        part[j, 0] = block[:, :width]
        part[j, 1] = block[:, width:]
        copy = remote(part.at[j, 1 - core], from_core.at[j], sems, (0, j), other_core)
        copy.start()
        first.append(copy)
    for j in range(CHUNKS):
        first[j].wait_recv()
        chip[j] = part[j, core] + from_core[j]
        copy = remote(chip.at[j], from_chip.at[j], sems, (1, j), other_chip)
        copy.start()
        second.append(copy)
    return first, second


def all_reduce(produce, part, from_core, chip, from_chip, total, sems, core, other_core, other_chip):
    first, second = reduce_chips(produce, part, from_core, chip, from_chip, sems, core, other_core, other_chip)
    third = []
    for j in range(CHUNKS):
        second[j].wait_recv()
        total[j, core] = chip[j] + from_chip[j]
        copy = remote(total.at[j, core], total.at[j, core], sems, (2, j), other_core)
        copy.start()
        third.append(copy)
    for copy in third:
        copy.wait_recv()
    return first + second + third


def lane_row(gain_ref):
    gain = gain_ref[...].astype(jnp.float32)
    return jnp.concatenate([gain[k:k + 1] for k in range(gain.shape[0])], axis=1)


def norm_chunks(chunks, gain_ref):
    width = chunks[0].shape[1]
    gain = lane_row(gain_ref)
    square = sum(jnp.sum(c * c, axis=1, keepdims=True) for c in chunks)
    inv = lax.rsqrt(square / (width * len(chunks)) + NORM_EPS)
    return jnp.concatenate([(c * inv * gain[:, k * width:(k + 1) * width]).astype(jnp.bfloat16)
                            for k, c in enumerate(chunks)], axis=1)


def swiglu_hidden(u_ref, wg_ref, wu_ref, act_ref):
    block = 512
    for n in range(wg_ref.shape[1] // block):
        cols = pl.ds(n * block, block)
        gate = jnp.dot(u_ref[...], wg_ref[:, cols], preferred_element_type=jnp.float32)
        upper = jnp.dot(u_ref[...], wu_ref[:, cols], preferred_element_type=jnp.float32)
        act_ref[:, cols] = (jax.nn.silu(gate) * upper).astype(jnp.bfloat16)


def chunk_dot(lhs_ref, w_ref):
    block = w_ref.shape[1] // CHUNKS
    return lambda j: jnp.dot(lhs_ref[...], w_ref[:, j * block:(j + 1) * block], preferred_element_type=jnp.float32)


def half_lane(shape):
    return lax.broadcasted_iota(jnp.int32, shape, 1) < shape[1] // 2


def half_sums(value):
    low = half_lane(value.shape)
    return jnp.where(low, jnp.sum(jnp.where(low, value, 0.0), axis=1, keepdims=True),
                     jnp.sum(jnp.where(low, 0.0, value), axis=1, keepdims=True))


def by_group(columns, group):
    low = half_lane(columns[0].shape)
    out = []
    for g in range(group):
        a, b = columns[g // 2], columns[group // 2 + g // 2]
        if g % 2 == 0:
            out.append(jnp.where(low, a, pltpu.roll(b, b.shape[1] // 2, 1)))
        else:
            out.append(jnp.where(low, pltpu.roll(a, a.shape[1] // 2, 1), b))
    return out


def store_block_diagonal(ref, groups, lead=()):
    rows, lanes = groups[0].shape
    low = half_lane((rows, lanes))
    for g, value in enumerate(groups):
        ref[lead + (pl.ds(g, rows, stride=8), slice(None))] = jnp.where(low, value, 0.0)
        ref[lead + (pl.ds(4 + g, rows, stride=8), slice(None))] = jnp.where(low, 0.0, value)


def load_groups(ref, lead, rows, lanes, group):
    low = half_lane((rows, lanes))
    return [jnp.where(low, ref[lead, pl.ds(g, rows, stride=8), :], ref[lead, pl.ds(4 + g, rows, stride=8), :]) for g in range(group)]


def pack_partial(tx, outs, tops, totals):
    group = len(outs)
    lane = lax.rem(lax.broadcasted_iota(jnp.int32, outs[0].shape, 1), outs[0].shape[1] // 2)
    packed = jnp.zeros_like(outs[0])
    for g in range(group):
        tx[g] = outs[g]
        packed = jnp.where(lane == g, tops[g], packed)
        packed = jnp.where(lane == group + g, totals[g], packed)
    tx[group] = packed


def unpack_partial(rx, group):
    packed = rx[group]
    low = half_lane(packed.shape)
    middle = packed.shape[1] // 2

    def spread(k):
        return jnp.where(low, jnp.broadcast_to(packed[:, k:k + 1], packed.shape), jnp.broadcast_to(packed[:, middle + k:middle + k + 1], packed.shape))

    return [rx[g] for g in range(group)], [spread(g) for g in range(group)], [spread(group + g) for g in range(group)]


def merge(parts):
    best = parts[0][1]
    for _, top, _ in parts[1:]:
        best = jnp.maximum(best, top)
    out, total = 0.0, 0.0
    for value, top, count in parts:
        weight = jnp.exp(top - best)
        out = out + value * weight
        total = total + count * weight
    return out / jnp.where(total > 0, total, 1.0)


def load_projection(w_hbm, w_ref, sems, group, head_dim):
    out = []
    for g in range(group):
        for h in range(2):
            out.append(pltpu.make_async_copy(w_hbm.at[pl.ds((h * group + g) * head_dim, head_dim), :],
                                             w_ref.at[pl.ds((g * 2 + h) * head_dim, head_dim), :], sems.at[g * 2 + h]))
    return out


def self_layer(x, keys, values, seq_len, gains, freqs, wq, wk, wv, wo, wg, wu, wd, wqc, group):
    batch, width = x.shape
    feat = wk.shape[1]
    head_dim = feat // 2
    slots = keys.shape[1]
    mine = batch // 2
    ff = wg.shape[1]
    qcols = wq.shape[1]
    loads = batch // GROUP_ROWS
    chunk = width // CHUNKS // 2

    def kernel(seq_ref, x_hbm, ga_hbm, gm_hbm, gx_hbm, gq_hbm, f_hbm, k_hbm, v_hbm, wq_hbm, wk_hbm, wv_hbm, wo_hbm, wg_hbm, wu_hbm, wd_hbm, wqc_hbm,
               kn_ref, vn_ref, qx_ref, h_ref,
               x_ref, ga_ref, gm_ref, gx_ref, gq_ref, f_ref, wq_ref, wk_ref, wv_ref, kbuf, vbuf, wo_ref, wg_ref, wu_ref, wd_ref, wqc_ref,
               seqf, qg_ref, q3_ref, o_ref, m_ref, l_ref, tx, rx, att_ref, u_ref, act_ref,
               part, from_core, chip, from_chip, total, qtx, qrx,
               xsem, wsem, ksem, vsem, osem, red_sems, pair_sems):
        row, core, other_core, other_chip, other_row = neighbours()
        barrier = pltpu.get_barrier_semaphore()
        greet(barrier, (other_core, other_chip, other_row))

        small = [pltpu.make_async_copy(src, dst, xsem.at[i]) for i, (src, dst) in enumerate(
            ((f_hbm, f_ref), (ga_hbm, ga_ref), (x_hbm, x_ref), (gm_hbm, gm_ref), (gx_hbm, gx_ref), (gq_hbm, gq_ref)))]
        for copy in small:
            copy.start()

        def fetch(src, dst, index):
            copy = pltpu.make_async_copy(src, dst, wsem.at[index])
            copy.start()
            return copy

        c_q, c_k, c_v = fetch(wq_hbm, wq_ref, 0), fetch(wk_hbm, wk_ref, 1), fetch(wv_hbm, wv_ref, 2)

        def cache_copies(index):
            start = lax.rem((1 - row) * mine + index * GROUP_ROWS, batch)
            rows = pl.ds(pl.multiple_of(start * feat, GROUP_ROWS * feat), GROUP_ROWS * feat)
            return (pltpu.make_async_copy(k_hbm.at[rows, :], kbuf.at[rows, :], ksem.at[index]),
                    pltpu.make_async_copy(v_hbm.at[rows, :], vbuf.at[rows, :], vsem.at[index]))

        def start_cache(quarter):
            for index in range(quarter * loads // 4, (quarter + 1) * loads // 4):
                for copy in cache_copies(index):
                    copy.start()

        c_o = load_projection(wo_hbm, wo_ref, osem, group, head_dim)
        c_g, c_u, c_d, c_qc = (pltpu.make_async_copy(src, dst, wsem.at[3 + i]) for i, (src, dst) in enumerate(
            ((wg_hbm, wg_ref), (wu_hbm, wu_ref), (wd_hbm, wd_ref), (wqc_hbm, wqc_ref))))
        start_cache(0)
        for b in range(batch):
            seqf[b:b + 1, :] = jnp.full((1, feat), seq_ref[b].astype(jnp.float32))
        for copy in small:
            copy.wait()
        angles = seqf[...] * f_ref[...]
        lane = lax.rem(lax.broadcasted_iota(jnp.int32, (batch, feat), 1), head_dim)
        first = lane < head_dim // 2
        cos_t = jnp.cos(angles)
        sin_t = jnp.where(first, -jnp.sin(angles), jnp.sin(angles))

        def rope(value):
            partner = jnp.where(first, pltpu.roll(value, feat - head_dim // 2, 1), pltpu.roll(value, head_dim // 2, 1))
            return (value * cos_t + partner * sin_t).astype(jnp.bfloat16).astype(jnp.float32)

        x_float = x_ref[...].astype(jnp.float32)
        inv = lax.rsqrt(jnp.mean(x_float * x_float, axis=1, keepdims=True) + NORM_EPS)
        x_norm = (x_float * inv * lane_row(ga_ref)).astype(jnp.bfloat16)
        c_q.wait()
        start_cache(1)
        query = jnp.dot(x_norm, wq_ref[...], preferred_element_type=jnp.float32)
        groups = by_group([rope(query[:, n * feat:(n + 1) * feat]) for n in range(qcols // feat)], group)
        for g in range(group):
            qg_ref[g] = groups[g]
        store_block_diagonal(q3_ref, groups)
        c_k.wait()
        key_new = rope(jnp.dot(x_norm, wk_ref[...], preferred_element_type=jnp.float32))
        c_v.wait()
        val_new = jnp.dot(x_norm, wv_ref[...], preferred_element_type=jnp.float32).astype(jnp.bfloat16)
        kn_ref[...] = key_new
        vn_ref[...] = val_new.astype(jnp.float32)

        def attend(phase, start, local):
            q_a = q3_ref[pl.ds(pl.multiple_of(start * 8, 16), 8), :]
            q_b = q3_ref[pl.ds(pl.multiple_of(start * 8, 16) + 8, 8), :]
            zero = jnp.zeros_like(q_a)
            q_pair = jnp.concatenate([jnp.concatenate([q_a, zero], axis=1), jnp.concatenate([zero, q_b], axis=1)], axis=0).astype(jnp.bfloat16)
            rows = pl.ds(pl.multiple_of(start * feat, 2 * feat), 2 * feat)
            scores = jnp.dot(q_pair, kbuf[rows, :], preferred_element_type=jnp.float32)
            slot = lax.broadcasted_iota(jnp.int32, scores.shape, 1)
            sub = lax.broadcasted_iota(jnp.int32, scores.shape, 0)
            visible = slot < jnp.where(sub < 8, seq_ref[start], seq_ref[start + 1]) - row * slots
            scores = jnp.where(visible, scores, MASK_VALUE)
            top = jnp.max(scores, axis=1, keepdims=True)
            probs = jnp.where(visible, jnp.exp((scores - top) * SCALE), 0.0)
            count = jnp.sum(probs, axis=1, keepdims=True)
            out = lax.dot_general(probs.astype(jnp.bfloat16), vbuf[rows, :], (((1,), (1,)), ((), ())), preferred_element_type=jnp.float32)
            for half in range(2):
                where = pl.ds(local * 8 + 8 * half, 8)
                o_ref[phase, where, :] = out[8 * half:8 * half + 8, feat * half:feat * half + feat]
                m_ref[phase, where, :] = jnp.broadcast_to(top[8 * half:8 * half + 8] * SCALE, (8, feat))
                l_ref[phase, where, :] = jnp.broadcast_to(count[8 * half:8 * half + 8], (8, feat))

        def attend_quarter(quarter, following):
            for index in range(quarter * loads // 4, (quarter + 1) * loads // 4):
                for copy in cache_copies(index):
                    copy.wait()
            following()
            phase, part_rows = quarter // 2, mine // 2
            start = lax.rem((1 + phase - row) * mine, batch)
            for p in range(part_rows // 2):
                local = (quarter % 2) * part_rows + 2 * p
                attend(phase, start + local, local)

        def start_all(*copies):
            for copy in copies:
                copy.start()

        attend_quarter(0, lambda: start_cache(2))
        attend_quarter(1, lambda: start_cache(3))
        pack_partial(tx, *(load_groups(ref, 0, mine, feat, group) for ref in (o_ref, m_ref, l_ref)))
        pl.semaphore_wait(barrier, 3)
        sent = remote(tx, rx, pair_sems, (0,), other_row)
        sent.start()
        attend_quarter(2, lambda: start_all(*c_o, c_g))
        attend_quarter(3, lambda: start_all(c_u))
        start_all(c_d, c_qc)

        own = pl.ds(pl.multiple_of(row * mine, mine), mine)
        key_own, val_own = kn_ref[own, :], vn_ref[own, :]
        outs, tops, counts = (load_groups(ref, 1, mine, feat, group) for ref in (o_ref, m_ref, l_ref))
        new_tops = [half_sums(qg_ref[g, own, :] * key_own) * SCALE for g in range(group)]
        sent.wait_recv()
        outs_p, tops_p, counts_p = unpack_partial(rx, group)
        for g in range(group):
            merged = merge(((outs[g], tops[g], counts[g]), (outs_p[g], tops_p[g], counts_p[g]), (val_own, new_tops[g], 1.0)))
            att_ref[:, g * feat:(g + 1) * feat] = merged.astype(jnp.bfloat16)
        for copy in c_o:
            copy.wait()
        pending = [sent]
        ends = (core, other_core, other_chip)
        pending += all_reduce(chunk_dot(att_ref, wo_ref), part.at[0], from_core.at[0], chip.at[0], from_chip.at[0], total.at[0], red_sems.at[0], *ends)
        cols = [slice(k * chunk, (k + 1) * chunk) for k in range(2 * CHUNKS)]
        hidden = [(x_ref[own, cols[k]].astype(jnp.float32) + total[0, k // 2, k % 2]).astype(jnp.bfloat16).astype(jnp.float32) for k in range(2 * CHUNKS)]
        for k in range(2 * CHUNKS):
            h_ref[k] = hidden[k]
        u_ref[...] = norm_chunks(hidden, gm_ref)
        c_g.wait()
        c_u.wait()
        swiglu_hidden(u_ref, wg_ref, wu_ref, act_ref)
        c_d.wait()
        pending += all_reduce(chunk_dot(act_ref, wd_ref), part.at[1], from_core.at[1], chip.at[1], from_chip.at[1], total.at[1], red_sems.at[1], *ends)
        hidden = [(h_ref[k] + total[1, k // 2, k % 2]).astype(jnp.bfloat16).astype(jnp.float32) for k in range(2 * CHUNKS)]
        for k in range(2 * CHUNKS):
            h_ref[k] = hidden[k]
        u_ref[...] = norm_chunks(hidden, gx_ref)
        c_qc.wait()
        query = jnp.dot(u_ref[...], wqc_ref[...], preferred_element_type=jnp.float32)
        groups = by_group([query[:, n * feat:(n + 1) * feat] for n in range(qcols // feat)], group)
        gain = jnp.concatenate([gq_ref[...].astype(jnp.float32)] * 2, axis=1)
        groups = [(v * lax.rsqrt(half_sums(v * v) / head_dim + NORM_EPS) * gain).astype(jnp.bfloat16).astype(jnp.float32) for v in groups]
        for g in range(group):
            qtx[g] = groups[g]
        sent = remote(qtx, qrx, pair_sems, (1,), other_row)
        sent.start()
        pending.append(sent)
        store_block_diagonal(qx_ref, groups, (row,))
        sent.wait_recv()
        store_block_diagonal(qx_ref, [qrx[g] for g in range(group)], (1 - row,))
        for copy in pending:
            copy.wait_send()

    bf16, f32 = jnp.bfloat16, jnp.float32
    chunk_shape = (2, CHUNKS, mine, chunk)
    return pl.pallas_call(
        kernel,
        out_shape=(jax.ShapeDtypeStruct((batch, feat), f32), jax.ShapeDtypeStruct((batch, feat), f32),
                   jax.ShapeDtypeStruct((2, mine * 8, feat), f32), jax.ShapeDtypeStruct((2 * CHUNKS, mine, chunk), f32)),
        in_specs=[SMEM] + [ANY] * 16,
        out_specs=(VMEM,) * 4,
        scratch_shapes=[pltpu.VMEM(a.shape, a.dtype) for a in (x, *gains, freqs)]
                       + [pltpu.VMEM(wq.shape, bf16), pltpu.VMEM(wk.shape, bf16), pltpu.VMEM(wv.shape, bf16),
                        pltpu.VMEM(keys.shape, bf16), pltpu.VMEM(values.shape, bf16), pltpu.VMEM(wo.shape, bf16),
                        pltpu.VMEM(wg.shape, bf16), pltpu.VMEM(wu.shape, bf16), pltpu.VMEM(wd.shape, bf16), pltpu.VMEM(wqc.shape, bf16),
                        pltpu.VMEM((batch, feat), f32), pltpu.VMEM((group, batch, feat), f32),
                        pltpu.VMEM((batch * 8, feat), f32)] + [pltpu.VMEM((2, mine * 8, feat), f32)] * 3
                       + [pltpu.VMEM((group + 1, mine, feat), f32)] * 2
                       + [pltpu.VMEM((mine, group * feat), bf16), pltpu.VMEM((mine, width), bf16), pltpu.VMEM((mine, ff), bf16)]
                       + [pltpu.VMEM((2, CHUNKS, 2, mine, chunk), f32)] + [pltpu.VMEM(chunk_shape, f32)] * 3 + [pltpu.VMEM((2, CHUNKS, 2, mine, chunk), f32)]
                       + [pltpu.VMEM((group, mine, feat), f32)] * 2
                       + [pltpu.SemaphoreType.DMA((6,)), pltpu.SemaphoreType.DMA((7,)), pltpu.SemaphoreType.DMA((loads,)), pltpu.SemaphoreType.DMA((loads,)), pltpu.SemaphoreType.DMA((2 * group,)),
                          pltpu.SemaphoreType.DMA((2, 2, 3, CHUNKS)), pltpu.SemaphoreType.DMA((2, 2))],
        compiler_params=pltpu.CompilerParams(vmem_limit_bytes=53 * 1024 * 1024, collective_id=1, has_side_effects=True),
        cost_estimate=pl.CostEstimate(flops=2 * batch * width * (3 * ff + 3 * qcols), bytes_accessed=50 * 1024 * 1024, transcendentals=batch * 8 * slots),
        name='self_layer',
    )(seq_len, *in_hbm(x, *gains, freqs, keys, values, wq, wk, wv, wo, wg, wu, wd, wqc))


def cross_tail(packed, hidden_in, tile_rows, gates, gain, wo, wg, wu, wd, group):
    mine = hidden_in.shape[1]
    feat = packed.shape[3]
    head_dim = feat // 2
    width, ff = wg.shape
    tiles = tile_rows.shape[0]
    chunk = width // CHUNKS // 2

    def kernel(tile_ref, gate_ref, p_ref, h_ref, gain_hbm, wo_hbm, wg_hbm, wu_hbm, wd_hbm, final,
               gain_ref, wo_ref, wg_ref, wu_ref, wd_ref, on_ref, h3_ref, rx, att_ref, u_ref, act_ref,
               part, from_core, chip, from_chip, total,
               gsem, wsem, osem, red_sems, pair_sems, far_sems):
        row, core, other_core, other_chip, other_row = neighbours()
        barrier = pltpu.get_barrier_semaphore()
        greet(barrier, (other_core, other_chip, other_row))
        c_o = load_projection(wo_hbm, wo_ref, osem, group, head_dim)
        c_gain = pltpu.make_async_copy(gain_hbm, gain_ref, gsem)
        for copy in c_o + [c_gain]:
            copy.start()
        c_w = [pltpu.make_async_copy(src, dst, wsem.at[i]) for i, (src, dst) in enumerate(((wg_hbm, wg_ref), (wu_hbm, wu_ref), (wd_hbm, wd_ref)))]
        for copy in c_w:
            copy.start()
        pl.semaphore_wait(barrier, 3)
        sent = remote(p_ref.at[1 - row], rx, pair_sems, (0,), other_row)
        sent.start()
        for r in range(mine):
            seen = tile_ref[0, row * mine + r]
            for t in range(1, tiles):
                seen = jnp.maximum(seen, tile_ref[t, row * mine + r])
            on_ref[r:r + 1, :] = jnp.full((1, chunk), jnp.where(seen != 0, 1.0, 0.0))
        gate_att = jnp.tanh(jnp.full((1, chunk), gate_ref[0]))
        gate_mlp = jnp.tanh(jnp.full((1, chunk), gate_ref[1]))
        outs, tops, counts = unpack_partial(p_ref.at[row], group)
        sent.wait_recv()
        outs_p, tops_p, counts_p = unpack_partial(rx, group)
        for g in range(group):
            merged = merge(((outs[g], tops[g], counts[g]), (outs_p[g], tops_p[g], counts_p[g])))
            att_ref[:, g * feat:(g + 1) * feat] = merged.astype(jnp.bfloat16)
        for copy in c_o + [c_gain]:
            copy.wait()
        pending = [sent]
        ends = (core, other_core, other_chip)
        pending += all_reduce(chunk_dot(att_ref, wo_ref), part.at[0], from_core.at[0], chip.at[0], from_chip.at[0], total, red_sems.at[0], *ends)
        hidden = [(h_ref[k] + gate_att * on_ref[...] * total[k // 2, k % 2]).astype(jnp.bfloat16).astype(jnp.float32) for k in range(2 * CHUNKS)]
        for k in range(2 * CHUNKS):
            h3_ref[k] = hidden[k]
        u_ref[...] = norm_chunks(hidden, gain_ref)
        c_w[0].wait()
        c_w[1].wait()
        swiglu_hidden(u_ref, wg_ref, wu_ref, act_ref)
        c_w[2].wait()
        first, second = reduce_chips(chunk_dot(act_ref, wd_ref), part.at[1], from_core.at[1], chip.at[1], from_chip.at[1], red_sems.at[1], *ends)
        pending += first + second
        near, far, relay = [], [], []
        for j in range(CHUNKS):
            second[j].wait_recv()
            summed = chip[1, j] + from_chip[1, j]
            place = (pl.ds(pl.multiple_of(row * mine, mine), mine), pl.ds(pl.multiple_of((2 * j + core) * chunk, chunk), chunk))
            final[place] = (h3_ref[2 * j + core] + gate_mlp * on_ref[...] * summed).astype(jnp.bfloat16).astype(jnp.float32)
            piece = final.at[place]
            far.append(remote(piece, piece, far_sems, (0, j), other_row))
            far[j].start()
            near.append(remote(piece, piece, far_sems, (1, j), other_core))
            near[j].start()
        for j in range(CHUNKS):
            far[j].wait_recv()
            place = (pl.ds(pl.multiple_of((1 - row) * mine, mine), mine), pl.ds(pl.multiple_of((2 * j + core) * chunk, chunk), chunk))
            piece = final.at[place]
            relay.append(remote(piece, piece, far_sems, (2, j), other_core))
            relay[j].start()
        for j in range(CHUNKS):
            near[j].wait_recv()
        for j in range(CHUNKS):
            relay[j].wait_recv()
        for copy in pending + near + far + relay:
            copy.wait_send()

    bf16, f32 = jnp.bfloat16, jnp.float32
    chunk_shape = (2, CHUNKS, mine, chunk)
    return pl.pallas_call(
        kernel,
        out_shape=jax.ShapeDtypeStruct((2 * mine, width), f32),
        in_specs=[SMEM, SMEM] + [VMEM] * 2 + [ANY] * 5,
        out_specs=VMEM,
        scratch_shapes=[pltpu.VMEM(gain.shape, bf16), pltpu.VMEM(wo.shape, bf16), pltpu.VMEM(wg.shape, bf16), pltpu.VMEM(wu.shape, bf16), pltpu.VMEM(wd.shape, bf16),
                        pltpu.VMEM((mine, chunk), f32), pltpu.VMEM((2 * CHUNKS, mine, chunk), f32)]
                       + [pltpu.VMEM((group + 1, mine, feat), f32)]
                       + [pltpu.VMEM((mine, group * feat), bf16), pltpu.VMEM((mine, width), bf16), pltpu.VMEM((mine, ff), bf16)]
                       + [pltpu.VMEM((2, CHUNKS, 2, mine, chunk), f32)] + [pltpu.VMEM(chunk_shape, f32)] * 3 + [pltpu.VMEM((CHUNKS, 2, mine, chunk), f32)]
                       + [pltpu.SemaphoreType.DMA, pltpu.SemaphoreType.DMA((3,)), pltpu.SemaphoreType.DMA((2 * group,)),
                          pltpu.SemaphoreType.DMA((2, 2, 3, CHUNKS)), pltpu.SemaphoreType.DMA((2, 1)), pltpu.SemaphoreType.DMA((2, 3, CHUNKS))],
        compiler_params=pltpu.CompilerParams(vmem_limit_bytes=36 * 1024 * 1024, collective_id=2, has_side_effects=True),
        cost_estimate=pl.CostEstimate(flops=4 * mine * width * 3 * ff, bytes_accessed=30 * 1024 * 1024, transcendentals=mine * ff),
        name='cross_tail',
    )(tile_rows, gates, packed, hidden_in, *in_hbm(gain, wo, wg, wu, wd))


def cross_attention(query_bd, keys, values, tile_rows, key_new, val_new):
    rows, feat, tokens = keys.shape
    tiles = tile_rows.shape[0]
    half_rows = rows // 2
    head_dim = feat // 2
    tile_tok = tokens // 2
    base_one = tile_tok // LANES * LANES
    width = tokens - base_one
    width_zero = min(width, -(-tile_tok // LANES) * LANES)

    def kernel(tile_ref, q_ref, kin_ref, vin_ref, k_hbm, v_hbm, p_ref, kn_ref, vn_ref,
               list_ref, o_ref, m_ref, l_ref, s_ref, kbuf, vbuf, ksem, vsem):
        kv_index = lax.axis_index('kv')
        first_tile = kv_index * (tiles // 2)

        def collect(tile, count):
            def add(row, count):
                list_ref[count] = row
                return count + jnp.where(tile_ref[first_tile + tile, row] != 0, 1, 0)

            end = lax.fori_loop(0, rows, add, count, unroll=8)
            list_ref[end] = list_ref[jnp.maximum(end - 1, 0)]
            return end

        def copies(index, is_one, hbm, buf, sem):
            slot = lax.rem(index, SLOTS)
            span = pl.ds(base_one, width) if is_one else pl.ds(0, width_zero)
            dest = pl.ds(0, width) if is_one else pl.ds(0, width_zero)
            return [pltpu.make_async_copy(hbm.at[list_ref[2 * index + half], :, span], buf.at[slot, pl.ds(half * feat, feat), dest], sem.at[slot, half])
                    for half in range(2)]

        key_side, val_side = (k_hbm, kbuf, ksem), (v_hbm, vbuf, vsem)

        def start(index, is_one):
            for copy in copies(index, is_one, *key_side) + copies(index, is_one, *val_side):
                copy.start()

        def wait(index, side):
            @pl.when(index < pairs_zero)
            def _():
                for copy in copies(index, False, *side):
                    copy.wait()

            @pl.when((index >= pairs_zero) & (index < pairs))
            def _():
                for copy in copies(index, True, *side):
                    copy.wait()

        n_zero = collect(0, jnp.int32(0))
        pairs_zero = (n_zero + 1) // 2
        for index in range(SLOTS - 1):
            pl.when(index < pairs_zero)(functools.partial(start, jnp.int32(index), False))
        end_one = collect(1, 2 * pairs_zero)
        pairs = (end_one + 1) // 2
        for index in range(SLOTS - 1):
            pl.when((index >= pairs_zero) & (index < pairs))(functools.partial(start, jnp.int32(index), True))
        o_ref[...] = jnp.zeros_like(o_ref)
        l_ref[...] = jnp.zeros_like(l_ref)
        m_ref[...] = jnp.full_like(m_ref, MASK_VALUE)
        for src, dst in ((kin_ref, kn_ref), (vin_ref, vn_ref)):
            dst[...] = jnp.stack([src[:, :head_dim], src[:, head_dim:]], axis=1).astype(jnp.bfloat16)

        def scores_of(index):
            last = jnp.minimum(index, jnp.maximum(pairs - 1, 0))
            q_a, q_b = (q_ref[pl.ds(pl.multiple_of(list_ref[2 * last + half] * 8, 8), 8), :] for half in range(2))
            zero = jnp.zeros_like(q_a)
            q_pair = jnp.concatenate([jnp.concatenate([q_a, zero], axis=1), jnp.concatenate([zero, q_b], axis=1)], axis=0).astype(jnp.bfloat16)
            return jnp.dot(q_pair, kbuf[lax.rem(index, SLOTS)], preferred_element_type=jnp.float32)

        @pl.when(pairs > 0)
        def _():
            wait(jnp.int32(0), key_side)
            s_ref[0] = scores_of(jnp.int32(0))

        def step(index, carry):
            ahead = index + SLOTS - 1
            pl.when(ahead < pairs_zero)(functools.partial(start, ahead, False))
            pl.when((ahead >= pairs_zero) & (ahead < pairs))(functools.partial(start, ahead, True))
            wait(index + 1, key_side)
            wait(index, val_side)
            slot = lax.rem(index, SLOTS)
            is_one = index >= pairs_zero
            low = jnp.where(is_one, tile_tok - base_one, 0)
            high = jnp.where(is_one, width, tile_tok)
            end = jnp.where(is_one, end_one, n_zero)
            high_b = jnp.where(2 * index + 1 == end, 0, high)
            scores = s_ref[lax.rem(index, 2)]
            lane = lax.broadcasted_iota(jnp.int32, scores.shape, 1)
            sub = lax.broadcasted_iota(jnp.int32, scores.shape, 0)
            visible = (lane >= low) & (lane < jnp.where(sub < 8, high, high_b))
            scores = jnp.where(visible, scores, MASK_VALUE)
            top = jnp.max(scores, axis=1, keepdims=True)
            probs = jnp.where(visible, jnp.exp((scores - top) * SCALE), 0.0)
            total = jnp.sum(probs, axis=1, keepdims=True)
            following = scores_of(index + 1)
            lane_v = lax.broadcasted_iota(jnp.int32, (2 * feat, width - width_zero), 1)
            tail = jnp.where(lane_v < jnp.where(is_one, width, 0), vbuf[slot, :, width_zero:], jnp.zeros((), jnp.bfloat16))
            vals = jnp.concatenate([vbuf[slot, :, :width_zero], tail], axis=1)
            out = lax.dot_general(probs.astype(jnp.bfloat16), vals, (((1,), (1,)), ((), ())), preferred_element_type=jnp.float32)
            for half in range(2):
                where = pl.ds(pl.multiple_of(list_ref[2 * index + half] * 8, 8), 8)
                part = out[8 * half:8 * half + 8, feat * half:feat * half + feat]
                top_new = jnp.broadcast_to(top[8 * half:8 * half + 8] * SCALE, (8, feat))
                total_new = jnp.broadcast_to(total[8 * half:8 * half + 8], (8, feat))
                top_old = m_ref[where, :]
                best = jnp.maximum(top_old, top_new)
                w_old = jnp.exp(top_old - best)
                w_new = jnp.exp(top_new - best)
                m_ref[where, :] = best
                l_ref[where, :] = l_ref[where, :] * w_old + total_new * w_new
                o_ref[where, :] = o_ref[where, :] * w_old + part * w_new
            s_ref[lax.rem(index + 1, 2)] = following
            return carry

        lax.fori_loop(0, pairs, step, 0)
        low_half = half_lane((half_rows, feat))
        for half in range(2):
            def groups(ref):
                at = half * half_rows * 8
                return [jnp.where(low_half, ref[pl.ds(at + g, half_rows, stride=8), :], ref[pl.ds(at + 4 + g, half_rows, stride=8), :]) for g in range(4)]

            pack_partial(p_ref.at[half], groups(o_ref), groups(m_ref), groups(l_ref))

    state = pltpu.VMEM((rows * 8, feat), jnp.float32)
    heads = jax.ShapeDtypeStruct((rows, 2, head_dim), jnp.bfloat16)
    return pl.pallas_call(
        kernel,
        out_shape=(jax.ShapeDtypeStruct((2, 5, half_rows, feat), jnp.float32), heads, heads),
        in_specs=[SMEM, VMEM, VMEM, VMEM, ANY, ANY],
        out_specs=(VMEM,) * 3,
        scratch_shapes=[pltpu.SMEM((2 * rows + 8,), jnp.int32), state, state, state,
                        pltpu.VMEM((2, 16, width), jnp.float32),
                        pltpu.VMEM((SLOTS, 2 * feat, width), jnp.bfloat16),
                        pltpu.VMEM((SLOTS, 2 * feat, width), jnp.bfloat16),
                        pltpu.SemaphoreType.DMA((SLOTS, 2)), pltpu.SemaphoreType.DMA((SLOTS, 2))],
        compiler_params=pltpu.CompilerParams(vmem_limit_bytes=24 * 1024 * 1024),
        cost_estimate=pl.CostEstimate(flops=4 * 8 * feat * tokens * rows, bytes_accessed=2 * feat * tokens * rows, transcendentals=8 * tokens * rows),
        name='cross_attention',
    )(tile_rows, query_bd.reshape(rows * 8, feat), key_new, val_new, *in_hbm(keys, values))


def solution(mesh):
    rows_spec = P('dp', None)
    cache_spec = P('dp', 'tp', 'kv', None)
    new_spec = P('dp', 'tp', None)
    col_spec = P(None, 'tp')
    row_spec = P('tp', None)
    vec_spec = P(None)
    in_specs = (rows_spec, cache_spec, cache_spec, P('dp'), cache_spec, cache_spec, rows_spec,
                vec_spec, col_spec, col_spec, col_spec, row_spec, vec_spec, col_spec, col_spec, row_spec,
                vec_spec, col_spec, vec_spec, row_spec, vec_spec, vec_spec, col_spec, col_spec, row_spec)
    out_specs = (rows_spec, new_spec, new_spec)

    def device_step(x, ks_cache, vs_cache, seq_len, kx_cache, vx_cache, tile_vis, attn_norm, wq_self, wk_self, wv_self, wo_self, mlp_norm, wg_self, wu_self, wd_self, xattn_norm, wq_cross, q_norm, wo_cross, cross_gates, xmlp_norm, wg_cross, wu_cross, wd_cross):
        batch, width = x.shape
        kv_local, slots, head_dim = ks_cache.shape[1:]
        feat = kv_local * head_dim
        group = wq_self.shape[1] // feat
        tokens = kx_cache.shape[2]
        freqs = jnp.tile(rope_freqs(head_dim), 2 * feat // head_dim)[None]

        def lane_rows(gain):
            return gain.reshape(-1, LANES)

        def token_minor(cache):
            return jnp.swapaxes(cache, 2, 3).reshape(batch, feat, cache.shape[2])

        key_new, val_new, query_x, h_two = self_layer(
            x, token_minor(ks_cache).reshape(batch * feat, slots), token_minor(vs_cache).reshape(batch * feat, slots), seq_len,
            [lane_rows(attn_norm), lane_rows(mlp_norm), lane_rows(xattn_norm), q_norm[None]], freqs,
            wq_self, wk_self, wv_self, wo_self, wg_self, wu_self, wd_self, wq_cross, group)
        tile_rows = tile_vis.T
        packed, key_new, val_new = cross_attention(query_x, token_minor(kx_cache), token_minor(vx_cache), tile_rows, key_new, val_new)
        h_four = cross_tail(packed, h_two, tile_rows, cross_gates, lane_rows(xmlp_norm), wo_cross, wg_cross, wu_cross, wd_cross, group)
        return h_four.astype(jnp.bfloat16), key_new, val_new

    return jax.shard_map(device_step, mesh=mesh, in_specs=in_specs, out_specs=out_specs, check_vma=False)
```

```python
import functools
import math
import jax
import jax.numpy as jnp
import numpy as np
from jax import lax
from jax.experimental import pallas as pl
from jax.experimental.pallas import tpu as pltpu
from jax.sharding import PartitionSpec as P

NORM_EPS = 1e-5
ROPE_THETA = 500000.0
MASK_VALUE = -1e30
LANES = 128
SLOTS = 7
AHEAD = 2
SCALE = 0.125


def rope_freqs(head_dim):
    freq_list = []
    for index in range(head_dim // 2):
        base_freq = 1.0 / (ROPE_THETA ** (2.0 * index / head_dim))
        wave_len = 2.0 * math.pi / base_freq
        if wave_len < 2048.0:
            freq_list.append(base_freq)
        elif wave_len > 8192.0:
            freq_list.append(base_freq / 8.0)
        else:
            smooth = (8192.0 / wave_len - 1.0) / 3.0
            freq_list.append((1.0 - smooth) * base_freq / 8.0 + smooth * base_freq)
    return np.array(freq_list, dtype=np.float32)


MESH_ID = pl.DeviceIdType.MESH
CHUNKS = 4
LAST_CHUNKS = 4
ANY = pl.BlockSpec(memory_space=pl.ANY)
VMEM = pl.BlockSpec(memory_space=pltpu.VMEM)
SMEM = pl.BlockSpec(memory_space=pltpu.SMEM)
GROUP_ROWS = 8


def in_hbm(*arrays):
    return [pltpu.with_memory_space_constraint(a, pltpu.HBM) for a in arrays]


def neighbours():
    row = lax.axis_index('kv')
    place = lax.axis_index('tp')
    core = lax.rem(place, 2)
    return row, core, {'tp': place + 1 - 2 * core}, {'tp': lax.rem(place + 2, 4)}, {'kv': 1 - row}


def greet(barrier, peers):
    for peer in peers:
        pl.semaphore_signal(barrier, inc=1, device_id=peer, device_id_type=MESH_ID)


def remote(src, dst, sems, index, peer):
    return pltpu.make_async_remote_copy(src_ref=src, dst_ref=dst, send_sem=sems.at[(0,) + index], recv_sem=sems.at[(1,) + index],
                                        device_id=peer, device_id_type=MESH_ID)


def reduce_chips(produce, part, from_core, chip, from_chip, sems, core, other_core, other_chip):
    first, second = [], []
    chunks = part.shape[0]
    for j in range(chunks):
        block = produce(j)
        width = block.shape[1] // 2
        part[j, 0] = block[:, :width]
        part[j, 1] = block[:, width:]
        copy = remote(part.at[j, 1 - core], from_core.at[j], sems, (0, j), other_core)
        copy.start()
        first.append(copy)
    for j in range(chunks):
        first[j].wait_recv()
        chip[j] = part[j, core] + from_core[j]
        copy = remote(chip.at[j], from_chip.at[j], sems, (1, j), other_chip)
        copy.start()
        second.append(copy)
    return first, second


def all_reduce(produce, use, part, from_core, chip, from_chip, total, sems, core, other_core, other_chip):
    first, second = reduce_chips(produce, part, from_core, chip, from_chip, sems, core, other_core, other_chip)
    chunks, width = part.shape[0], part.shape[3]

    def column(j, half):
        return pl.multiple_of((2 * j + half) * width, width)

    third = []
    for j in range(chunks):
        second[j].wait_recv()
        total[j, core] = chip[j] + from_chip[j]
        third.append(remote(total.at[j, core], total.at[j, core], sems, (2, j), other_core))
        third[j].start()
        if j > 0:
            third[j - 1].wait_recv()
            use(column(j - 1, 1 - core), total[j - 1, 1 - core])
        use(column(j, core), total[j, core])
    third[-1].wait_recv()
    use(column(chunks - 1, 1 - core), total[chunks - 1, 1 - core])
    return first + second + third


def lane_row(gain_ref):
    gain = gain_ref[...].astype(jnp.float32)
    return jnp.concatenate([gain[k:k + 1] for k in range(gain.shape[0])], axis=1)


def norm_products(old_at, h_ref, square_ref, gain_ref, pairs):
    square_ref[...] = jnp.zeros_like(square_ref)
    for _, acc in pairs:
        acc[...] = jnp.zeros_like(acc)

    def use(column, summed):
        width = summed.shape[1]
        cols = pl.ds(column, width)
        hidden = (old_at(cols, summed)).astype(jnp.bfloat16).astype(jnp.float32)
        h_ref[:, cols] = hidden
        square_ref[...] += jnp.sum(hidden * hidden, axis=1, keepdims=True)
        scaled = (hidden * gain_ref[:, cols]).astype(jnp.bfloat16)
        for w_ref, acc in pairs:
            block = min(512, acc.shape[1])
            for n in range(0, acc.shape[1], block):
                acc[:, n:n + block] += jnp.dot(scaled, w_ref[cols, n:n + block], preferred_element_type=jnp.float32)

    return use


def norm_scale(square_ref, width):
    return lax.rsqrt(square_ref[:, :1] / width + NORM_EPS)


def swiglu_hidden(inv, gate_ref, upper_ref, act_ref):
    block = 512
    for n in range(0, act_ref.shape[1], block):
        cols = slice(n, n + block)
        act_ref[:, cols] = (jax.nn.silu(gate_ref[:, cols] * inv) * (upper_ref[:, cols] * inv)).astype(jnp.bfloat16)


def chunk_dot(lhs_ref, w_ref, chunks):
    block = w_ref.shape[1] // chunks
    return lambda j: jnp.dot(lhs_ref[...], w_ref[:, j * block:(j + 1) * block], preferred_element_type=jnp.float32)


def half_lane(shape):
    return lax.broadcasted_iota(jnp.int32, shape, 1) < shape[1] // 2


def half_sums(value):
    low = half_lane(value.shape)
    return jnp.where(low, jnp.sum(jnp.where(low, value, 0.0), axis=1, keepdims=True),
                     jnp.sum(jnp.where(low, 0.0, value), axis=1, keepdims=True))


def by_group(columns, group):
    low = half_lane(columns[0].shape)
    out = []
    for g in range(group):
        a, b = columns[g // 2], columns[group // 2 + g // 2]
        if g % 2 == 0:
            out.append(jnp.where(low, a, pltpu.roll(b, b.shape[1] // 2, 1)))
        else:
            out.append(jnp.where(low, pltpu.roll(a, a.shape[1] // 2, 1), b))
    return out


def store_block_diagonal(ref, groups, lead=()):
    rows, lanes = groups[0].shape
    low = half_lane((rows, lanes))
    for g, value in enumerate(groups):
        ref[lead + (pl.ds(g, rows, stride=8), slice(None))] = jnp.where(low, value, 0.0)
        ref[lead + (pl.ds(4 + g, rows, stride=8), slice(None))] = jnp.where(low, 0.0, value)


def load_groups(ref, lead, rows, lanes, group):
    low = half_lane((rows, lanes))
    return [jnp.where(low, ref[lead, pl.ds(g, rows, stride=8), :], ref[lead, pl.ds(4 + g, rows, stride=8), :]) for g in range(group)]


def pack_partial(tx, outs, tops, totals):
    group = len(outs)
    lane = lax.rem(lax.broadcasted_iota(jnp.int32, outs[0].shape, 1), outs[0].shape[1] // 2)
    packed = jnp.zeros_like(outs[0])
    for g in range(group):
        tx[g] = outs[g]
        packed = jnp.where(lane == g, tops[g], packed)
        packed = jnp.where(lane == group + g, totals[g], packed)
    tx[group] = packed


def unpack_partial(rx, group):
    packed = rx[group]
    low = half_lane(packed.shape)
    middle = packed.shape[1] // 2

    def spread(k):
        return jnp.where(low, jnp.broadcast_to(packed[:, k:k + 1], packed.shape), jnp.broadcast_to(packed[:, middle + k:middle + k + 1], packed.shape))

    return [rx[g] for g in range(group)], [spread(g) for g in range(group)], [spread(group + g) for g in range(group)]


def merge(parts):
    best = parts[0][1]
    for _, top, _ in parts[1:]:
        best = jnp.maximum(best, top)
    out, total = 0.0, 0.0
    for value, top, count in parts:
        weight = jnp.exp(top - best)
        out = out + value * weight
        total = total + count * weight
    return out / jnp.where(total > 0, total, 1.0)


def load_projection(w_hbm, w_ref, sems, group, head_dim):
    out = []
    for g in range(group):
        for h in range(2):
            out.append(pltpu.make_async_copy(w_hbm.at[pl.ds((h * group + g) * head_dim, head_dim), :],
                                             w_ref.at[pl.ds((g * 2 + h) * head_dim, head_dim), :], sems.at[g * 2 + h]))
    return out


def self_layer(x, keys, values, seq_len, gains, freqs, wq, wk, wv, wo, wg, wu, wd, wqc, group):
    batch, width = x.shape
    feat = wk.shape[1]
    head_dim = feat // 2
    slots = keys.shape[1]
    mine = batch // 2
    ff = wg.shape[1]
    qcols = wq.shape[1]
    loads = batch // GROUP_ROWS
    chunk = width // CHUNKS // 2

    def kernel(seq_hbm, x_hbm, ga_hbm, gm_hbm, gx_hbm, gq_hbm, f_hbm, k_hbm, v_hbm, wq_hbm, wk_hbm, wv_hbm, wo_hbm, wg_hbm, wu_hbm, wd_hbm, wqc_hbm,
               kn_ref, vn_ref, qx_ref, h_ref,
               seq_ref, x_ref, ga_ref, gm_ref, gx_ref, gq_ref, f_ref, wq_ref, wk_ref, wv_ref, kbuf, vbuf, wo_ref, wg_ref, wu_ref, wd_ref, wqc_ref,
               seqf, qg_ref, q3_ref, o_ref, m_ref, l_ref, tx, rx, att_ref, gm_row, gx_row, square, gate_acc, upper_acc, query_acc, act_ref,
               part, from_core, chip, from_chip, total, qtx, qrx,
               xsem, wsem, ksem, vsem, osem, red_sems, pair_sems):
        row, core, other_core, other_chip, other_row = neighbours()
        barrier = pltpu.get_barrier_semaphore()
        greet(barrier, (other_core, other_chip, other_row))

        small = [pltpu.make_async_copy(src, dst, xsem.at[i]) for i, (src, dst) in enumerate(
            ((seq_hbm, seq_ref), (f_hbm, f_ref), (ga_hbm, ga_ref), (x_hbm, x_ref), (gm_hbm, gm_ref), (gx_hbm, gx_ref), (gq_hbm, gq_ref)))]
        for copy in small:
            copy.start()

        def fetch(src, dst, index):
            copy = pltpu.make_async_copy(src, dst, wsem.at[index])
            copy.start()
            return copy

        c_q, c_k, c_v = fetch(wq_hbm, wq_ref, 0), fetch(wk_hbm, wk_ref, 1), fetch(wv_hbm, wv_ref, 2)

        def cache_copies(index):
            start = lax.rem((1 - row) * mine + index * GROUP_ROWS, batch)
            rows = pl.ds(pl.multiple_of(start * feat, GROUP_ROWS * feat), GROUP_ROWS * feat)
            return (pltpu.make_async_copy(k_hbm.at[rows, :], kbuf.at[rows, :], ksem.at[index]),
                    pltpu.make_async_copy(v_hbm.at[rows, :], vbuf.at[rows, :], vsem.at[index]))

        def start_cache(quarter):
            for index in range(quarter * loads // 4, (quarter + 1) * loads // 4):
                for copy in cache_copies(index):
                    copy.start()

        c_o = load_projection(wo_hbm, wo_ref, osem, group, head_dim)
        c_g, c_u, c_d, c_qc = (pltpu.make_async_copy(src, dst, wsem.at[3 + i]) for i, (src, dst) in enumerate(
            ((wg_hbm, wg_ref), (wu_hbm, wu_ref), (wd_hbm, wd_ref), (wqc_hbm, wqc_ref))))
        start_cache(0)
        for copy in small:
            copy.wait()
        for b in range(batch):
            seqf[b:b + 1, :] = jnp.full((1, feat), seq_ref[b].astype(jnp.float32))
        gm_row[...] = lane_row(gm_ref)
        gx_row[...] = lane_row(gx_ref)
        angles = seqf[...] * f_ref[...]
        lane = lax.rem(lax.broadcasted_iota(jnp.int32, (batch, feat), 1), head_dim)
        first = lane < head_dim // 2
        cos_t = jnp.cos(angles)
        sin_t = jnp.where(first, -jnp.sin(angles), jnp.sin(angles))

        def rope(value):
            partner = jnp.where(first, pltpu.roll(value, feat - head_dim // 2, 1), pltpu.roll(value, head_dim // 2, 1))
            return (value * cos_t + partner * sin_t).astype(jnp.bfloat16).astype(jnp.float32)

        x_float = x_ref[...].astype(jnp.float32)
        inv = lax.rsqrt(jnp.mean(x_float * x_float, axis=1, keepdims=True) + NORM_EPS)
        x_norm = (x_float * inv * lane_row(ga_ref)).astype(jnp.bfloat16)
        c_q.wait()
        start_cache(1)
        query = jnp.dot(x_norm, wq_ref[...], preferred_element_type=jnp.float32)
        groups = by_group([rope(query[:, n * feat:(n + 1) * feat]) for n in range(qcols // feat)], group)
        for g in range(group):
            qg_ref[g] = groups[g]
        store_block_diagonal(q3_ref, groups)
        c_k.wait()
        key_new = rope(jnp.dot(x_norm, wk_ref[...], preferred_element_type=jnp.float32))
        c_v.wait()
        val_new = jnp.dot(x_norm, wv_ref[...], preferred_element_type=jnp.float32).astype(jnp.bfloat16)
        kn_ref[...] = key_new
        vn_ref[...] = val_new.astype(jnp.float32)

        def scores_of(start):
            q_a = q3_ref[pl.ds(pl.multiple_of(start * 8, 16), 8), :]
            q_b = q3_ref[pl.ds(pl.multiple_of(start * 8, 16) + 8, 8), :]
            zero = jnp.zeros_like(q_a)
            q_pair = jnp.concatenate([jnp.concatenate([q_a, zero], axis=1), jnp.concatenate([zero, q_b], axis=1)], axis=0).astype(jnp.bfloat16)
            rows = pl.ds(pl.multiple_of(start * feat, 2 * feat), 2 * feat)
            return jnp.dot(q_pair, kbuf[rows, :], preferred_element_type=jnp.float32)

        def probs_of(scores, start):
            slot = lax.broadcasted_iota(jnp.int32, scores.shape, 1)
            sub = lax.broadcasted_iota(jnp.int32, scores.shape, 0)
            visible = slot < jnp.where(sub < 8, seq_ref[start], seq_ref[start + 1]) - row * slots
            scores = jnp.where(visible, scores, MASK_VALUE)
            top = jnp.max(scores, axis=1, keepdims=True)
            probs = jnp.where(visible, jnp.exp((scores - top) * SCALE), 0.0)
            return probs.astype(jnp.bfloat16), top, jnp.sum(probs, axis=1, keepdims=True)

        def weigh(probs, top, count, phase, start, local):
            rows = pl.ds(pl.multiple_of(start * feat, 2 * feat), 2 * feat)
            out = lax.dot_general(probs, vbuf[rows, :], (((1,), (1,)), ((), ())), preferred_element_type=jnp.float32)
            for half in range(2):
                where = pl.ds(local * 8 + 8 * half, 8)
                o_ref[phase, where, :] = out[8 * half:8 * half + 8, feat * half:feat * half + feat]
                m_ref[phase, where, :] = jnp.broadcast_to(top[8 * half:8 * half + 8] * SCALE, (8, feat))
                l_ref[phase, where, :] = jnp.broadcast_to(count[8 * half:8 * half + 8], (8, feat))

        def attend_quarter(quarter, following):
            for index in range(quarter * loads // 4, (quarter + 1) * loads // 4):
                for copy in cache_copies(index):
                    copy.wait()
            following()
            phase, part_rows = quarter // 2, mine // 2
            start = lax.rem((1 + phase - row) * mine, batch)
            places = [(quarter % 2) * part_rows + 2 * p for p in range(part_rows // 2)]
            scores = [scores_of(start + local) for local in places[:AHEAD]]
            for p, local in enumerate(places):
                soft = probs_of(scores[p], start + local)
                if p + AHEAD < len(places):
                    scores.append(scores_of(start + places[p + AHEAD]))
                weigh(*soft, phase, start + local, local)

        def start_all(*copies):
            for copy in copies:
                copy.start()

        attend_quarter(0, lambda: start_cache(2))
        attend_quarter(1, lambda: start_cache(3))
        pack_partial(tx, *(load_groups(ref, 0, mine, feat, group) for ref in (o_ref, m_ref, l_ref)))
        pl.semaphore_wait(barrier, 3)
        sent = remote(tx, rx, pair_sems, (0,), other_row)
        sent.start()
        attend_quarter(2, lambda: start_all(*c_o, c_g))
        attend_quarter(3, lambda: start_all(c_u))
        start_all(c_d, c_qc)

        own = pl.ds(pl.multiple_of(row * mine, mine), mine)
        key_own, val_own = kn_ref[own, :], vn_ref[own, :]
        outs, tops, counts = (load_groups(ref, 1, mine, feat, group) for ref in (o_ref, m_ref, l_ref))
        new_tops = [half_sums(qg_ref[g, own, :] * key_own) * SCALE for g in range(group)]
        sent.wait_recv()
        outs_p, tops_p, counts_p = unpack_partial(rx, group)
        for g in range(group):
            merged = merge(((outs[g], tops[g], counts[g]), (outs_p[g], tops_p[g], counts_p[g]), (val_own, new_tops[g], 1.0)))
            att_ref[:, g * feat:(g + 1) * feat] = merged.astype(jnp.bfloat16)
        for copy in c_o:
            copy.wait()
        pending = [sent]
        ends = (core, other_core, other_chip)
        c_g.wait()
        c_u.wait()
        use = norm_products(lambda cols, summed: x_ref[own, cols].astype(jnp.float32) + summed, h_ref, square, gm_row, ((wg_ref, gate_acc), (wu_ref, upper_acc)))
        pending += all_reduce(chunk_dot(att_ref, wo_ref, CHUNKS), use, part.at[0], from_core.at[0], chip.at[0], from_chip.at[0], total.at[0], red_sems.at[0], *ends)
        swiglu_hidden(norm_scale(square, width), gate_acc, upper_acc, act_ref)
        c_d.wait()
        c_qc.wait()
        use = norm_products(lambda cols, summed: h_ref[:, cols] + summed, h_ref, square, gx_row, ((wqc_ref, query_acc),))
        pending += all_reduce(chunk_dot(act_ref, wd_ref, CHUNKS), use, part.at[1], from_core.at[1], chip.at[1], from_chip.at[1], total.at[1], red_sems.at[1], *ends)
        query = query_acc[...] * norm_scale(square, width)
        groups = by_group([query[:, n * feat:(n + 1) * feat] for n in range(qcols // feat)], group)
        gain = jnp.concatenate([gq_ref[...].astype(jnp.float32)] * 2, axis=1)
        groups = [(v * lax.rsqrt(half_sums(v * v) / head_dim + NORM_EPS) * gain).astype(jnp.bfloat16).astype(jnp.float32) for v in groups]
        for g in range(group):
            qtx[g] = groups[g]
        sent = remote(qtx, qrx, pair_sems, (1,), other_row)
        sent.start()
        pending.append(sent)
        store_block_diagonal(qx_ref, groups, (row,))
        sent.wait_recv()
        store_block_diagonal(qx_ref, [qrx[g] for g in range(group)], (1 - row,))
        for copy in pending:
            copy.wait_send()

    bf16, f32 = jnp.bfloat16, jnp.float32
    chunk_shape = (2, CHUNKS, mine, chunk)
    return pl.pallas_call(
        kernel,
        out_shape=(jax.ShapeDtypeStruct((batch, feat), f32), jax.ShapeDtypeStruct((batch, feat), f32),
                   jax.ShapeDtypeStruct((2, mine * 8, feat), f32), jax.ShapeDtypeStruct((mine, width), f32)),
        in_specs=[ANY] * 17,
        out_specs=(VMEM,) * 4,
        scratch_shapes=[pltpu.SMEM(seq_len.shape, seq_len.dtype)] + [pltpu.VMEM(a.shape, a.dtype) for a in (x, *gains, freqs)]
                       + [pltpu.VMEM(wq.shape, bf16), pltpu.VMEM(wk.shape, bf16), pltpu.VMEM(wv.shape, bf16),
                        pltpu.VMEM(keys.shape, bf16), pltpu.VMEM(values.shape, bf16), pltpu.VMEM(wo.shape, bf16),
                        pltpu.VMEM(wg.shape, bf16), pltpu.VMEM(wu.shape, bf16), pltpu.VMEM(wd.shape, bf16), pltpu.VMEM(wqc.shape, bf16),
                        pltpu.VMEM((batch, feat), f32), pltpu.VMEM((group, batch, feat), f32),
                        pltpu.VMEM((batch * 8, feat), f32)] + [pltpu.VMEM((2, mine * 8, feat), f32)] * 3
                       + [pltpu.VMEM((group + 1, mine, feat), f32)] * 2
                       + [pltpu.VMEM((mine, group * feat), bf16), pltpu.VMEM((1, width), f32), pltpu.VMEM((1, width), f32), pltpu.VMEM((mine, LANES), f32),
                          pltpu.VMEM((mine, ff), f32), pltpu.VMEM((mine, ff), f32), pltpu.VMEM((mine, qcols), f32), pltpu.VMEM((mine, ff), bf16)]
                       + [pltpu.VMEM((2, CHUNKS, 2, mine, chunk), f32)] + [pltpu.VMEM(chunk_shape, f32)] * 3 + [pltpu.VMEM((2, CHUNKS, 2, mine, chunk), f32)]
                       + [pltpu.VMEM((group, mine, feat), f32)] * 2
                       + [pltpu.SemaphoreType.DMA((7,)), pltpu.SemaphoreType.DMA((7,)), pltpu.SemaphoreType.DMA((loads,)), pltpu.SemaphoreType.DMA((loads,)), pltpu.SemaphoreType.DMA((2 * group,)),
                          pltpu.SemaphoreType.DMA((2, 2, 3, CHUNKS)), pltpu.SemaphoreType.DMA((2, 2))],
        compiler_params=pltpu.CompilerParams(vmem_limit_bytes=53 * 1024 * 1024, collective_id=1, has_side_effects=True),
        cost_estimate=pl.CostEstimate(flops=2 * batch * width * (3 * ff + 3 * qcols), bytes_accessed=50 * 1024 * 1024, transcendentals=batch * 8 * slots),
        name='self_layer',
    )(*in_hbm(seq_len, x, *gains, freqs, keys, values, wq, wk, wv, wo, wg, wu, wd, wqc))


def cross_tail(packed, hidden_in, tile_rows, gates, gain, wo, wg, wu, wd, group):
    mine = hidden_in.shape[0]
    feat = packed.shape[3]
    head_dim = feat // 2
    width, ff = wg.shape
    tiles = tile_rows.shape[0]
    chunk = width // CHUNKS // 2
    last = width // LAST_CHUNKS // 2

    def kernel(tile_hbm, gate_hbm, p_ref, h_ref, gain_hbm, wo_hbm, wg_hbm, wu_hbm, wd_hbm, final,
               tile_ref, gate_ref, gain_ref, wo_ref, wg_ref, wu_ref, wd_ref, on_ref, h3_ref, rx, att_ref, gain_row, square, gate_acc, upper_acc, act_ref,
               part, from_core, chip, from_chip, total, last_part, last_from_core, last_chip, last_from_chip,
               gsem, wsem, osem, red_sems, last_sems, pair_sems, far_sems):
        row, core, other_core, other_chip, other_row = neighbours()
        barrier = pltpu.get_barrier_semaphore()
        greet(barrier, (other_core, other_chip, other_row))
        c_o = load_projection(wo_hbm, wo_ref, osem, group, head_dim)
        small = [pltpu.make_async_copy(src, dst, gsem.at[i]) for i, (src, dst) in enumerate(((tile_hbm, tile_ref), (gate_hbm, gate_ref), (gain_hbm, gain_ref)))]
        for copy in small + c_o:
            copy.start()
        c_w = [pltpu.make_async_copy(src, dst, wsem.at[i]) for i, (src, dst) in enumerate(((wg_hbm, wg_ref), (wu_hbm, wu_ref), (wd_hbm, wd_ref)))]
        for copy in c_w:
            copy.start()
        pl.semaphore_wait(barrier, 3)
        sent = remote(p_ref.at[1 - row], rx, pair_sems, (0,), other_row)
        sent.start()
        for copy in small:
            copy.wait()
        gain_row[...] = lane_row(gain_ref)
        for r in range(mine):
            seen = tile_ref[0, row * mine + r]
            for t in range(1, tiles):
                seen = jnp.maximum(seen, tile_ref[t, row * mine + r])
            on_ref[r:r + 1, :] = jnp.full((1, LANES), jnp.where(seen != 0, 1.0, 0.0))
        gate_att = jnp.tanh(jnp.full((1, LANES), gate_ref[0]))[:, :1]
        gate_mlp = jnp.tanh(jnp.full((1, LANES), gate_ref[1]))[:, :1]
        outs, tops, counts = unpack_partial(p_ref.at[row], group)
        sent.wait_recv()
        outs_p, tops_p, counts_p = unpack_partial(rx, group)
        for g in range(group):
            merged = merge(((outs[g], tops[g], counts[g]), (outs_p[g], tops_p[g], counts_p[g])))
            att_ref[:, g * feat:(g + 1) * feat] = merged.astype(jnp.bfloat16)
        for copy in c_o:
            copy.wait()
        pending = [sent]
        ends = (core, other_core, other_chip)
        c_w[0].wait()
        c_w[1].wait()
        scale_att, scale_mlp = gate_att * on_ref[:, :1], gate_mlp * on_ref[:, :1]
        use = norm_products(lambda cols, summed: h_ref[:, cols] + scale_att * summed, h3_ref, square, gain_row, ((wg_ref, gate_acc), (wu_ref, upper_acc)))
        pending += all_reduce(chunk_dot(att_ref, wo_ref, CHUNKS), use, part, from_core, chip, from_chip, total, red_sems, *ends)
        swiglu_hidden(norm_scale(square, width), gate_acc, upper_acc, act_ref)
        c_w[2].wait()
        first, second = reduce_chips(chunk_dot(act_ref, wd_ref, LAST_CHUNKS), last_part, last_from_core, last_chip, last_from_chip, last_sems, *ends)
        pending += first + second
        near, far, relay = [], [], []
        for j in range(LAST_CHUNKS):
            second[j].wait_recv()
            summed = last_chip[j] + last_from_chip[j]
            cols = pl.ds(pl.multiple_of((2 * j + core) * last, last), last)
            place = (pl.ds(pl.multiple_of(row * mine, mine), mine), cols)
            final[place] = (h3_ref[:, cols] + scale_mlp * summed).astype(jnp.bfloat16).astype(jnp.float32)
            piece = final.at[place]
            far.append(remote(piece, piece, far_sems, (0, j), other_row))
            far[j].start()
            near.append(remote(piece, piece, far_sems, (1, j), other_core))
            near[j].start()
        for j in range(LAST_CHUNKS):
            far[j].wait_recv()
            place = (pl.ds(pl.multiple_of((1 - row) * mine, mine), mine), pl.ds(pl.multiple_of((2 * j + core) * last, last), last))
            piece = final.at[place]
            relay.append(remote(piece, piece, far_sems, (2, j), other_core))
            relay[j].start()
        for j in range(LAST_CHUNKS):
            near[j].wait_recv()
        for j in range(LAST_CHUNKS):
            relay[j].wait_recv()
        for copy in pending + near + far + relay:
            copy.wait_send()

    bf16, f32 = jnp.bfloat16, jnp.float32
    chunk_shape, last_shape = (CHUNKS, mine, chunk), (LAST_CHUNKS, mine, last)
    return pl.pallas_call(
        kernel,
        out_shape=jax.ShapeDtypeStruct((2 * mine, width), f32),
        in_specs=[ANY] * 2 + [VMEM] * 2 + [ANY] * 5,
        out_specs=VMEM,
        scratch_shapes=[pltpu.SMEM(tile_rows.shape, tile_rows.dtype), pltpu.SMEM(gates.shape, gates.dtype), pltpu.VMEM(gain.shape, bf16), pltpu.VMEM(wo.shape, bf16), pltpu.VMEM(wg.shape, bf16), pltpu.VMEM(wu.shape, bf16), pltpu.VMEM(wd.shape, bf16),
                        pltpu.VMEM((mine, LANES), f32), pltpu.VMEM((mine, width), f32)]
                       + [pltpu.VMEM((group + 1, mine, feat), f32)]
                       + [pltpu.VMEM((mine, group * feat), bf16), pltpu.VMEM((1, width), f32), pltpu.VMEM((mine, LANES), f32),
                          pltpu.VMEM((mine, ff), f32), pltpu.VMEM((mine, ff), f32), pltpu.VMEM((mine, ff), bf16)]
                       + [pltpu.VMEM((CHUNKS, 2, mine, chunk), f32)] + [pltpu.VMEM(chunk_shape, f32)] * 3 + [pltpu.VMEM((CHUNKS, 2, mine, chunk), f32)]
                       + [pltpu.VMEM((LAST_CHUNKS, 2, mine, last), f32)] + [pltpu.VMEM(last_shape, f32)] * 3
                       + [pltpu.SemaphoreType.DMA((3,)), pltpu.SemaphoreType.DMA((3,)), pltpu.SemaphoreType.DMA((2 * group,)),
                          pltpu.SemaphoreType.DMA((2, 3, CHUNKS)), pltpu.SemaphoreType.DMA((2, 2, LAST_CHUNKS)), pltpu.SemaphoreType.DMA((2, 1)), pltpu.SemaphoreType.DMA((2, 3, LAST_CHUNKS))],
        compiler_params=pltpu.CompilerParams(vmem_limit_bytes=36 * 1024 * 1024, collective_id=2, has_side_effects=True),
        cost_estimate=pl.CostEstimate(flops=4 * mine * width * 3 * ff, bytes_accessed=30 * 1024 * 1024, transcendentals=mine * ff),
        name='cross_tail',
    )(*in_hbm(tile_rows, gates), packed, hidden_in, *in_hbm(gain, wo, wg, wu, wd))


def cross_attention(query_bd, keys, values, tile_rows, key_new, val_new):
    rows, feat, tokens = keys.shape
    tiles = tile_rows.shape[0]
    half_rows = rows // 2
    head_dim = feat // 2
    tile_tok = tokens // 2
    base_one = tile_tok // LANES * LANES
    width = tokens - base_one
    width_zero = min(width, -(-tile_tok // LANES) * LANES)

    def kernel(tile_hbm, q_ref, kin_ref, vin_ref, k_hbm, v_hbm, p_ref, kn_ref, vn_ref,
               tile_ref, list_ref, o_ref, m_ref, l_ref, s_ref, kbuf, vbuf, tsem, ksem, vsem):
        kv_index = lax.axis_index('kv')
        first_tile = kv_index * (tiles // 2)

        def collect(tile, count):
            def add(row, count):
                list_ref[count] = row
                return count + jnp.where(tile_ref[first_tile + tile, row] != 0, 1, 0)

            end = lax.fori_loop(0, rows, add, count, unroll=8)
            list_ref[end] = list_ref[jnp.maximum(end - 1, 0)]
            return end

        def copies(index, is_one, hbm, buf, sem):
            slot = lax.rem(index, SLOTS)
            span = pl.ds(base_one, width) if is_one else pl.ds(0, width_zero)
            dest = pl.ds(0, width) if is_one else pl.ds(0, width_zero)
            return [pltpu.make_async_copy(hbm.at[list_ref[2 * index + half], :, span], buf.at[slot, pl.ds(half * feat, feat), dest], sem.at[slot, half])
                    for half in range(2)]

        key_side, val_side = (k_hbm, kbuf, ksem), (v_hbm, vbuf, vsem)

        def start(index, is_one):
            for copy in copies(index, is_one, *key_side) + copies(index, is_one, *val_side):
                copy.start()

        def wait(index, side):
            @pl.when(index < pairs_zero)
            def _():
                for copy in copies(index, False, *side):
                    copy.wait()

            @pl.when((index >= pairs_zero) & (index < pairs))
            def _():
                for copy in copies(index, True, *side):
                    copy.wait()

        tile_copy = pltpu.make_async_copy(tile_hbm, tile_ref, tsem)
        tile_copy.start()
        tile_copy.wait()
        n_zero = collect(0, jnp.int32(0))
        pairs_zero = (n_zero + 1) // 2
        for index in range(SLOTS - 1):
            pl.when(index < pairs_zero)(functools.partial(start, jnp.int32(index), False))
        end_one = collect(1, 2 * pairs_zero)
        pairs = (end_one + 1) // 2
        for index in range(SLOTS - 1):
            pl.when((index >= pairs_zero) & (index < pairs))(functools.partial(start, jnp.int32(index), True))
        o_ref[...] = jnp.zeros_like(o_ref)
        l_ref[...] = jnp.zeros_like(l_ref)
        m_ref[...] = jnp.full_like(m_ref, MASK_VALUE)
        for src, dst in ((kin_ref, kn_ref), (vin_ref, vn_ref)):
            dst[...] = jnp.stack([src[:, :head_dim], src[:, head_dim:]], axis=1).astype(jnp.bfloat16)

        def scores_of(index):
            last = jnp.minimum(index, jnp.maximum(pairs - 1, 0))
            q_a, q_b = (q_ref[pl.ds(pl.multiple_of(list_ref[2 * last + half] * 8, 8), 8), :] for half in range(2))
            zero = jnp.zeros_like(q_a)
            q_pair = jnp.concatenate([jnp.concatenate([q_a, zero], axis=1), jnp.concatenate([zero, q_b], axis=1)], axis=0).astype(jnp.bfloat16)
            return jnp.dot(q_pair, kbuf[lax.rem(index, SLOTS)], preferred_element_type=jnp.float32)

        @pl.when(pairs > 0)
        def _():
            wait(jnp.int32(0), key_side)
            s_ref[0] = scores_of(jnp.int32(0))

        def step(index, carry):
            ahead = index + SLOTS - 1
            pl.when(ahead < pairs_zero)(functools.partial(start, ahead, False))
            pl.when((ahead >= pairs_zero) & (ahead < pairs))(functools.partial(start, ahead, True))
            wait(index + 1, key_side)
            wait(index, val_side)
            slot = lax.rem(index, SLOTS)
            is_one = index >= pairs_zero
            low = jnp.where(is_one, tile_tok - base_one, 0)
            high = jnp.where(is_one, width, tile_tok)
            end = jnp.where(is_one, end_one, n_zero)
            high_b = jnp.where(2 * index + 1 == end, 0, high)
            scores = s_ref[lax.rem(index, 2)]
            lane = lax.broadcasted_iota(jnp.int32, scores.shape, 1)
            sub = lax.broadcasted_iota(jnp.int32, scores.shape, 0)
            visible = (lane >= low) & (lane < jnp.where(sub < 8, high, high_b))
            scores = jnp.where(visible, scores, MASK_VALUE)
            top = jnp.max(scores, axis=1, keepdims=True)
            probs = jnp.where(visible, jnp.exp((scores - top) * SCALE), 0.0)
            total = jnp.sum(probs, axis=1, keepdims=True)
            following = scores_of(index + 1)
            lane_v = lax.broadcasted_iota(jnp.int32, (2 * feat, width - width_zero), 1)
            tail = jnp.where(lane_v < jnp.where(is_one, width, 0), vbuf[slot, :, width_zero:], jnp.zeros((), jnp.bfloat16))
            vals = jnp.concatenate([vbuf[slot, :, :width_zero], tail], axis=1)
            out = lax.dot_general(probs.astype(jnp.bfloat16), vals, (((1,), (1,)), ((), ())), preferred_element_type=jnp.float32)
            for half in range(2):
                where = pl.ds(pl.multiple_of(list_ref[2 * index + half] * 8, 8), 8)
                part = out[8 * half:8 * half + 8, feat * half:feat * half + feat]
                top_new = jnp.broadcast_to(top[8 * half:8 * half + 8] * SCALE, (8, feat))
                total_new = jnp.broadcast_to(total[8 * half:8 * half + 8], (8, feat))
                top_old = m_ref[where, :]
                best = jnp.maximum(top_old, top_new)
                w_old = jnp.exp(top_old - best)
                w_new = jnp.exp(top_new - best)
                m_ref[where, :] = best
                l_ref[where, :] = l_ref[where, :] * w_old + total_new * w_new
                o_ref[where, :] = o_ref[where, :] * w_old + part * w_new
            s_ref[lax.rem(index + 1, 2)] = following
            return carry

        lax.fori_loop(0, pairs, step, 0)
        low_half = half_lane((half_rows, feat))
        for half in range(2):
            def groups(ref):
                at = half * half_rows * 8
                return [jnp.where(low_half, ref[pl.ds(at + g, half_rows, stride=8), :], ref[pl.ds(at + 4 + g, half_rows, stride=8), :]) for g in range(4)]

            pack_partial(p_ref.at[half], groups(o_ref), groups(m_ref), groups(l_ref))

    state = pltpu.VMEM((rows * 8, feat), jnp.float32)
    heads = jax.ShapeDtypeStruct((rows, 2, head_dim), jnp.bfloat16)
    return pl.pallas_call(
        kernel,
        out_shape=(jax.ShapeDtypeStruct((2, 5, half_rows, feat), jnp.float32), heads, heads),
        in_specs=[ANY, VMEM, VMEM, VMEM, ANY, ANY],
        out_specs=(VMEM,) * 3,
        scratch_shapes=[pltpu.SMEM(tile_rows.shape, jnp.int32), pltpu.SMEM((2 * rows + 8,), jnp.int32), state, state, state,
                        pltpu.VMEM((2, 16, width), jnp.float32),
                        pltpu.VMEM((SLOTS, 2 * feat, width), jnp.bfloat16),
                        pltpu.VMEM((SLOTS, 2 * feat, width), jnp.bfloat16),
                        pltpu.SemaphoreType.DMA, pltpu.SemaphoreType.DMA((SLOTS, 2)), pltpu.SemaphoreType.DMA((SLOTS, 2))],
        compiler_params=pltpu.CompilerParams(vmem_limit_bytes=30 * 1024 * 1024),
        cost_estimate=pl.CostEstimate(flops=4 * 8 * feat * tokens * rows, bytes_accessed=2 * feat * tokens * rows, transcendentals=8 * tokens * rows),
        name='cross_attention',
    )(*in_hbm(tile_rows), query_bd.reshape(rows * 8, feat), key_new, val_new, *in_hbm(keys, values))


def solution(mesh):
    rows_spec = P('dp', None)
    cache_spec = P('dp', 'tp', 'kv', None)
    new_spec = P('dp', 'tp', None)
    col_spec = P(None, 'tp')
    row_spec = P('tp', None)
    vec_spec = P(None)
    in_specs = (rows_spec, cache_spec, cache_spec, P('dp'), cache_spec, cache_spec, rows_spec,
                vec_spec, col_spec, col_spec, col_spec, row_spec, vec_spec, col_spec, col_spec, row_spec,
                vec_spec, col_spec, vec_spec, row_spec, vec_spec, vec_spec, col_spec, col_spec, row_spec)
    out_specs = (rows_spec, new_spec, new_spec)

    def device_step(x, ks_cache, vs_cache, seq_len, kx_cache, vx_cache, tile_vis, attn_norm, wq_self, wk_self, wv_self, wo_self, mlp_norm, wg_self, wu_self, wd_self, xattn_norm, wq_cross, q_norm, wo_cross, cross_gates, xmlp_norm, wg_cross, wu_cross, wd_cross):
        batch, width = x.shape
        kv_local, slots, head_dim = ks_cache.shape[1:]
        feat = kv_local * head_dim
        group = wq_self.shape[1] // feat
        tokens = kx_cache.shape[2]
        freqs = jnp.asarray(np.tile(rope_freqs(head_dim), 2 * feat // head_dim)[None])

        def lane_rows(gain):
            return gain.reshape(-1, LANES)

        def token_minor(cache):
            return jnp.swapaxes(cache, 2, 3).reshape(batch, feat, cache.shape[2])

        key_new, val_new, query_x, h_two = self_layer(
            x, token_minor(ks_cache).reshape(batch * feat, slots), token_minor(vs_cache).reshape(batch * feat, slots), seq_len,
            [lane_rows(attn_norm), lane_rows(mlp_norm), lane_rows(xattn_norm), q_norm[None]], freqs,
            wq_self, wk_self, wv_self, wo_self, wg_self, wu_self, wd_self, wq_cross, group)
        tile_rows = tile_vis.T
        packed, key_new, val_new = cross_attention(query_x, token_minor(kx_cache), token_minor(vx_cache), tile_rows, key_new, val_new)
        h_four = cross_tail(packed, h_two, tile_rows, cross_gates, lane_rows(xmlp_norm), wo_cross, wg_cross, wu_cross, wd_cross, group)
        return h_four.astype(jnp.bfloat16), key_new, val_new

    return jax.shard_map(device_step, mesh=mesh, in_specs=in_specs, out_specs=out_specs, check_vma=False)
```

```python
import functools
import math
import jax
import jax.numpy as jnp
import numpy as np
from jax import lax
from jax.experimental import pallas as pl
from jax.experimental.pallas import tpu as pltpu
from jax.sharding import PartitionSpec as P

NORM_EPS = 1e-5
ROPE_THETA = 500000.0
MASK_VALUE = -1e30
LANES = 128
SLOTS = 7
AHEAD = 2
SCALE = 0.125


def rope_freqs(head_dim):
    freq_list = []
    for index in range(head_dim // 2):
        base_freq = 1.0 / (ROPE_THETA ** (2.0 * index / head_dim))
        wave_len = 2.0 * math.pi / base_freq
        if wave_len < 2048.0:
            freq_list.append(base_freq)
        elif wave_len > 8192.0:
            freq_list.append(base_freq / 8.0)
        else:
            smooth = (8192.0 / wave_len - 1.0) / 3.0
            freq_list.append((1.0 - smooth) * base_freq / 8.0 + smooth * base_freq)
    return np.array(freq_list, dtype=np.float32)


MESH_ID = pl.DeviceIdType.MESH
CHUNKS = 4
LAST_CHUNKS = 4
ANY = pl.BlockSpec(memory_space=pl.ANY)
VMEM = pl.BlockSpec(memory_space=pltpu.VMEM)
SMEM = pl.BlockSpec(memory_space=pltpu.SMEM)
GROUP_ROWS = 8


def in_hbm(*arrays):
    return [pltpu.with_memory_space_constraint(a, pltpu.HBM) for a in arrays]


def neighbours():
    row = lax.axis_index('kv')
    place = lax.axis_index('tp')
    core = lax.rem(place, 2)
    return row, core, {'tp': place + 1 - 2 * core}, {'tp': lax.rem(place + 2, 4)}, {'kv': 1 - row}


def greet(barrier, peers):
    for peer in peers:
        pl.semaphore_signal(barrier, inc=1, device_id=peer, device_id_type=MESH_ID)


def remote(src, dst, sems, index, peer):
    return pltpu.make_async_remote_copy(src_ref=src, dst_ref=dst, send_sem=sems.at[(0,) + index], recv_sem=sems.at[(1,) + index],
                                        device_id=peer, device_id_type=MESH_ID)


def reduce_chips(produce, part, from_core, chip, from_chip, sems, core, other_core, other_chip):
    first, second = [], []
    chunks = part.shape[0]
    for j in range(chunks):
        block = produce(j)
        width = block.shape[1] // 2
        part[j, 0] = block[:, :width]
        part[j, 1] = block[:, width:]
        copy = remote(part.at[j, 1 - core], from_core.at[j], sems, (0, j), other_core)
        copy.start()
        first.append(copy)
    for j in range(chunks):
        first[j].wait_recv()
        chip[j] = part[j, core] + from_core[j]
        copy = remote(chip.at[j], from_chip.at[j], sems, (1, j), other_chip)
        copy.start()
        second.append(copy)
    return first, second


def all_reduce(produce, use, part, from_core, chip, from_chip, total, sems, core, other_core, other_chip):
    first, second = reduce_chips(produce, part, from_core, chip, from_chip, sems, core, other_core, other_chip)
    chunks, width = part.shape[0], part.shape[3]

    def column(j, half):
        return pl.multiple_of((2 * j + half) * width, width)

    third = []
    for j in range(chunks):
        second[j].wait_recv()
        total[j, core] = chip[j] + from_chip[j]
        third.append(remote(total.at[j, core], total.at[j, core], sems, (2, j), other_core))
        third[j].start()
        if j > 0:
            third[j - 1].wait_recv()
            use(column(j - 1, 1 - core), total[j - 1, 1 - core])
        use(column(j, core), total[j, core])
    third[-1].wait_recv()
    use(column(chunks - 1, 1 - core), total[chunks - 1, 1 - core])
    return first + second + third


def lane_row(gain_ref):
    gain = gain_ref[...].astype(jnp.float32)
    return jnp.concatenate([gain[k:k + 1] for k in range(gain.shape[0])], axis=1)


def norm_products(old_at, h_ref, square_ref, gain_ref, pairs, ready):
    square_ref[...] = jnp.zeros_like(square_ref)
    for _, acc in pairs:
        acc[...] = jnp.zeros_like(acc)
    waits = [ready]

    def use(column, summed):
        width = summed.shape[1]
        cols = pl.ds(column, width)
        hidden = (old_at(cols, summed)).astype(jnp.bfloat16).astype(jnp.float32)
        h_ref[:, cols] = hidden
        square_ref[...] += jnp.sum(hidden * hidden, axis=1, keepdims=True)
        scaled = (hidden * gain_ref[:, cols]).astype(jnp.bfloat16)
        if waits:
            waits.pop()()
        for w_ref, acc in pairs:
            block = min(512, acc.shape[1])
            for n in range(0, acc.shape[1], block):
                acc[:, n:n + block] += jnp.dot(scaled, w_ref[cols, n:n + block], preferred_element_type=jnp.float32)

    return use


def norm_scale(square_ref, width):
    return lax.rsqrt(square_ref[:, :1] / width + NORM_EPS)


def swiglu_hidden(inv, gate_ref, upper_ref, act_ref):
    block = 512
    for n in range(0, act_ref.shape[1], block):
        cols = slice(n, n + block)
        act_ref[:, cols] = (jax.nn.silu(gate_ref[:, cols] * inv) * (upper_ref[:, cols] * inv)).astype(jnp.bfloat16)


def chunk_dot(lhs_ref, w_ref, chunks):
    block = w_ref.shape[1] // chunks
    return lambda j: jnp.dot(lhs_ref[...], w_ref[:, j * block:(j + 1) * block], preferred_element_type=jnp.float32)


def half_lane(shape):
    return lax.broadcasted_iota(jnp.int32, shape, 1) < shape[1] // 2


def half_sums(value):
    low = half_lane(value.shape)
    return jnp.where(low, jnp.sum(jnp.where(low, value, 0.0), axis=1, keepdims=True),
                     jnp.sum(jnp.where(low, 0.0, value), axis=1, keepdims=True))


def by_group(columns, group):
    low = half_lane(columns[0].shape)
    out = []
    for g in range(group):
        a, b = columns[g // 2], columns[group // 2 + g // 2]
        if g % 2 == 0:
            out.append(jnp.where(low, a, pltpu.roll(b, b.shape[1] // 2, 1)))
        else:
            out.append(jnp.where(low, pltpu.roll(a, a.shape[1] // 2, 1), b))
    return out


def store_block_diagonal(ref, groups, lead=()):
    rows, lanes = groups[0].shape
    low = half_lane((rows, lanes))
    for g, value in enumerate(groups):
        ref[lead + (pl.ds(g, rows, stride=8), slice(None))] = jnp.where(low, value, 0.0)
        ref[lead + (pl.ds(4 + g, rows, stride=8), slice(None))] = jnp.where(low, 0.0, value)


def load_groups(ref, lead, rows, lanes, group):
    low = half_lane((rows, lanes))
    return [jnp.where(low, ref[lead, pl.ds(g, rows, stride=8), :], ref[lead, pl.ds(4 + g, rows, stride=8), :]) for g in range(group)]


def pack_partial(tx, outs, tops, totals):
    group = len(outs)
    lane = lax.rem(lax.broadcasted_iota(jnp.int32, outs[0].shape, 1), outs[0].shape[1] // 2)
    packed = jnp.zeros_like(outs[0])
    for g in range(group):
        tx[g] = outs[g]
        packed = jnp.where(lane == g, tops[g], packed)
        packed = jnp.where(lane == group + g, totals[g], packed)
    tx[group] = packed


def unpack_partial(rx, group):
    packed = rx[group]
    low = half_lane(packed.shape)
    middle = packed.shape[1] // 2

    def spread(k):
        return jnp.where(low, jnp.broadcast_to(packed[:, k:k + 1], packed.shape), jnp.broadcast_to(packed[:, middle + k:middle + k + 1], packed.shape))

    return [rx[g] for g in range(group)], [spread(g) for g in range(group)], [spread(group + g) for g in range(group)]


def merge(parts):
    best = parts[0][1]
    for _, top, _ in parts[1:]:
        best = jnp.maximum(best, top)
    out, total = 0.0, 0.0
    for value, top, count in parts:
        weight = jnp.exp(top - best)
        out = out + value * weight
        total = total + count * weight
    return out / jnp.where(total > 0, total, 1.0)


def load_projection(w_hbm, w_ref, sems, group, head_dim):
    out = []
    for g in range(group):
        for h in range(2):
            out.append(pltpu.make_async_copy(w_hbm.at[pl.ds((h * group + g) * head_dim, head_dim), :],
                                             w_ref.at[pl.ds((g * 2 + h) * head_dim, head_dim), :], sems.at[g * 2 + h]))
    return out


def self_layer(x, keys, values, seq_len, gains, freqs, wq, wk, wv, wo, wg, wu, wd, wqc, group):
    batch, width = x.shape
    feat = wk.shape[1]
    head_dim = feat // 2
    slots = keys.shape[1]
    mine = batch // 2
    ff = wg.shape[1]
    qcols = wq.shape[1]
    loads = batch // GROUP_ROWS
    chunk = width // CHUNKS // 2

    def kernel(seq_hbm, x_hbm, ga_hbm, gm_hbm, gx_hbm, gq_hbm, f_hbm, k_hbm, v_hbm, wq_hbm, wk_hbm, wv_hbm, wo_hbm, wg_hbm, wu_hbm, wd_hbm, wqc_hbm,
               kn_ref, vn_ref, qx_ref, h_ref,
               seq_ref, x_ref, ga_ref, gm_ref, gx_ref, gq_ref, f_ref, wq_ref, wk_ref, wv_ref, kbuf, vbuf, wo_ref, wg_ref, wu_ref, wd_ref, wqc_ref,
               seqf, qg_ref, q3_ref, o_ref, m_ref, l_ref, tx, rx, att_ref, gm_row, gx_row, square, gate_acc, upper_acc, query_acc, act_ref,
               part, from_core, chip, from_chip, total, qtx, qrx,
               xsem, wsem, ksem, vsem, osem, red_sems, pair_sems):
        row, core, other_core, other_chip, other_row = neighbours()
        barrier = pltpu.get_barrier_semaphore()
        greet(barrier, (other_core, other_chip, other_row))

        small = [pltpu.make_async_copy(src, dst, xsem.at[i]) for i, (src, dst) in enumerate(
            ((seq_hbm, seq_ref), (f_hbm, f_ref), (ga_hbm, ga_ref), (x_hbm, x_ref), (gm_hbm, gm_ref), (gx_hbm, gx_ref), (gq_hbm, gq_ref)))]
        for copy in small:
            copy.start()

        def fetch(src, dst, index):
            copy = pltpu.make_async_copy(src, dst, wsem.at[index])
            copy.start()
            return copy

        c_q, c_k, c_v = fetch(wq_hbm, wq_ref, 0), fetch(wk_hbm, wk_ref, 1), fetch(wv_hbm, wv_ref, 2)

        def cache_copies(index):
            start = lax.rem((1 - row) * mine + index * GROUP_ROWS, batch)
            rows = pl.ds(pl.multiple_of(start * feat, GROUP_ROWS * feat), GROUP_ROWS * feat)
            return (pltpu.make_async_copy(k_hbm.at[rows, :], kbuf.at[rows, :], ksem.at[index]),
                    pltpu.make_async_copy(v_hbm.at[rows, :], vbuf.at[rows, :], vsem.at[index]))

        def start_cache(quarter):
            for index in range(quarter * loads // 4, (quarter + 1) * loads // 4):
                for copy in cache_copies(index):
                    copy.start()

        c_o = load_projection(wo_hbm, wo_ref, osem, group, head_dim)
        c_g, c_u, c_d, c_qc = (pltpu.make_async_copy(src, dst, wsem.at[3 + i]) for i, (src, dst) in enumerate(
            ((wg_hbm, wg_ref), (wu_hbm, wu_ref), (wd_hbm, wd_ref), (wqc_hbm, wqc_ref))))
        start_cache(0)
        for copy in small:
            copy.wait()
        for b in range(batch):
            seqf[b:b + 1, :] = jnp.full((1, feat), seq_ref[b].astype(jnp.float32))
        gm_row[...] = lane_row(gm_ref)
        gx_row[...] = lane_row(gx_ref)
        angles = seqf[...] * f_ref[...]
        lane = lax.rem(lax.broadcasted_iota(jnp.int32, (batch, feat), 1), head_dim)
        first = lane < head_dim // 2
        cos_t = jnp.cos(angles)
        sin_t = jnp.where(first, -jnp.sin(angles), jnp.sin(angles))

        def rope(value):
            partner = jnp.where(first, pltpu.roll(value, feat - head_dim // 2, 1), pltpu.roll(value, head_dim // 2, 1))
            return (value * cos_t + partner * sin_t).astype(jnp.bfloat16).astype(jnp.float32)

        x_float = x_ref[...].astype(jnp.float32)
        inv = lax.rsqrt(jnp.mean(x_float * x_float, axis=1, keepdims=True) + NORM_EPS)
        x_norm = (x_float * inv * lane_row(ga_ref)).astype(jnp.bfloat16)
        c_q.wait()
        start_cache(1)
        query = jnp.dot(x_norm, wq_ref[...], preferred_element_type=jnp.float32)
        groups = by_group([rope(query[:, n * feat:(n + 1) * feat]) for n in range(qcols // feat)], group)
        for g in range(group):
            qg_ref[g] = groups[g]
        store_block_diagonal(q3_ref, groups)
        c_k.wait()
        key_new = rope(jnp.dot(x_norm, wk_ref[...], preferred_element_type=jnp.float32))
        c_v.wait()
        val_new = jnp.dot(x_norm, wv_ref[...], preferred_element_type=jnp.float32).astype(jnp.bfloat16)
        kn_ref[...] = key_new
        vn_ref[...] = val_new.astype(jnp.float32)

        def scores_of(start):
            q_a = q3_ref[pl.ds(pl.multiple_of(start * 8, 16), 8), :]
            q_b = q3_ref[pl.ds(pl.multiple_of(start * 8, 16) + 8, 8), :]
            zero = jnp.zeros_like(q_a)
            q_pair = jnp.concatenate([jnp.concatenate([q_a, zero], axis=1), jnp.concatenate([zero, q_b], axis=1)], axis=0).astype(jnp.bfloat16)
            rows = pl.ds(pl.multiple_of(start * feat, 2 * feat), 2 * feat)
            return jnp.dot(q_pair, kbuf[rows, :], preferred_element_type=jnp.float32)

        def probs_of(scores, start):
            slot = lax.broadcasted_iota(jnp.int32, scores.shape, 1)
            sub = lax.broadcasted_iota(jnp.int32, scores.shape, 0)
            visible = slot < jnp.where(sub < 8, seq_ref[start], seq_ref[start + 1]) - row * slots
            scores = jnp.where(visible, scores, MASK_VALUE)
            top = jnp.max(scores, axis=1, keepdims=True)
            probs = jnp.where(visible, jnp.exp((scores - top) * SCALE), 0.0)
            return probs.astype(jnp.bfloat16), top, jnp.sum(probs, axis=1, keepdims=True)

        def weigh(probs, top, count, phase, start, local):
            rows = pl.ds(pl.multiple_of(start * feat, 2 * feat), 2 * feat)
            out = lax.dot_general(probs, vbuf[rows, :], (((1,), (1,)), ((), ())), preferred_element_type=jnp.float32)
            for half in range(2):
                where = pl.ds(local * 8 + 8 * half, 8)
                o_ref[phase, where, :] = out[8 * half:8 * half + 8, feat * half:feat * half + feat]
                m_ref[phase, where, :] = jnp.broadcast_to(top[8 * half:8 * half + 8] * SCALE, (8, feat))
                l_ref[phase, where, :] = jnp.broadcast_to(count[8 * half:8 * half + 8], (8, feat))

        def attend_quarter(quarter, following):
            for index in range(quarter * loads // 4, (quarter + 1) * loads // 4):
                for copy in cache_copies(index):
                    copy.wait()
            following()
            phase, part_rows = quarter // 2, mine // 2
            start = lax.rem((1 + phase - row) * mine, batch)
            places = [(quarter % 2) * part_rows + 2 * p for p in range(part_rows // 2)]
            scores = [scores_of(start + local) for local in places[:AHEAD]]
            for p, local in enumerate(places):
                soft = probs_of(scores[p], start + local)
                if p + AHEAD < len(places):
                    scores.append(scores_of(start + places[p + AHEAD]))
                weigh(*soft, phase, start + local, local)

        def start_all(*copies):
            for copy in copies:
                copy.start()

        attend_quarter(0, lambda: start_cache(2))
        attend_quarter(1, lambda: start_cache(3))
        pack_partial(tx, *(load_groups(ref, 0, mine, feat, group) for ref in (o_ref, m_ref, l_ref)))
        pl.semaphore_wait(barrier, 3)
        sent = remote(tx, rx, pair_sems, (0,), other_row)
        sent.start()
        attend_quarter(2, lambda: start_all(*c_o, c_g))
        attend_quarter(3, lambda: start_all(c_u))

        own = pl.ds(pl.multiple_of(row * mine, mine), mine)
        key_own, val_own = kn_ref[own, :], vn_ref[own, :]
        outs, tops, counts = (load_groups(ref, 1, mine, feat, group) for ref in (o_ref, m_ref, l_ref))
        new_tops = [half_sums(qg_ref[g, own, :] * key_own) * SCALE for g in range(group)]
        sent.wait_recv()
        outs_p, tops_p, counts_p = unpack_partial(rx, group)
        for g in range(group):
            merged = merge(((outs[g], tops[g], counts[g]), (outs_p[g], tops_p[g], counts_p[g]), (val_own, new_tops[g], 1.0)))
            att_ref[:, g * feat:(g + 1) * feat] = merged.astype(jnp.bfloat16)
        for copy in c_o:
            copy.wait()
        pending = [sent]
        ends = (core, other_core, other_chip)

        def weights_ready():
            c_g.wait()
            c_u.wait()
            start_all(c_d, c_qc)

        use = norm_products(lambda cols, summed: x_ref[own, cols].astype(jnp.float32) + summed, h_ref, square, gm_row, ((wg_ref, gate_acc), (wu_ref, upper_acc)), weights_ready)
        pending += all_reduce(chunk_dot(att_ref, wo_ref, CHUNKS), use, part.at[0], from_core.at[0], chip.at[0], from_chip.at[0], total.at[0], red_sems.at[0], *ends)
        swiglu_hidden(norm_scale(square, width), gate_acc, upper_acc, act_ref)
        c_d.wait()
        use = norm_products(lambda cols, summed: h_ref[:, cols] + summed, h_ref, square, gx_row, ((wqc_ref, query_acc),), c_qc.wait)
        pending += all_reduce(chunk_dot(act_ref, wd_ref, CHUNKS), use, part.at[1], from_core.at[1], chip.at[1], from_chip.at[1], total.at[1], red_sems.at[1], *ends)
        query = query_acc[...] * norm_scale(square, width)
        groups = by_group([query[:, n * feat:(n + 1) * feat] for n in range(qcols // feat)], group)
        gain = jnp.concatenate([gq_ref[...].astype(jnp.float32)] * 2, axis=1)
        groups = [(v * lax.rsqrt(half_sums(v * v) / head_dim + NORM_EPS) * gain).astype(jnp.bfloat16).astype(jnp.float32) for v in groups]
        for g in range(group):
            qtx[g] = groups[g]
        sent = remote(qtx, qrx, pair_sems, (1,), other_row)
        sent.start()
        pending.append(sent)
        store_block_diagonal(qx_ref, groups, (row,))
        sent.wait_recv()
        store_block_diagonal(qx_ref, [qrx[g] for g in range(group)], (1 - row,))
        for copy in pending:
            copy.wait_send()

    bf16, f32 = jnp.bfloat16, jnp.float32
    chunk_shape = (2, CHUNKS, mine, chunk)
    return pl.pallas_call(
        kernel,
        out_shape=(jax.ShapeDtypeStruct((batch, feat), f32), jax.ShapeDtypeStruct((batch, feat), f32),
                   jax.ShapeDtypeStruct((2, mine * 8, feat), f32), jax.ShapeDtypeStruct((mine, width), f32)),
        in_specs=[ANY] * 17,
        out_specs=(VMEM,) * 4,
        scratch_shapes=[pltpu.SMEM(seq_len.shape, seq_len.dtype)] + [pltpu.VMEM(a.shape, a.dtype) for a in (x, *gains, freqs)]
                       + [pltpu.VMEM(wq.shape, bf16), pltpu.VMEM(wk.shape, bf16), pltpu.VMEM(wv.shape, bf16),
                        pltpu.VMEM(keys.shape, bf16), pltpu.VMEM(values.shape, bf16), pltpu.VMEM(wo.shape, bf16),
                        pltpu.VMEM(wg.shape, bf16), pltpu.VMEM(wu.shape, bf16), pltpu.VMEM(wd.shape, bf16), pltpu.VMEM(wqc.shape, bf16),
                        pltpu.VMEM((batch, feat), f32), pltpu.VMEM((group, batch, feat), f32),
                        pltpu.VMEM((batch * 8, feat), f32)] + [pltpu.VMEM((2, mine * 8, feat), f32)] * 3
                       + [pltpu.VMEM((group + 1, mine, feat), f32)] * 2
                       + [pltpu.VMEM((mine, group * feat), bf16), pltpu.VMEM((1, width), f32), pltpu.VMEM((1, width), f32), pltpu.VMEM((mine, LANES), f32),
                          pltpu.VMEM((mine, ff), f32), pltpu.VMEM((mine, ff), f32), pltpu.VMEM((mine, qcols), f32), pltpu.VMEM((mine, ff), bf16)]
                       + [pltpu.VMEM((2, CHUNKS, 2, mine, chunk), f32)] + [pltpu.VMEM(chunk_shape, f32)] * 3 + [pltpu.VMEM((2, CHUNKS, 2, mine, chunk), f32)]
                       + [pltpu.VMEM((group, mine, feat), f32)] * 2
                       + [pltpu.SemaphoreType.DMA((7,)), pltpu.SemaphoreType.DMA((7,)), pltpu.SemaphoreType.DMA((loads,)), pltpu.SemaphoreType.DMA((loads,)), pltpu.SemaphoreType.DMA((2 * group,)),
                          pltpu.SemaphoreType.DMA((2, 2, 3, CHUNKS)), pltpu.SemaphoreType.DMA((2, 2))],
        compiler_params=pltpu.CompilerParams(vmem_limit_bytes=53 * 1024 * 1024, collective_id=1, has_side_effects=True),
        cost_estimate=pl.CostEstimate(flops=2 * batch * width * (3 * ff + 3 * qcols), bytes_accessed=50 * 1024 * 1024, transcendentals=batch * 8 * slots),
        name='self_layer',
    )(*in_hbm(seq_len, x, *gains, freqs, keys, values, wq, wk, wv, wo, wg, wu, wd, wqc))


def cross_tail(packed, hidden_in, tile_rows, gates, gain, wo, wg, wu, wd, group):
    mine = hidden_in.shape[0]
    feat = packed.shape[3]
    head_dim = feat // 2
    width, ff = wg.shape
    tiles = tile_rows.shape[0]
    chunk = width // CHUNKS // 2
    last = width // LAST_CHUNKS // 2

    def kernel(tile_hbm, gate_hbm, p_ref, h_ref, gain_hbm, wo_hbm, wg_hbm, wu_hbm, wd_hbm, final,
               tile_ref, gate_ref, gain_ref, wo_ref, wg_ref, wu_ref, wd_ref, on_ref, h3_ref, rx, att_ref, gain_row, square, gate_acc, upper_acc, act_ref,
               part, from_core, chip, from_chip, total, last_part, last_from_core, last_chip, last_from_chip,
               gsem, wsem, osem, red_sems, last_sems, pair_sems, far_sems):
        row, core, other_core, other_chip, other_row = neighbours()
        barrier = pltpu.get_barrier_semaphore()
        greet(barrier, (other_core, other_chip, other_row))
        c_o = load_projection(wo_hbm, wo_ref, osem, group, head_dim)
        small = [pltpu.make_async_copy(src, dst, gsem.at[i]) for i, (src, dst) in enumerate(((tile_hbm, tile_ref), (gate_hbm, gate_ref), (gain_hbm, gain_ref)))]
        for copy in small + c_o:
            copy.start()
        c_w = [pltpu.make_async_copy(src, dst, wsem.at[i]) for i, (src, dst) in enumerate(((wg_hbm, wg_ref), (wu_hbm, wu_ref), (wd_hbm, wd_ref)))]
        for copy in c_w[:2]:
            copy.start()
        pl.semaphore_wait(barrier, 3)
        sent = remote(p_ref.at[1 - row], rx, pair_sems, (0,), other_row)
        sent.start()
        for copy in small:
            copy.wait()
        gain_row[...] = lane_row(gain_ref)
        for r in range(mine):
            seen = tile_ref[0, row * mine + r]
            for t in range(1, tiles):
                seen = jnp.maximum(seen, tile_ref[t, row * mine + r])
            on_ref[r:r + 1, :] = jnp.full((1, LANES), jnp.where(seen != 0, 1.0, 0.0))
        gate_att = jnp.tanh(jnp.full((1, LANES), gate_ref[0]))[:, :1]
        gate_mlp = jnp.tanh(jnp.full((1, LANES), gate_ref[1]))[:, :1]
        outs, tops, counts = unpack_partial(p_ref.at[row], group)
        sent.wait_recv()
        outs_p, tops_p, counts_p = unpack_partial(rx, group)
        for g in range(group):
            merged = merge(((outs[g], tops[g], counts[g]), (outs_p[g], tops_p[g], counts_p[g])))
            att_ref[:, g * feat:(g + 1) * feat] = merged.astype(jnp.bfloat16)
        for copy in c_o:
            copy.wait()
        pending = [sent]
        ends = (core, other_core, other_chip)
        scale_att, scale_mlp = gate_att * on_ref[:, :1], gate_mlp * on_ref[:, :1]

        def weights_ready():
            c_w[0].wait()
            c_w[1].wait()
            c_w[2].start()

        use = norm_products(lambda cols, summed: h_ref[:, cols] + scale_att * summed, h3_ref, square, gain_row, ((wg_ref, gate_acc), (wu_ref, upper_acc)), weights_ready)
        pending += all_reduce(chunk_dot(att_ref, wo_ref, CHUNKS), use, part, from_core, chip, from_chip, total, red_sems, *ends)
        swiglu_hidden(norm_scale(square, width), gate_acc, upper_acc, act_ref)
        c_w[2].wait()
        first, second = reduce_chips(chunk_dot(act_ref, wd_ref, LAST_CHUNKS), last_part, last_from_core, last_chip, last_from_chip, last_sems, *ends)
        pending += first + second
        near, far, relay = [], [], []
        for j in range(LAST_CHUNKS):
            second[j].wait_recv()
            summed = last_chip[j] + last_from_chip[j]
            cols = pl.ds(pl.multiple_of((2 * j + core) * last, last), last)
            place = (pl.ds(pl.multiple_of(row * mine, mine), mine), cols)
            final[place] = (h3_ref[:, cols] + scale_mlp * summed).astype(jnp.bfloat16).astype(jnp.float32)
            piece = final.at[place]
            far.append(remote(piece, piece, far_sems, (0, j), other_row))
            far[j].start()
            near.append(remote(piece, piece, far_sems, (1, j), other_core))
            near[j].start()
        for j in range(LAST_CHUNKS):
            far[j].wait_recv()
            place = (pl.ds(pl.multiple_of((1 - row) * mine, mine), mine), pl.ds(pl.multiple_of((2 * j + core) * last, last), last))
            piece = final.at[place]
            relay.append(remote(piece, piece, far_sems, (2, j), other_core))
            relay[j].start()
        for j in range(LAST_CHUNKS):
            near[j].wait_recv()
        for j in range(LAST_CHUNKS):
            relay[j].wait_recv()
        for copy in pending + near + far + relay:
            copy.wait_send()

    bf16, f32 = jnp.bfloat16, jnp.float32
    chunk_shape, last_shape = (CHUNKS, mine, chunk), (LAST_CHUNKS, mine, last)
    return pl.pallas_call(
        kernel,
        out_shape=jax.ShapeDtypeStruct((2 * mine, width), f32),
        in_specs=[ANY] * 2 + [VMEM] * 2 + [ANY] * 5,
        out_specs=VMEM,
        scratch_shapes=[pltpu.SMEM(tile_rows.shape, tile_rows.dtype), pltpu.SMEM(gates.shape, gates.dtype), pltpu.VMEM(gain.shape, bf16), pltpu.VMEM(wo.shape, bf16), pltpu.VMEM(wg.shape, bf16), pltpu.VMEM(wu.shape, bf16), pltpu.VMEM(wd.shape, bf16),
                        pltpu.VMEM((mine, LANES), f32), pltpu.VMEM((mine, width), f32)]
                       + [pltpu.VMEM((group + 1, mine, feat), f32)]
                       + [pltpu.VMEM((mine, group * feat), bf16), pltpu.VMEM((1, width), f32), pltpu.VMEM((mine, LANES), f32),
                          pltpu.VMEM((mine, ff), f32), pltpu.VMEM((mine, ff), f32), pltpu.VMEM((mine, ff), bf16)]
                       + [pltpu.VMEM((CHUNKS, 2, mine, chunk), f32)] + [pltpu.VMEM(chunk_shape, f32)] * 3 + [pltpu.VMEM((CHUNKS, 2, mine, chunk), f32)]
                       + [pltpu.VMEM((LAST_CHUNKS, 2, mine, last), f32)] + [pltpu.VMEM(last_shape, f32)] * 3
                       + [pltpu.SemaphoreType.DMA((3,)), pltpu.SemaphoreType.DMA((3,)), pltpu.SemaphoreType.DMA((2 * group,)),
                          pltpu.SemaphoreType.DMA((2, 3, CHUNKS)), pltpu.SemaphoreType.DMA((2, 2, LAST_CHUNKS)), pltpu.SemaphoreType.DMA((2, 1)), pltpu.SemaphoreType.DMA((2, 3, LAST_CHUNKS))],
        compiler_params=pltpu.CompilerParams(vmem_limit_bytes=36 * 1024 * 1024, collective_id=2, has_side_effects=True),
        cost_estimate=pl.CostEstimate(flops=4 * mine * width * 3 * ff, bytes_accessed=30 * 1024 * 1024, transcendentals=mine * ff),
        name='cross_tail',
    )(*in_hbm(tile_rows, gates), packed, hidden_in, *in_hbm(gain, wo, wg, wu, wd))


def cross_attention(query_bd, keys, values, tile_rows, key_new, val_new):
    rows, feat, tokens = keys.shape
    tiles = tile_rows.shape[0]
    half_rows = rows // 2
    head_dim = feat // 2
    tile_tok = tokens // 2
    base_one = tile_tok // LANES * LANES
    width = tokens - base_one
    width_zero = min(width, -(-tile_tok // LANES) * LANES)

    def kernel(tile_hbm, q_ref, kin_ref, vin_ref, k_hbm, v_hbm, p_ref, kn_ref, vn_ref,
               tile_ref, list_ref, o_ref, m_ref, l_ref, s_ref, kbuf, vbuf, tsem, ksem, vsem):
        kv_index = lax.axis_index('kv')
        first_tile = kv_index * (tiles // 2)

        def collect(tile, count):
            def add(row, count):
                list_ref[count] = row
                return count + jnp.where(tile_ref[first_tile + tile, row] != 0, 1, 0)

            end = lax.fori_loop(0, rows, add, count, unroll=8)
            list_ref[end] = list_ref[jnp.maximum(end - 1, 0)]
            return end

        def copies(index, is_one, hbm, buf, sem):
            slot = lax.rem(index, SLOTS)
            span = pl.ds(base_one, width) if is_one else pl.ds(0, width_zero)
            dest = pl.ds(0, width) if is_one else pl.ds(0, width_zero)
            return [pltpu.make_async_copy(hbm.at[list_ref[2 * index + half], :, span], buf.at[slot, pl.ds(half * feat, feat), dest], sem.at[slot, half])
                    for half in range(2)]

        key_side, val_side = (k_hbm, kbuf, ksem), (v_hbm, vbuf, vsem)

        def start(index, is_one):
            for copy in copies(index, is_one, *key_side) + copies(index, is_one, *val_side):
                copy.start()

        def wait(index, side):
            @pl.when(index < pairs_zero)
            def _():
                for copy in copies(index, False, *side):
                    copy.wait()

            @pl.when((index >= pairs_zero) & (index < pairs))
            def _():
                for copy in copies(index, True, *side):
                    copy.wait()

        tile_copy = pltpu.make_async_copy(tile_hbm, tile_ref, tsem)
        tile_copy.start()
        tile_copy.wait()
        n_zero = collect(0, jnp.int32(0))
        pairs_zero = (n_zero + 1) // 2
        for index in range(SLOTS - 1):
            pl.when(index < pairs_zero)(functools.partial(start, jnp.int32(index), False))
        end_one = collect(1, 2 * pairs_zero)
        pairs = (end_one + 1) // 2
        for index in range(SLOTS - 1):
            pl.when((index >= pairs_zero) & (index < pairs))(functools.partial(start, jnp.int32(index), True))
        o_ref[...] = jnp.zeros_like(o_ref)
        l_ref[...] = jnp.zeros_like(l_ref)
        m_ref[...] = jnp.full_like(m_ref, MASK_VALUE)
        for src, dst in ((kin_ref, kn_ref), (vin_ref, vn_ref)):
            dst[...] = jnp.stack([src[:, :head_dim], src[:, head_dim:]], axis=1).astype(jnp.bfloat16)

        def scores_of(index):
            last = jnp.minimum(index, jnp.maximum(pairs - 1, 0))
            q_a, q_b = (q_ref[pl.ds(pl.multiple_of(list_ref[2 * last + half] * 8, 8), 8), :] for half in range(2))
            zero = jnp.zeros_like(q_a)
            q_pair = jnp.concatenate([jnp.concatenate([q_a, zero], axis=1), jnp.concatenate([zero, q_b], axis=1)], axis=0).astype(jnp.bfloat16)
            return jnp.dot(q_pair, kbuf[lax.rem(index, SLOTS)], preferred_element_type=jnp.float32)

        @pl.when(pairs > 0)
        def _():
            wait(jnp.int32(0), key_side)
            s_ref[0] = scores_of(jnp.int32(0))

        def step(index, carry):
            ahead = index + SLOTS - 1
            pl.when(ahead < pairs_zero)(functools.partial(start, ahead, False))
            pl.when((ahead >= pairs_zero) & (ahead < pairs))(functools.partial(start, ahead, True))
            wait(index + 1, key_side)
            wait(index, val_side)
            slot = lax.rem(index, SLOTS)
            is_one = index >= pairs_zero
            low = jnp.where(is_one, tile_tok - base_one, 0)
            high = jnp.where(is_one, width, tile_tok)
            end = jnp.where(is_one, end_one, n_zero)
            high_b = jnp.where(2 * index + 1 == end, 0, high)
            scores = s_ref[lax.rem(index, 2)]
            lane = lax.broadcasted_iota(jnp.int32, scores.shape, 1)
            sub = lax.broadcasted_iota(jnp.int32, scores.shape, 0)
            visible = (lane >= low) & (lane < jnp.where(sub < 8, high, high_b))
            scores = jnp.where(visible, scores, MASK_VALUE)
            top = jnp.max(scores, axis=1, keepdims=True)
            probs = jnp.where(visible, jnp.exp((scores - top) * SCALE), 0.0)
            total = jnp.sum(probs, axis=1, keepdims=True)
            following = scores_of(index + 1)
            lane_v = lax.broadcasted_iota(jnp.int32, (2 * feat, width - width_zero), 1)
            tail = jnp.where(lane_v < jnp.where(is_one, width, 0), vbuf[slot, :, width_zero:], jnp.zeros((), jnp.bfloat16))
            vals = jnp.concatenate([vbuf[slot, :, :width_zero], tail], axis=1)
            out = lax.dot_general(probs.astype(jnp.bfloat16), vals, (((1,), (1,)), ((), ())), preferred_element_type=jnp.float32)
            for half in range(2):
                where = pl.ds(pl.multiple_of(list_ref[2 * index + half] * 8, 8), 8)
                part = out[8 * half:8 * half + 8, feat * half:feat * half + feat]
                top_new = jnp.broadcast_to(top[8 * half:8 * half + 8] * SCALE, (8, feat))
                total_new = jnp.broadcast_to(total[8 * half:8 * half + 8], (8, feat))
                top_old = m_ref[where, :]
                best = jnp.maximum(top_old, top_new)
                w_old = jnp.exp(top_old - best)
                w_new = jnp.exp(top_new - best)
                m_ref[where, :] = best
                l_ref[where, :] = l_ref[where, :] * w_old + total_new * w_new
                o_ref[where, :] = o_ref[where, :] * w_old + part * w_new
            s_ref[lax.rem(index + 1, 2)] = following
            return carry

        lax.fori_loop(0, pairs, step, 0)
        low_half = half_lane((half_rows, feat))
        for half in range(2):
            def groups(ref):
                at = half * half_rows * 8
                return [jnp.where(low_half, ref[pl.ds(at + g, half_rows, stride=8), :], ref[pl.ds(at + 4 + g, half_rows, stride=8), :]) for g in range(4)]

            pack_partial(p_ref.at[half], groups(o_ref), groups(m_ref), groups(l_ref))

    state = pltpu.VMEM((rows * 8, feat), jnp.float32)
    heads = jax.ShapeDtypeStruct((rows, 2, head_dim), jnp.bfloat16)
    return pl.pallas_call(
        kernel,
        out_shape=(jax.ShapeDtypeStruct((2, 5, half_rows, feat), jnp.float32), heads, heads),
        in_specs=[ANY, VMEM, VMEM, VMEM, ANY, ANY],
        out_specs=(VMEM,) * 3,
        scratch_shapes=[pltpu.SMEM(tile_rows.shape, jnp.int32), pltpu.SMEM((2 * rows + 8,), jnp.int32), state, state, state,
                        pltpu.VMEM((2, 16, width), jnp.float32),
                        pltpu.VMEM((SLOTS, 2 * feat, width), jnp.bfloat16),
                        pltpu.VMEM((SLOTS, 2 * feat, width), jnp.bfloat16),
                        pltpu.SemaphoreType.DMA, pltpu.SemaphoreType.DMA((SLOTS, 2)), pltpu.SemaphoreType.DMA((SLOTS, 2))],
        compiler_params=pltpu.CompilerParams(vmem_limit_bytes=30 * 1024 * 1024),
        cost_estimate=pl.CostEstimate(flops=4 * 8 * feat * tokens * rows, bytes_accessed=2 * feat * tokens * rows, transcendentals=8 * tokens * rows),
        name='cross_attention',
    )(*in_hbm(tile_rows), query_bd.reshape(rows * 8, feat), key_new, val_new, *in_hbm(keys, values))


def solution(mesh):
    rows_spec = P('dp', None)
    cache_spec = P('dp', 'tp', 'kv', None)
    new_spec = P('dp', 'tp', None)
    col_spec = P(None, 'tp')
    row_spec = P('tp', None)
    vec_spec = P(None)
    in_specs = (rows_spec, cache_spec, cache_spec, P('dp'), cache_spec, cache_spec, rows_spec,
                vec_spec, col_spec, col_spec, col_spec, row_spec, vec_spec, col_spec, col_spec, row_spec,
                vec_spec, col_spec, vec_spec, row_spec, vec_spec, vec_spec, col_spec, col_spec, row_spec)
    out_specs = (rows_spec, new_spec, new_spec)

    def device_step(x, ks_cache, vs_cache, seq_len, kx_cache, vx_cache, tile_vis, attn_norm, wq_self, wk_self, wv_self, wo_self, mlp_norm, wg_self, wu_self, wd_self, xattn_norm, wq_cross, q_norm, wo_cross, cross_gates, xmlp_norm, wg_cross, wu_cross, wd_cross):
        batch, width = x.shape
        kv_local, slots, head_dim = ks_cache.shape[1:]
        feat = kv_local * head_dim
        group = wq_self.shape[1] // feat
        tokens = kx_cache.shape[2]
        freqs = jnp.asarray(np.tile(rope_freqs(head_dim), 2 * feat // head_dim)[None])

        def lane_rows(gain):
            return gain.reshape(-1, LANES)

        def token_minor(cache):
            return jnp.swapaxes(cache, 2, 3).reshape(batch, feat, cache.shape[2])

        key_new, val_new, query_x, h_two = self_layer(
            x, token_minor(ks_cache).reshape(batch * feat, slots), token_minor(vs_cache).reshape(batch * feat, slots), seq_len,
            [lane_rows(attn_norm), lane_rows(mlp_norm), lane_rows(xattn_norm), q_norm[None]], freqs,
            wq_self, wk_self, wv_self, wo_self, wg_self, wu_self, wd_self, wq_cross, group)
        tile_rows = tile_vis.T
        packed, key_new, val_new = cross_attention(query_x, token_minor(kx_cache), token_minor(vx_cache), tile_rows, key_new, val_new)
        h_four = cross_tail(packed, h_two, tile_rows, cross_gates, lane_rows(xmlp_norm), wo_cross, wg_cross, wu_cross, wd_cross, group)
        return h_four.astype(jnp.bfloat16), key_new, val_new

    return jax.shard_map(device_step, mesh=mesh, in_specs=in_specs, out_specs=out_specs, check_vma=False)
```

```python
import functools
import math
import jax
import jax.numpy as jnp
import numpy as np
from jax import lax
from jax.experimental import pallas as pl
from jax.experimental.pallas import tpu as pltpu
from jax.sharding import PartitionSpec as P

NORM_EPS = 1e-5
ROPE_THETA = 500000.0
MASK_VALUE = -1e30
LANES = 128
SLOTS = 7
AHEAD = 2
SCALE = 0.125


def rope_freqs(head_dim):
    freq_list = []
    for index in range(head_dim // 2):
        base_freq = 1.0 / (ROPE_THETA ** (2.0 * index / head_dim))
        wave_len = 2.0 * math.pi / base_freq
        if wave_len < 2048.0:
            freq_list.append(base_freq)
        elif wave_len > 8192.0:
            freq_list.append(base_freq / 8.0)
        else:
            smooth = (8192.0 / wave_len - 1.0) / 3.0
            freq_list.append((1.0 - smooth) * base_freq / 8.0 + smooth * base_freq)
    return np.array(freq_list, dtype=np.float32)


MESH_ID = pl.DeviceIdType.MESH
CHUNKS = 4
LAST_CHUNKS = 4
ANY = pl.BlockSpec(memory_space=pl.ANY)
VMEM = pl.BlockSpec(memory_space=pltpu.VMEM)
SMEM = pl.BlockSpec(memory_space=pltpu.SMEM)
GROUP_ROWS = 8


def in_hbm(*arrays):
    return [pltpu.with_memory_space_constraint(a, pltpu.HBM) for a in arrays]


def neighbours():
    row = lax.axis_index('kv')
    place = lax.axis_index('tp')
    core = lax.rem(place, 2)
    return row, core, {'tp': place + 1 - 2 * core}, {'tp': lax.rem(place + 2, 4)}, {'kv': 1 - row}


def greet(barrier, peers):
    for peer in peers:
        pl.semaphore_signal(barrier, inc=1, device_id=peer, device_id_type=MESH_ID)


def remote(src, dst, sems, index, peer):
    return pltpu.make_async_remote_copy(src_ref=src, dst_ref=dst, send_sem=sems.at[(0,) + index], recv_sem=sems.at[(1,) + index],
                                        device_id=peer, device_id_type=MESH_ID)


def reduce_chips(produce, part, from_core, chip, from_chip, sems, core, other_core, other_chip):
    first, second = [], []
    chunks = part.shape[0]
    for j in range(chunks):
        block = produce(j)
        width = block.shape[1] // 2
        part[j, 0] = block[:, :width]
        part[j, 1] = block[:, width:]
        copy = remote(part.at[j, 1 - core], from_core.at[j], sems, (0, j), other_core)
        copy.start()
        first.append(copy)
    for j in range(chunks):
        first[j].wait_recv()
        chip[j] = part[j, core] + from_core[j]
        copy = remote(chip.at[j], from_chip.at[j], sems, (1, j), other_chip)
        copy.start()
        second.append(copy)
    return first, second


def all_reduce(produce, use, part, from_core, chip, from_chip, total, sems, core, other_core, other_chip):
    first, second = reduce_chips(produce, part, from_core, chip, from_chip, sems, core, other_core, other_chip)
    chunks, width = part.shape[0], part.shape[3]

    def column(j, half):
        return pl.multiple_of((2 * j + half) * width, width)

    third = []
    for j in range(chunks):
        second[j].wait_recv()
        total[j, core] = chip[j] + from_chip[j]
        third.append(remote(total.at[j, core], total.at[j, core], sems, (2, j), other_core))
        third[j].start()
        if j > 0:
            third[j - 1].wait_recv()
            use(column(j - 1, 1 - core), total[j - 1, 1 - core])
        use(column(j, core), total[j, core])
    third[-1].wait_recv()
    use(column(chunks - 1, 1 - core), total[chunks - 1, 1 - core])
    return first + second + third


def lane_row(gain_ref):
    gain = gain_ref[...].astype(jnp.float32)
    return jnp.concatenate([gain[k:k + 1] for k in range(gain.shape[0])], axis=1)


def norm_products(old_at, h_ref, square_ref, gain_ref, pairs, ready):
    square_ref[...] = jnp.zeros_like(square_ref)
    for _, acc in pairs:
        acc[...] = jnp.zeros_like(acc)
    waits = [ready]

    def use(column, summed):
        width = summed.shape[1]
        cols = pl.ds(column, width)
        hidden = (old_at(cols, summed)).astype(jnp.bfloat16).astype(jnp.float32)
        h_ref[:, cols] = hidden
        square_ref[...] += jnp.sum(hidden * hidden, axis=1, keepdims=True)
        scaled = (hidden * gain_ref[:, cols]).astype(jnp.bfloat16)
        if waits:
            waits.pop()()
        for w_ref, acc in pairs:
            block = min(512, acc.shape[1])
            for n in range(0, acc.shape[1], block):
                acc[:, n:n + block] += jnp.dot(scaled, w_ref[cols, n:n + block], preferred_element_type=jnp.float32)

    return use


def norm_scale(square_ref, width):
    return lax.rsqrt(square_ref[:, :1] / width + NORM_EPS)


def swiglu_hidden(inv, gate_ref, upper_ref, act_ref):
    block = 512
    for n in range(0, act_ref.shape[1], block):
        cols = slice(n, n + block)
        act_ref[:, cols] = (jax.nn.silu(gate_ref[:, cols] * inv) * (upper_ref[:, cols] * inv)).astype(jnp.bfloat16)


def chunk_dot(lhs_ref, w_ref, chunks):
    block = w_ref.shape[1] // chunks
    return lambda j: jnp.dot(lhs_ref[...], w_ref[:, j * block:(j + 1) * block], preferred_element_type=jnp.float32)


def half_lane(shape):
    return lax.broadcasted_iota(jnp.int32, shape, 1) < shape[1] // 2


def half_sums(value):
    low = half_lane(value.shape)
    return jnp.where(low, jnp.sum(jnp.where(low, value, 0.0), axis=1, keepdims=True),
                     jnp.sum(jnp.where(low, 0.0, value), axis=1, keepdims=True))


def by_group(columns, group):
    low = half_lane(columns[0].shape)
    out = []
    for g in range(group):
        a, b = columns[g // 2], columns[group // 2 + g // 2]
        if g % 2 == 0:
            out.append(jnp.where(low, a, pltpu.roll(b, b.shape[1] // 2, 1)))
        else:
            out.append(jnp.where(low, pltpu.roll(a, a.shape[1] // 2, 1), b))
    return out


def store_block_diagonal(ref, groups, lead=()):
    rows, lanes = groups[0].shape
    low = half_lane((rows, lanes))
    for g, value in enumerate(groups):
        ref[lead + (pl.ds(g, rows, stride=8), slice(None))] = jnp.where(low, value, 0.0)
        ref[lead + (pl.ds(4 + g, rows, stride=8), slice(None))] = jnp.where(low, 0.0, value)


def load_groups(ref, lead, start, rows, lanes, group):
    low = half_lane((rows, lanes))
    return [jnp.where(low, ref[lead, pl.ds(start + g, rows, stride=8), :], ref[lead, pl.ds(start + 4 + g, rows, stride=8), :]) for g in range(group)]


def pack_partial(tx, outs, tops, totals):
    group = len(outs)
    lane = lax.rem(lax.broadcasted_iota(jnp.int32, outs[0].shape, 1), outs[0].shape[1] // 2)
    packed = jnp.zeros_like(outs[0])
    for g in range(group):
        tx[g] = outs[g]
        packed = jnp.where(lane == g, tops[g], packed)
        packed = jnp.where(lane == group + g, totals[g], packed)
    tx[group] = packed


def unpack_partial(rx, group):
    packed = rx[group]
    low = half_lane(packed.shape)
    middle = packed.shape[1] // 2

    def spread(k):
        return jnp.where(low, jnp.broadcast_to(packed[:, k:k + 1], packed.shape), jnp.broadcast_to(packed[:, middle + k:middle + k + 1], packed.shape))

    return [rx[g] for g in range(group)], [spread(g) for g in range(group)], [spread(group + g) for g in range(group)]


def merge(parts):
    best = parts[0][1]
    for _, top, _ in parts[1:]:
        best = jnp.maximum(best, top)
    out, total = 0.0, 0.0
    for value, top, count in parts:
        weight = jnp.exp(top - best)
        out = out + value * weight
        total = total + count * weight
    return out / jnp.where(total > 0, total, 1.0)


def load_projection(w_hbm, w_ref, sems, group, head_dim):
    out = []
    for g in range(group):
        for h in range(2):
            out.append(pltpu.make_async_copy(w_hbm.at[pl.ds((h * group + g) * head_dim, head_dim), :],
                                             w_ref.at[pl.ds((g * 2 + h) * head_dim, head_dim), :], sems.at[g * 2 + h]))
    return out


def self_layer(x, keys, values, seq_len, gains, freqs, wq, wk, wv, wo, wg, wu, wd, wqc, group):
    batch, width = x.shape
    feat = wk.shape[1]
    head_dim = feat // 2
    slots = keys.shape[1]
    mine = batch // 2
    ff = wg.shape[1]
    qcols = wq.shape[1]
    loads = batch // GROUP_ROWS
    chunk = width // CHUNKS // 2

    def kernel(seq_hbm, x_hbm, ga_hbm, gm_hbm, gx_hbm, gq_hbm, f_hbm, k_hbm, v_hbm, wq_hbm, wk_hbm, wv_hbm, wo_hbm, wg_hbm, wu_hbm, wd_hbm, wqc_hbm,
               kn_ref, vn_ref, qx_ref, h_ref,
               seq_ref, x_ref, ga_ref, gm_ref, gx_ref, gq_ref, f_ref, wq_ref, wk_ref, wv_ref, kbuf, vbuf, wo_ref, wg_ref, wu_ref, wd_ref, wqc_ref,
               seqf, qg_ref, q3_ref, o_ref, m_ref, l_ref, tx, rx, att_ref, gm_row, gx_row, square, gate_acc, upper_acc, query_acc, act_ref,
               part, from_core, chip, from_chip, total, qtx, qrx,
               xsem, wsem, ksem, vsem, osem, red_sems, pair_sems):
        row, core, other_core, other_chip, other_row = neighbours()
        barrier = pltpu.get_barrier_semaphore()
        greet(barrier, (other_core, other_chip, other_row))

        small = [pltpu.make_async_copy(src, dst, xsem.at[i]) for i, (src, dst) in enumerate(
            ((seq_hbm, seq_ref), (f_hbm, f_ref), (ga_hbm, ga_ref), (x_hbm, x_ref), (gm_hbm, gm_ref), (gx_hbm, gx_ref), (gq_hbm, gq_ref)))]
        for copy in small:
            copy.start()

        def fetch(src, dst, index):
            copy = pltpu.make_async_copy(src, dst, wsem.at[index])
            copy.start()
            return copy

        c_q, c_k, c_v = fetch(wq_hbm, wq_ref, 0), fetch(wk_hbm, wk_ref, 1), fetch(wv_hbm, wv_ref, 2)

        def cache_copies(index):
            start = lax.rem((1 - row) * mine + index * GROUP_ROWS, batch)
            rows = pl.ds(pl.multiple_of(start * feat, GROUP_ROWS * feat), GROUP_ROWS * feat)
            return (pltpu.make_async_copy(k_hbm.at[rows, :], kbuf.at[rows, :], ksem.at[index]),
                    pltpu.make_async_copy(v_hbm.at[rows, :], vbuf.at[rows, :], vsem.at[index]))

        def start_cache(quarter):
            for index in range(quarter * loads // 4, (quarter + 1) * loads // 4):
                for copy in cache_copies(index):
                    copy.start()

        c_o = load_projection(wo_hbm, wo_ref, osem, group, head_dim)
        c_g, c_u, c_d, c_qc = (pltpu.make_async_copy(src, dst, wsem.at[3 + i]) for i, (src, dst) in enumerate(
            ((wg_hbm, wg_ref), (wu_hbm, wu_ref), (wd_hbm, wd_ref), (wqc_hbm, wqc_ref))))
        start_cache(0)
        for copy in small:
            copy.wait()
        for b in range(batch):
            seqf[b:b + 1, :] = jnp.full((1, feat), seq_ref[b].astype(jnp.float32))
        gm_row[...] = lane_row(gm_ref)
        gx_row[...] = lane_row(gx_ref)
        angles = seqf[...] * f_ref[...]
        lane = lax.rem(lax.broadcasted_iota(jnp.int32, (batch, feat), 1), head_dim)
        first = lane < head_dim // 2
        cos_t = jnp.cos(angles)
        sin_t = jnp.where(first, -jnp.sin(angles), jnp.sin(angles))

        def rope(value):
            partner = jnp.where(first, pltpu.roll(value, feat - head_dim // 2, 1), pltpu.roll(value, head_dim // 2, 1))
            return (value * cos_t + partner * sin_t).astype(jnp.bfloat16).astype(jnp.float32)

        x_float = x_ref[...].astype(jnp.float32)
        inv = lax.rsqrt(jnp.mean(x_float * x_float, axis=1, keepdims=True) + NORM_EPS)
        x_norm = (x_float * inv * lane_row(ga_ref)).astype(jnp.bfloat16)
        c_q.wait()
        start_cache(1)
        query = jnp.dot(x_norm, wq_ref[...], preferred_element_type=jnp.float32)
        groups = by_group([rope(query[:, n * feat:(n + 1) * feat]) for n in range(qcols // feat)], group)
        for g in range(group):
            qg_ref[g] = groups[g]
        store_block_diagonal(q3_ref, groups)
        c_k.wait()
        key_new = rope(jnp.dot(x_norm, wk_ref[...], preferred_element_type=jnp.float32))
        c_v.wait()
        val_new = jnp.dot(x_norm, wv_ref[...], preferred_element_type=jnp.float32).astype(jnp.bfloat16)
        kn_ref[...] = key_new
        vn_ref[...] = val_new.astype(jnp.float32)

        def scores_of(start):
            q_a = q3_ref[pl.ds(pl.multiple_of(start * 8, 16), 8), :]
            q_b = q3_ref[pl.ds(pl.multiple_of(start * 8, 16) + 8, 8), :]
            zero = jnp.zeros_like(q_a)
            q_pair = jnp.concatenate([jnp.concatenate([q_a, zero], axis=1), jnp.concatenate([zero, q_b], axis=1)], axis=0).astype(jnp.bfloat16)
            rows = pl.ds(pl.multiple_of(start * feat, 2 * feat), 2 * feat)
            return jnp.dot(q_pair, kbuf[rows, :], preferred_element_type=jnp.float32)

        def probs_of(scores, start):
            slot = lax.broadcasted_iota(jnp.int32, scores.shape, 1)
            sub = lax.broadcasted_iota(jnp.int32, scores.shape, 0)
            visible = slot < jnp.where(sub < 8, seq_ref[start], seq_ref[start + 1]) - row * slots
            scores = jnp.where(visible, scores, MASK_VALUE)
            top = jnp.max(scores, axis=1, keepdims=True)
            probs = jnp.where(visible, jnp.exp((scores - top) * SCALE), 0.0)
            return probs.astype(jnp.bfloat16), top, jnp.sum(probs, axis=1, keepdims=True)

        def weigh(probs, top, count, phase, start, local):
            rows = pl.ds(pl.multiple_of(start * feat, 2 * feat), 2 * feat)
            out = lax.dot_general(probs, vbuf[rows, :], (((1,), (1,)), ((), ())), preferred_element_type=jnp.float32)
            for half in range(2):
                where = pl.ds(local * 8 + 8 * half, 8)
                o_ref[phase, where, :] = out[8 * half:8 * half + 8, feat * half:feat * half + feat]
                m_ref[phase, where, :] = jnp.broadcast_to(top[8 * half:8 * half + 8] * SCALE, (8, feat))
                l_ref[phase, where, :] = jnp.broadcast_to(count[8 * half:8 * half + 8], (8, feat))

        def attend_quarter(quarter, following):
            for index in range(quarter * loads // 4, (quarter + 1) * loads // 4):
                for copy in cache_copies(index):
                    copy.wait()
            following()
            phase, part_rows = quarter // 2, mine // 2
            start = lax.rem((1 + phase - row) * mine, batch)
            places = [(quarter % 2) * part_rows + 2 * p for p in range(part_rows // 2)]
            scores = [scores_of(start + local) for local in places[:AHEAD]]
            for p, local in enumerate(places):
                soft = probs_of(scores[p], start + local)
                if p + AHEAD < len(places):
                    scores.append(scores_of(start + places[p + AHEAD]))
                weigh(*soft, phase, start + local, local)

        def start_all(*copies):
            for copy in copies:
                copy.start()

        part_rows = mine // 2
        shared = []

        def share(part):
            pack_partial(tx.at[part], *(load_groups(ref, 0, part * part_rows * 8, part_rows, feat, group) for ref in (o_ref, m_ref, l_ref)))
            if part == 0:
                pl.semaphore_wait(barrier, 3)
            shared.append(remote(tx.at[part], rx.at[part], pair_sems, (part,), other_row))
            shared[part].start()

        attend_quarter(0, lambda: start_cache(2))
        share(0)
        attend_quarter(1, lambda: start_cache(3))
        share(1)
        attend_quarter(2, lambda: start_all(*c_o, c_g))
        attend_quarter(3, lambda: start_all(c_u))
        own = pl.ds(pl.multiple_of(row * mine, mine), mine)
        for piece in range(2):
            here = pl.ds(pl.multiple_of(row * mine + piece * part_rows, part_rows), part_rows)
            key_own, val_own = kn_ref[here, :], vn_ref[here, :]
            outs, tops, counts = (load_groups(ref, 1, piece * part_rows * 8, part_rows, feat, group) for ref in (o_ref, m_ref, l_ref))
            new_tops = [half_sums(qg_ref[g, here, :] * key_own) * SCALE for g in range(group)]
            shared[piece].wait_recv()
            outs_p, tops_p, counts_p = unpack_partial(rx.at[piece], group)
            for g in range(group):
                merged = merge(((outs[g], tops[g], counts[g]), (outs_p[g], tops_p[g], counts_p[g]), (val_own, new_tops[g], 1.0)))
                att_ref[piece * part_rows:(piece + 1) * part_rows, g * feat:(g + 1) * feat] = merged.astype(jnp.bfloat16)
        for copy in c_o:
            copy.wait()
        pending = list(shared)
        ends = (core, other_core, other_chip)

        def weights_ready():
            c_g.wait()
            c_u.wait()
            start_all(c_d, c_qc)

        use = norm_products(lambda cols, summed: x_ref[own, cols].astype(jnp.float32) + summed, h_ref, square, gm_row, ((wg_ref, gate_acc), (wu_ref, upper_acc)), weights_ready)
        pending += all_reduce(chunk_dot(att_ref, wo_ref, CHUNKS), use, part.at[0], from_core.at[0], chip.at[0], from_chip.at[0], total.at[0], red_sems.at[0], *ends)
        swiglu_hidden(norm_scale(square, width), gate_acc, upper_acc, act_ref)
        c_d.wait()
        use = norm_products(lambda cols, summed: h_ref[:, cols] + summed, h_ref, square, gx_row, ((wqc_ref, query_acc),), c_qc.wait)
        pending += all_reduce(chunk_dot(act_ref, wd_ref, CHUNKS), use, part.at[1], from_core.at[1], chip.at[1], from_chip.at[1], total.at[1], red_sems.at[1], *ends)
        query = query_acc[...] * norm_scale(square, width)
        groups = by_group([query[:, n * feat:(n + 1) * feat] for n in range(qcols // feat)], group)
        gain = jnp.concatenate([gq_ref[...].astype(jnp.float32)] * 2, axis=1)
        groups = [(v * lax.rsqrt(half_sums(v * v) / head_dim + NORM_EPS) * gain).astype(jnp.bfloat16).astype(jnp.float32) for v in groups]
        for g in range(group):
            qtx[g] = groups[g]
        sent = remote(qtx, qrx, pair_sems, (2,), other_row)
        sent.start()
        pending.append(sent)
        store_block_diagonal(qx_ref, groups, (row,))
        sent.wait_recv()
        store_block_diagonal(qx_ref, [qrx[g] for g in range(group)], (1 - row,))
        for copy in pending:
            copy.wait_send()

    bf16, f32 = jnp.bfloat16, jnp.float32
    chunk_shape = (2, CHUNKS, mine, chunk)
    return pl.pallas_call(
        kernel,
        out_shape=(jax.ShapeDtypeStruct((batch, feat), f32), jax.ShapeDtypeStruct((batch, feat), f32),
                   jax.ShapeDtypeStruct((2, mine * 8, feat), f32), jax.ShapeDtypeStruct((mine, width), f32)),
        in_specs=[ANY] * 17,
        out_specs=(VMEM,) * 4,
        scratch_shapes=[pltpu.SMEM(seq_len.shape, seq_len.dtype)] + [pltpu.VMEM(a.shape, a.dtype) for a in (x, *gains, freqs)]
                       + [pltpu.VMEM(wq.shape, bf16), pltpu.VMEM(wk.shape, bf16), pltpu.VMEM(wv.shape, bf16),
                        pltpu.VMEM(keys.shape, bf16), pltpu.VMEM(values.shape, bf16), pltpu.VMEM(wo.shape, bf16),
                        pltpu.VMEM(wg.shape, bf16), pltpu.VMEM(wu.shape, bf16), pltpu.VMEM(wd.shape, bf16), pltpu.VMEM(wqc.shape, bf16),
                        pltpu.VMEM((batch, feat), f32), pltpu.VMEM((group, batch, feat), f32),
                        pltpu.VMEM((batch * 8, feat), f32)] + [pltpu.VMEM((2, mine * 8, feat), f32)] * 3
                       + [pltpu.VMEM((2, group + 1, mine // 2, feat), f32)] * 2
                       + [pltpu.VMEM((mine, group * feat), bf16), pltpu.VMEM((1, width), f32), pltpu.VMEM((1, width), f32), pltpu.VMEM((mine, LANES), f32),
                          pltpu.VMEM((mine, ff), f32), pltpu.VMEM((mine, ff), f32), pltpu.VMEM((mine, qcols), f32), pltpu.VMEM((mine, ff), bf16)]
                       + [pltpu.VMEM((2, CHUNKS, 2, mine, chunk), f32)] + [pltpu.VMEM(chunk_shape, f32)] * 3 + [pltpu.VMEM((2, CHUNKS, 2, mine, chunk), f32)]
                       + [pltpu.VMEM((group, mine, feat), f32)] * 2
                       + [pltpu.SemaphoreType.DMA((7,)), pltpu.SemaphoreType.DMA((7,)), pltpu.SemaphoreType.DMA((loads,)), pltpu.SemaphoreType.DMA((loads,)), pltpu.SemaphoreType.DMA((2 * group,)),
                          pltpu.SemaphoreType.DMA((2, 2, 3, CHUNKS)), pltpu.SemaphoreType.DMA((2, 3))],
        compiler_params=pltpu.CompilerParams(vmem_limit_bytes=53 * 1024 * 1024, collective_id=1, has_side_effects=True),
        cost_estimate=pl.CostEstimate(flops=2 * batch * width * (3 * ff + 3 * qcols), bytes_accessed=50 * 1024 * 1024, transcendentals=batch * 8 * slots),
        name='self_layer',
    )(*in_hbm(seq_len, x, *gains, freqs, keys, values, wq, wk, wv, wo, wg, wu, wd, wqc))


def cross_tail(packed, hidden_in, tile_rows, gates, gain, wo, wg, wu, wd, group):
    mine = hidden_in.shape[0]
    feat = packed.shape[3]
    head_dim = feat // 2
    width, ff = wg.shape
    tiles = tile_rows.shape[0]
    chunk = width // CHUNKS // 2
    last = width // LAST_CHUNKS // 2

    def kernel(tile_hbm, gate_hbm, p_ref, h_ref, gain_hbm, wo_hbm, wg_hbm, wu_hbm, wd_hbm, final,
               tile_ref, gate_ref, gain_ref, wo_ref, wg_ref, wu_ref, wd_ref, on_ref, h3_ref, rx, att_ref, gain_row, square, gate_acc, upper_acc, act_ref,
               part, from_core, chip, from_chip, total, last_part, last_from_core, last_chip, last_from_chip,
               gsem, wsem, osem, red_sems, last_sems, pair_sems, far_sems):
        row, core, other_core, other_chip, other_row = neighbours()
        barrier = pltpu.get_barrier_semaphore()
        greet(barrier, (other_core, other_chip, other_row))
        c_o = load_projection(wo_hbm, wo_ref, osem, group, head_dim)
        small = [pltpu.make_async_copy(src, dst, gsem.at[i]) for i, (src, dst) in enumerate(((tile_hbm, tile_ref), (gate_hbm, gate_ref), (gain_hbm, gain_ref)))]
        for copy in small + c_o:
            copy.start()
        c_w = [pltpu.make_async_copy(src, dst, wsem.at[i]) for i, (src, dst) in enumerate(((wg_hbm, wg_ref), (wu_hbm, wu_ref), (wd_hbm, wd_ref)))]
        for copy in c_w[:2]:
            copy.start()
        pl.semaphore_wait(barrier, 3)
        sent = remote(p_ref.at[1 - row], rx, pair_sems, (0,), other_row)
        sent.start()
        for copy in small:
            copy.wait()
        gain_row[...] = lane_row(gain_ref)
        for r in range(mine):
            seen = tile_ref[0, row * mine + r]
            for t in range(1, tiles):
                seen = jnp.maximum(seen, tile_ref[t, row * mine + r])
            on_ref[r:r + 1, :] = jnp.full((1, LANES), jnp.where(seen != 0, 1.0, 0.0))
        gate_att = jnp.tanh(jnp.full((1, LANES), gate_ref[0]))[:, :1]
        gate_mlp = jnp.tanh(jnp.full((1, LANES), gate_ref[1]))[:, :1]
        outs, tops, counts = unpack_partial(p_ref.at[row], group)
        sent.wait_recv()
        outs_p, tops_p, counts_p = unpack_partial(rx, group)
        for g in range(group):
            merged = merge(((outs[g], tops[g], counts[g]), (outs_p[g], tops_p[g], counts_p[g])))
            att_ref[:, g * feat:(g + 1) * feat] = merged.astype(jnp.bfloat16)
        for copy in c_o:
            copy.wait()
        pending = [sent]
        ends = (core, other_core, other_chip)
        scale_att, scale_mlp = gate_att * on_ref[:, :1], gate_mlp * on_ref[:, :1]

        def weights_ready():
            c_w[0].wait()
            c_w[1].wait()
            c_w[2].start()

        use = norm_products(lambda cols, summed: h_ref[:, cols] + scale_att * summed, h3_ref, square, gain_row, ((wg_ref, gate_acc), (wu_ref, upper_acc)), weights_ready)
        pending += all_reduce(chunk_dot(att_ref, wo_ref, CHUNKS), use, part, from_core, chip, from_chip, total, red_sems, *ends)
        swiglu_hidden(norm_scale(square, width), gate_acc, upper_acc, act_ref)
        c_w[2].wait()
        first, second = reduce_chips(chunk_dot(act_ref, wd_ref, LAST_CHUNKS), last_part, last_from_core, last_chip, last_from_chip, last_sems, *ends)
        pending += first + second
        near, far, relay = [], [], []
        for j in range(LAST_CHUNKS):
            second[j].wait_recv()
            summed = last_chip[j] + last_from_chip[j]
            cols = pl.ds(pl.multiple_of((2 * j + core) * last, last), last)
            place = (pl.ds(pl.multiple_of(row * mine, mine), mine), cols)
            final[place] = (h3_ref[:, cols] + scale_mlp * summed).astype(jnp.bfloat16).astype(jnp.float32)
            piece = final.at[place]
            far.append(remote(piece, piece, far_sems, (0, j), other_row))
            far[j].start()
            near.append(remote(piece, piece, far_sems, (1, j), other_core))
            near[j].start()
        for j in range(LAST_CHUNKS):
            far[j].wait_recv()
            place = (pl.ds(pl.multiple_of((1 - row) * mine, mine), mine), pl.ds(pl.multiple_of((2 * j + core) * last, last), last))
            piece = final.at[place]
            relay.append(remote(piece, piece, far_sems, (2, j), other_core))
            relay[j].start()
        for j in range(LAST_CHUNKS):
            near[j].wait_recv()
        for j in range(LAST_CHUNKS):
            relay[j].wait_recv()
        for copy in pending + near + far + relay:
            copy.wait_send()

    bf16, f32 = jnp.bfloat16, jnp.float32
    chunk_shape, last_shape = (CHUNKS, mine, chunk), (LAST_CHUNKS, mine, last)
    return pl.pallas_call(
        kernel,
        out_shape=jax.ShapeDtypeStruct((2 * mine, width), f32),
        in_specs=[ANY] * 2 + [VMEM] * 2 + [ANY] * 5,
        out_specs=VMEM,
        scratch_shapes=[pltpu.SMEM(tile_rows.shape, tile_rows.dtype), pltpu.SMEM(gates.shape, gates.dtype), pltpu.VMEM(gain.shape, bf16), pltpu.VMEM(wo.shape, bf16), pltpu.VMEM(wg.shape, bf16), pltpu.VMEM(wu.shape, bf16), pltpu.VMEM(wd.shape, bf16),
                        pltpu.VMEM((mine, LANES), f32), pltpu.VMEM((mine, width), f32)]
                       + [pltpu.VMEM((group + 1, mine, feat), f32)]
                       + [pltpu.VMEM((mine, group * feat), bf16), pltpu.VMEM((1, width), f32), pltpu.VMEM((mine, LANES), f32),
                          pltpu.VMEM((mine, ff), f32), pltpu.VMEM((mine, ff), f32), pltpu.VMEM((mine, ff), bf16)]
                       + [pltpu.VMEM((CHUNKS, 2, mine, chunk), f32)] + [pltpu.VMEM(chunk_shape, f32)] * 3 + [pltpu.VMEM((CHUNKS, 2, mine, chunk), f32)]
                       + [pltpu.VMEM((LAST_CHUNKS, 2, mine, last), f32)] + [pltpu.VMEM(last_shape, f32)] * 3
                       + [pltpu.SemaphoreType.DMA((3,)), pltpu.SemaphoreType.DMA((3,)), pltpu.SemaphoreType.DMA((2 * group,)),
                          pltpu.SemaphoreType.DMA((2, 3, CHUNKS)), pltpu.SemaphoreType.DMA((2, 2, LAST_CHUNKS)), pltpu.SemaphoreType.DMA((2, 1)), pltpu.SemaphoreType.DMA((2, 3, LAST_CHUNKS))],
        compiler_params=pltpu.CompilerParams(vmem_limit_bytes=36 * 1024 * 1024, collective_id=2, has_side_effects=True),
        cost_estimate=pl.CostEstimate(flops=4 * mine * width * 3 * ff, bytes_accessed=30 * 1024 * 1024, transcendentals=mine * ff),
        name='cross_tail',
    )(*in_hbm(tile_rows, gates), packed, hidden_in, *in_hbm(gain, wo, wg, wu, wd))


def cross_attention(query_bd, keys, values, tile_rows, key_new, val_new):
    rows, feat, tokens = keys.shape
    tiles = tile_rows.shape[0]
    half_rows = rows // 2
    head_dim = feat // 2
    tile_tok = tokens // 2
    base_one = tile_tok // LANES * LANES
    width = tokens - base_one
    width_zero = min(width, -(-tile_tok // LANES) * LANES)

    def kernel(tile_hbm, q_ref, kin_ref, vin_ref, k_hbm, v_hbm, p_ref, kn_ref, vn_ref,
               tile_ref, list_ref, o_ref, m_ref, l_ref, s_ref, kbuf, vbuf, knb, vnb, tsem, nsem, ksem, vsem):
        kv_index = lax.axis_index('kv')
        first_tile = kv_index * (tiles // 2)

        def collect(tile, count):
            def add(row, count):
                list_ref[count] = row
                return count + jnp.where(tile_ref[first_tile + tile, row] != 0, 1, 0)

            end = lax.fori_loop(0, rows, add, count, unroll=16)
            list_ref[end] = list_ref[jnp.maximum(end - 1, 0)]
            return end

        def copies(index, is_one, hbm, buf, sem):
            slot = lax.rem(index, SLOTS)
            span = pl.ds(base_one, width) if is_one else pl.ds(0, width_zero)
            dest = pl.ds(0, width) if is_one else pl.ds(0, width_zero)
            return [pltpu.make_async_copy(hbm.at[list_ref[2 * index + half], :, span], buf.at[slot, pl.ds(half * feat, feat), dest], sem.at[slot, half])
                    for half in range(2)]

        key_side, val_side = (k_hbm, kbuf, ksem), (v_hbm, vbuf, vsem)

        def start(index, is_one):
            for copy in copies(index, is_one, *key_side) + copies(index, is_one, *val_side):
                copy.start()

        def wait(index, side):
            @pl.when(index < pairs_zero)
            def _():
                for copy in copies(index, False, *side):
                    copy.wait()

            @pl.when((index >= pairs_zero) & (index < pairs))
            def _():
                for copy in copies(index, True, *side):
                    copy.wait()

        tile_copy = pltpu.make_async_copy(tile_hbm, tile_ref, tsem)
        tile_copy.start()
        tile_copy.wait()
        n_zero = collect(0, jnp.int32(0))
        pairs_zero = (n_zero + 1) // 2
        for index in range(SLOTS - 1):
            pl.when(index < pairs_zero)(functools.partial(start, jnp.int32(index), False))
        end_one = collect(1, 2 * pairs_zero)
        pairs = (end_one + 1) // 2
        for index in range(SLOTS - 1):
            pl.when((index >= pairs_zero) & (index < pairs))(functools.partial(start, jnp.int32(index), True))
        o_ref[...] = jnp.zeros_like(o_ref)
        l_ref[...] = jnp.zeros_like(l_ref)
        m_ref[...] = jnp.full_like(m_ref, MASK_VALUE)
        new_copies = []
        for i, (src, dst, out) in enumerate(((kin_ref, knb, kn_ref), (vin_ref, vnb, vn_ref))):
            dst[...] = jnp.stack([src[:, :head_dim], src[:, head_dim:]], axis=1).astype(jnp.bfloat16)
            new_copies.append(pltpu.make_async_copy(dst, out, nsem.at[i]))
            new_copies[i].start()

        def scores_of(index):
            last = jnp.minimum(index, jnp.maximum(pairs - 1, 0))
            q_a, q_b = (q_ref[pl.ds(pl.multiple_of(list_ref[2 * last + half] * 8, 8), 8), :] for half in range(2))
            zero = jnp.zeros_like(q_a)
            q_pair = jnp.concatenate([jnp.concatenate([q_a, zero], axis=1), jnp.concatenate([zero, q_b], axis=1)], axis=0).astype(jnp.bfloat16)
            return jnp.dot(q_pair, kbuf[lax.rem(index, SLOTS)], preferred_element_type=jnp.float32)

        @pl.when(pairs > 0)
        def _():
            wait(jnp.int32(0), key_side)
            s_ref[0] = scores_of(jnp.int32(0))

        def step(index, carry):
            ahead = index + SLOTS - 1
            pl.when(ahead < pairs_zero)(functools.partial(start, ahead, False))
            pl.when((ahead >= pairs_zero) & (ahead < pairs))(functools.partial(start, ahead, True))
            wait(index + 1, key_side)
            wait(index, val_side)
            slot = lax.rem(index, SLOTS)
            is_one = index >= pairs_zero
            low = jnp.where(is_one, tile_tok - base_one, 0)
            high = jnp.where(is_one, width, tile_tok)
            end = jnp.where(is_one, end_one, n_zero)
            high_b = jnp.where(2 * index + 1 == end, 0, high)
            scores = s_ref[lax.rem(index, 2)]
            lane = lax.broadcasted_iota(jnp.int32, scores.shape, 1)
            sub = lax.broadcasted_iota(jnp.int32, scores.shape, 0)
            visible = (lane >= low) & (lane < jnp.where(sub < 8, high, high_b))
            scores = jnp.where(visible, scores, MASK_VALUE)
            top = jnp.max(scores, axis=1, keepdims=True)
            probs = jnp.where(visible, jnp.exp((scores - top) * SCALE), 0.0)
            total = jnp.sum(probs, axis=1, keepdims=True)
            following = scores_of(index + 1)
            lane_v = lax.broadcasted_iota(jnp.int32, (2 * feat, width - width_zero), 1)
            tail = jnp.where(lane_v < jnp.where(is_one, width, 0), vbuf[slot, :, width_zero:], jnp.zeros((), jnp.bfloat16))
            vals = jnp.concatenate([vbuf[slot, :, :width_zero], tail], axis=1)
            out = lax.dot_general(probs.astype(jnp.bfloat16), vals, (((1,), (1,)), ((), ())), preferred_element_type=jnp.float32)
            for half in range(2):
                where = pl.ds(pl.multiple_of(list_ref[2 * index + half] * 8, 8), 8)
                part = out[8 * half:8 * half + 8, feat * half:feat * half + feat]
                top_new = jnp.broadcast_to(top[8 * half:8 * half + 8] * SCALE, (8, feat))
                total_new = jnp.broadcast_to(total[8 * half:8 * half + 8], (8, feat))
                top_old = m_ref[where, :]
                best = jnp.maximum(top_old, top_new)
                w_old = jnp.exp(top_old - best)
                w_new = jnp.exp(top_new - best)
                m_ref[where, :] = best
                l_ref[where, :] = l_ref[where, :] * w_old + total_new * w_new
                o_ref[where, :] = o_ref[where, :] * w_old + part * w_new
            s_ref[lax.rem(index + 1, 2)] = following
            return carry

        lax.fori_loop(0, pairs, step, 0)
        low_half = half_lane((half_rows, feat))
        for half in range(2):
            def groups(ref):
                at = half * half_rows * 8
                return [jnp.where(low_half, ref[pl.ds(at + g, half_rows, stride=8), :], ref[pl.ds(at + 4 + g, half_rows, stride=8), :]) for g in range(4)]

            pack_partial(p_ref.at[half], groups(o_ref), groups(m_ref), groups(l_ref))
        for copy in new_copies:
            copy.wait()

    state = pltpu.VMEM((rows * 8, feat), jnp.float32)
    heads = jax.ShapeDtypeStruct((rows, 2, head_dim), jnp.bfloat16)
    return pl.pallas_call(
        kernel,
        out_shape=(jax.ShapeDtypeStruct((2, 5, half_rows, feat), jnp.float32), heads, heads),
        in_specs=[ANY, VMEM, VMEM, VMEM, ANY, ANY],
        out_specs=(VMEM, ANY, ANY),
        scratch_shapes=[pltpu.SMEM(tile_rows.shape, jnp.int32), pltpu.SMEM((2 * rows + 8,), jnp.int32), state, state, state,
                        pltpu.VMEM((2, 16, width), jnp.float32),
                        pltpu.VMEM((SLOTS, 2 * feat, width), jnp.bfloat16),
                        pltpu.VMEM((SLOTS, 2 * feat, width), jnp.bfloat16),
                        pltpu.VMEM(heads.shape, heads.dtype), pltpu.VMEM(heads.shape, heads.dtype),
                        pltpu.SemaphoreType.DMA, pltpu.SemaphoreType.DMA((2,)), pltpu.SemaphoreType.DMA((SLOTS, 2)), pltpu.SemaphoreType.DMA((SLOTS, 2))],
        compiler_params=pltpu.CompilerParams(vmem_limit_bytes=30 * 1024 * 1024),
        cost_estimate=pl.CostEstimate(flops=4 * 8 * feat * tokens * rows, bytes_accessed=2 * feat * tokens * rows, transcendentals=8 * tokens * rows),
        name='cross_attention',
    )(*in_hbm(tile_rows), query_bd.reshape(rows * 8, feat), key_new, val_new, *in_hbm(keys, values))


def solution(mesh):
    rows_spec = P('dp', None)
    cache_spec = P('dp', 'tp', 'kv', None)
    new_spec = P('dp', 'tp', None)
    col_spec = P(None, 'tp')
    row_spec = P('tp', None)
    vec_spec = P(None)
    in_specs = (rows_spec, cache_spec, cache_spec, P('dp'), cache_spec, cache_spec, rows_spec,
                vec_spec, col_spec, col_spec, col_spec, row_spec, vec_spec, col_spec, col_spec, row_spec,
                vec_spec, col_spec, vec_spec, row_spec, vec_spec, vec_spec, col_spec, col_spec, row_spec)
    out_specs = (rows_spec, new_spec, new_spec)

    def device_step(x, ks_cache, vs_cache, seq_len, kx_cache, vx_cache, tile_vis, attn_norm, wq_self, wk_self, wv_self, wo_self, mlp_norm, wg_self, wu_self, wd_self, xattn_norm, wq_cross, q_norm, wo_cross, cross_gates, xmlp_norm, wg_cross, wu_cross, wd_cross):
        batch, width = x.shape
        kv_local, slots, head_dim = ks_cache.shape[1:]
        feat = kv_local * head_dim
        group = wq_self.shape[1] // feat
        tokens = kx_cache.shape[2]
        freqs = jnp.asarray(np.tile(rope_freqs(head_dim), 2 * feat // head_dim)[None])

        def lane_rows(gain):
            return gain.reshape(-1, LANES)

        def token_minor(cache):
            return jnp.swapaxes(cache, 2, 3).reshape(batch, feat, cache.shape[2])

        key_new, val_new, query_x, h_two = self_layer(
            x, token_minor(ks_cache).reshape(batch * feat, slots), token_minor(vs_cache).reshape(batch * feat, slots), seq_len,
            [lane_rows(attn_norm), lane_rows(mlp_norm), lane_rows(xattn_norm), q_norm[None]], freqs,
            wq_self, wk_self, wv_self, wo_self, wg_self, wu_self, wd_self, wq_cross, group)
        tile_rows = tile_vis.T
        packed, key_new, val_new = cross_attention(query_x, token_minor(kx_cache), token_minor(vx_cache), tile_rows, key_new, val_new)
        h_four = cross_tail(packed, h_two, tile_rows, cross_gates, lane_rows(xmlp_norm), wo_cross, wg_cross, wu_cross, wd_cross, group)
        return h_four.astype(jnp.bfloat16), key_new, val_new

    return jax.shard_map(device_step, mesh=mesh, in_specs=in_specs, out_specs=out_specs, check_vma=False)
```

```python
import functools
import math
import jax
import jax.numpy as jnp
import numpy as np
from jax import lax
from jax.experimental import pallas as pl
from jax.experimental.pallas import tpu as pltpu
from jax.sharding import PartitionSpec as P

NORM_EPS = 1e-5
ROPE_THETA = 500000.0
MASK_VALUE = -1e30
LANES = 128
SLOTS = 7
AHEAD = 3
SCALE = 0.125


def rope_freqs(head_dim):
    freq_list = []
    for index in range(head_dim // 2):
        base_freq = 1.0 / (ROPE_THETA ** (2.0 * index / head_dim))
        wave_len = 2.0 * math.pi / base_freq
        if wave_len < 2048.0:
            freq_list.append(base_freq)
        elif wave_len > 8192.0:
            freq_list.append(base_freq / 8.0)
        else:
            smooth = (8192.0 / wave_len - 1.0) / 3.0
            freq_list.append((1.0 - smooth) * base_freq / 8.0 + smooth * base_freq)
    return np.array(freq_list, dtype=np.float32)


MESH_ID = pl.DeviceIdType.MESH
CHUNKS = 4
LAST_CHUNKS = 4
ANY = pl.BlockSpec(memory_space=pl.ANY)
VMEM = pl.BlockSpec(memory_space=pltpu.VMEM)
SMEM = pl.BlockSpec(memory_space=pltpu.SMEM)
GROUP_ROWS = 8


def in_hbm(*arrays):
    return [pltpu.with_memory_space_constraint(a, pltpu.HBM) for a in arrays]


def neighbours():
    row = lax.axis_index('kv')
    place = lax.axis_index('tp')
    core = lax.rem(place, 2)
    return row, core, {'tp': place + 1 - 2 * core}, {'tp': lax.rem(place + 2, 4)}, {'kv': 1 - row}


def greet(barrier, peers):
    for peer in peers:
        pl.semaphore_signal(barrier, inc=1, device_id=peer, device_id_type=MESH_ID)


def remote(src, dst, sems, index, peer):
    return pltpu.make_async_remote_copy(src_ref=src, dst_ref=dst, send_sem=sems.at[(0,) + index], recv_sem=sems.at[(1,) + index],
                                        device_id=peer, device_id_type=MESH_ID)


def reduce_chips(produce, part, from_core, chip, from_chip, sems, core, other_core, other_chip):
    first, second = [], []
    chunks = part.shape[0]
    for j in range(chunks):
        block = produce(j)
        width = block.shape[1] // 2
        part[j, 0] = block[:, :width]
        part[j, 1] = block[:, width:]
        copy = remote(part.at[j, 1 - core], from_core.at[j], sems, (0, j), other_core)
        copy.start()
        first.append(copy)
    for j in range(chunks):
        first[j].wait_recv()
        chip[j] = part[j, core] + from_core[j]
        copy = remote(chip.at[j], from_chip.at[j], sems, (1, j), other_chip)
        copy.start()
        second.append(copy)
    return first, second


def all_reduce(produce, use, part, from_core, chip, from_chip, total, sems, core, other_core, other_chip):
    first, second = reduce_chips(produce, part, from_core, chip, from_chip, sems, core, other_core, other_chip)
    chunks, width = part.shape[0], part.shape[3]

    def column(j, half):
        return pl.multiple_of((2 * j + half) * width, width)

    third = []
    for j in range(chunks):
        second[j].wait_recv()
        total[j, core] = chip[j] + from_chip[j]
        third.append(remote(total.at[j, core], total.at[j, core], sems, (2, j), other_core))
        third[j].start()
        if j > 0:
            third[j - 1].wait_recv()
            use(column(j - 1, 1 - core), total[j - 1, 1 - core])
        use(column(j, core), total[j, core])
    third[-1].wait_recv()
    use(column(chunks - 1, 1 - core), total[chunks - 1, 1 - core])
    return first + second + third


def lane_row(gain_ref):
    gain = gain_ref[...].astype(jnp.float32)
    return jnp.concatenate([gain[k:k + 1] for k in range(gain.shape[0])], axis=1)


def norm_products(old_at, h_ref, square_ref, gain_ref, pairs, ready):
    square_ref[...] = jnp.zeros_like(square_ref)
    for _, acc in pairs:
        acc[...] = jnp.zeros_like(acc)
    waits = [ready]

    def use(column, summed):
        width = summed.shape[1]
        cols = pl.ds(column, width)
        hidden = (old_at(cols, summed)).astype(jnp.bfloat16).astype(jnp.float32)
        h_ref[:, cols] = hidden
        square_ref[...] += jnp.sum(hidden * hidden, axis=1, keepdims=True)
        scaled = (hidden * gain_ref[:, cols]).astype(jnp.bfloat16)
        if waits:
            waits.pop()()
        for w_ref, acc in pairs:
            block = min(512, acc.shape[1])
            for n in range(0, acc.shape[1], block):
                acc[:, n:n + block] += jnp.dot(scaled, w_ref[cols, n:n + block], preferred_element_type=jnp.float32)

    return use


def norm_scale(square_ref, width):
    return lax.rsqrt(square_ref[:, :1] / width + NORM_EPS)


def swiglu_hidden(inv, gate_ref, upper_ref, act_ref):
    block = 512
    for n in range(0, act_ref.shape[1], block):
        cols = slice(n, n + block)
        act_ref[:, cols] = (jax.nn.silu(gate_ref[:, cols] * inv) * (upper_ref[:, cols] * inv)).astype(jnp.bfloat16)


def chunk_dot(lhs_ref, w_ref, chunks):
    block = w_ref.shape[1] // chunks
    return lambda j: jnp.dot(lhs_ref[...], w_ref[:, j * block:(j + 1) * block], preferred_element_type=jnp.float32)


def half_lane(shape):
    return lax.broadcasted_iota(jnp.int32, shape, 1) < shape[1] // 2


def half_sums(value):
    low = half_lane(value.shape)
    return jnp.where(low, jnp.sum(jnp.where(low, value, 0.0), axis=1, keepdims=True),
                     jnp.sum(jnp.where(low, 0.0, value), axis=1, keepdims=True))


def by_group(columns, group):
    low = half_lane(columns[0].shape)
    out = []
    for g in range(group):
        a, b = columns[g // 2], columns[group // 2 + g // 2]
        if g % 2 == 0:
            out.append(jnp.where(low, a, pltpu.roll(b, b.shape[1] // 2, 1)))
        else:
            out.append(jnp.where(low, pltpu.roll(a, a.shape[1] // 2, 1), b))
    return out


def store_block_diagonal(ref, groups, lead=()):
    rows, lanes = groups[0].shape
    low = half_lane((rows, lanes))
    for g, value in enumerate(groups):
        ref[lead + (pl.ds(g, rows, stride=8), slice(None))] = jnp.where(low, value, 0.0)
        ref[lead + (pl.ds(4 + g, rows, stride=8), slice(None))] = jnp.where(low, 0.0, value)


def load_groups(ref, lead, start, rows, lanes, group):
    low = half_lane((rows, lanes))
    return [jnp.where(low, ref[lead, pl.ds(start + g, rows, stride=8), :], ref[lead, pl.ds(start + 4 + g, rows, stride=8), :]) for g in range(group)]


def pack_partial(tx, outs, tops, totals):
    group = len(outs)
    lane = lax.rem(lax.broadcasted_iota(jnp.int32, outs[0].shape, 1), outs[0].shape[1] // 2)
    packed = jnp.zeros_like(outs[0])
    for g in range(group):
        tx[g] = outs[g]
        packed = jnp.where(lane == g, tops[g], packed)
        packed = jnp.where(lane == group + g, totals[g], packed)
    tx[group] = packed


def unpack_partial(rx, group):
    packed = rx[group]
    low = half_lane(packed.shape)
    middle = packed.shape[1] // 2

    def spread(k):
        return jnp.where(low, jnp.broadcast_to(packed[:, k:k + 1], packed.shape), jnp.broadcast_to(packed[:, middle + k:middle + k + 1], packed.shape))

    return [rx[g] for g in range(group)], [spread(g) for g in range(group)], [spread(group + g) for g in range(group)]


def merge(parts):
    best = parts[0][1]
    for _, top, _ in parts[1:]:
        best = jnp.maximum(best, top)
    out, total = 0.0, 0.0
    for value, top, count in parts:
        weight = jnp.exp(top - best)
        out = out + value * weight
        total = total + count * weight
    return out / jnp.where(total > 0, total, 1.0)


def load_projection(w_hbm, w_ref, sems, group, head_dim):
    out = []
    for g in range(group):
        for h in range(2):
            out.append(pltpu.make_async_copy(w_hbm.at[pl.ds((h * group + g) * head_dim, head_dim), :],
                                             w_ref.at[pl.ds((g * 2 + h) * head_dim, head_dim), :], sems.at[g * 2 + h]))
    return out


def self_layer(x, keys, values, seq_len, gains, freqs, wq, wk, wv, wo, wg, wu, wd, wqc, group):
    batch, width = x.shape
    feat = wk.shape[1]
    head_dim = feat // 2
    slots = keys.shape[1]
    mine = batch // 2
    ff = wg.shape[1]
    qcols = wq.shape[1]
    loads = batch // GROUP_ROWS
    chunk = width // CHUNKS // 2

    def kernel(seq_hbm, x_hbm, ga_hbm, gm_hbm, gx_hbm, gq_hbm, f_hbm, k_hbm, v_hbm, wq_hbm, wk_hbm, wv_hbm, wo_hbm, wg_hbm, wu_hbm, wd_hbm, wqc_hbm,
               kn_ref, vn_ref, qx_ref, h_ref,
               seq_ref, x_ref, ga_ref, gm_ref, gx_ref, gq_ref, f_ref, wq_ref, wk_ref, wv_ref, kbuf, vbuf, wo_ref, wg_ref, wu_ref, wd_ref, wqc_ref,
               seqf, qg_ref, q3_ref, o_ref, m_ref, l_ref, tx, rx, att_ref, gm_row, gx_row, square, gate_acc, upper_acc, query_acc, act_ref,
               part, from_core, chip, from_chip, total, qtx, qrx,
               xsem, wsem, ksem, vsem, osem, red_sems, pair_sems):
        row, core, other_core, other_chip, other_row = neighbours()
        barrier = pltpu.get_barrier_semaphore()
        greet(barrier, (other_core, other_chip, other_row))

        small = [pltpu.make_async_copy(src, dst, xsem.at[i]) for i, (src, dst) in enumerate(
            ((seq_hbm, seq_ref), (f_hbm, f_ref), (ga_hbm, ga_ref), (x_hbm, x_ref), (gm_hbm, gm_ref), (gx_hbm, gx_ref), (gq_hbm, gq_ref)))]
        for copy in small:
            copy.start()

        def fetch(src, dst, index):
            copy = pltpu.make_async_copy(src, dst, wsem.at[index])
            copy.start()
            return copy

        c_q, c_k, c_v = fetch(wq_hbm, wq_ref, 0), fetch(wk_hbm, wk_ref, 1), fetch(wv_hbm, wv_ref, 2)

        def cache_copies(index):
            start = lax.rem((1 - row) * mine + index * GROUP_ROWS, batch)
            rows = pl.ds(pl.multiple_of(start * feat, GROUP_ROWS * feat), GROUP_ROWS * feat)
            return (pltpu.make_async_copy(k_hbm.at[rows, :], kbuf.at[rows, :], ksem.at[index]),
                    pltpu.make_async_copy(v_hbm.at[rows, :], vbuf.at[rows, :], vsem.at[index]))

        def start_cache(quarter):
            for index in range(quarter * loads // 4, (quarter + 1) * loads // 4):
                for copy in cache_copies(index):
                    copy.start()

        c_o = load_projection(wo_hbm, wo_ref, osem, group, head_dim)
        c_g, c_u, c_d, c_qc = (pltpu.make_async_copy(src, dst, wsem.at[3 + i]) for i, (src, dst) in enumerate(
            ((wg_hbm, wg_ref), (wu_hbm, wu_ref), (wd_hbm, wd_ref), (wqc_hbm, wqc_ref))))
        start_cache(0)
        for copy in small:
            copy.wait()
        for b in range(batch):
            seqf[b:b + 1, :] = jnp.full((1, feat), seq_ref[b].astype(jnp.float32))
        gm_row[...] = lane_row(gm_ref)
        gx_row[...] = lane_row(gx_ref)
        angles = seqf[...] * f_ref[...]
        lane = lax.rem(lax.broadcasted_iota(jnp.int32, (batch, feat), 1), head_dim)
        first = lane < head_dim // 2
        cos_t = jnp.cos(angles)
        sin_t = jnp.where(first, -jnp.sin(angles), jnp.sin(angles))

        def rope(value):
            partner = jnp.where(first, pltpu.roll(value, feat - head_dim // 2, 1), pltpu.roll(value, head_dim // 2, 1))
            return (value * cos_t + partner * sin_t).astype(jnp.bfloat16).astype(jnp.float32)

        x_float = x_ref[...].astype(jnp.float32)
        inv = lax.rsqrt(jnp.mean(x_float * x_float, axis=1, keepdims=True) + NORM_EPS)
        x_norm = (x_float * inv * lane_row(ga_ref)).astype(jnp.bfloat16)
        c_q.wait()
        start_cache(1)
        query = jnp.dot(x_norm, wq_ref[...], preferred_element_type=jnp.float32)
        groups = by_group([rope(query[:, n * feat:(n + 1) * feat]) for n in range(qcols // feat)], group)
        for g in range(group):
            qg_ref[g] = groups[g]
        store_block_diagonal(q3_ref, groups)
        c_k.wait()
        key_new = rope(jnp.dot(x_norm, wk_ref[...], preferred_element_type=jnp.float32))
        c_v.wait()
        val_new = jnp.dot(x_norm, wv_ref[...], preferred_element_type=jnp.float32).astype(jnp.bfloat16)
        kn_ref[...] = key_new
        vn_ref[...] = val_new.astype(jnp.float32)

        def scores_of(start):
            q_a = q3_ref[pl.ds(pl.multiple_of(start * 8, 16), 8), :]
            q_b = q3_ref[pl.ds(pl.multiple_of(start * 8, 16) + 8, 8), :]
            zero = jnp.zeros_like(q_a)
            q_pair = jnp.concatenate([jnp.concatenate([q_a, zero], axis=1), jnp.concatenate([zero, q_b], axis=1)], axis=0).astype(jnp.bfloat16)
            rows = pl.ds(pl.multiple_of(start * feat, 2 * feat), 2 * feat)
            return jnp.dot(q_pair, kbuf[rows, :], preferred_element_type=jnp.float32)

        def probs_of(scores, start):
            slot = lax.broadcasted_iota(jnp.int32, scores.shape, 1)
            sub = lax.broadcasted_iota(jnp.int32, scores.shape, 0)
            visible = slot < jnp.where(sub < 8, seq_ref[start], seq_ref[start + 1]) - row * slots
            scores = jnp.where(visible, scores, MASK_VALUE)
            top = jnp.max(scores, axis=1, keepdims=True)
            probs = jnp.where(visible, jnp.exp((scores - top) * SCALE), 0.0)
            return probs.astype(jnp.bfloat16), top, jnp.sum(probs, axis=1, keepdims=True)

        def weigh(probs, top, count, phase, start, local):
            rows = pl.ds(pl.multiple_of(start * feat, 2 * feat), 2 * feat)
            out = lax.dot_general(probs, vbuf[rows, :], (((1,), (1,)), ((), ())), preferred_element_type=jnp.float32)
            for half in range(2):
                where = pl.ds(local * 8 + 8 * half, 8)
                o_ref[phase, where, :] = out[8 * half:8 * half + 8, feat * half:feat * half + feat]
                m_ref[phase, where, :] = jnp.broadcast_to(top[8 * half:8 * half + 8] * SCALE, (8, feat))
                l_ref[phase, where, :] = jnp.broadcast_to(count[8 * half:8 * half + 8], (8, feat))

        def attend_quarter(quarter, following):
            for index in range(quarter * loads // 4, (quarter + 1) * loads // 4):
                for copy in cache_copies(index):
                    copy.wait()
            following()
            phase, part_rows = quarter // 2, mine // 2
            start = lax.rem((1 + phase - row) * mine, batch)
            places = [(quarter % 2) * part_rows + 2 * p for p in range(part_rows // 2)]
            scores = [scores_of(start + local) for local in places[:AHEAD]]
            for p, local in enumerate(places):
                soft = probs_of(scores[p], start + local)
                if p + AHEAD < len(places):
                    scores.append(scores_of(start + places[p + AHEAD]))
                weigh(*soft, phase, start + local, local)

        def start_all(*copies):
            for copy in copies:
                copy.start()

        part_rows = mine // 2
        shared = []

        def share(part):
            pack_partial(tx.at[part], *(load_groups(ref, 0, part * part_rows * 8, part_rows, feat, group) for ref in (o_ref, m_ref, l_ref)))
            if part == 0:
                pl.semaphore_wait(barrier, 3)
            shared.append(remote(tx.at[part], rx.at[part], pair_sems, (part,), other_row))
            shared[part].start()

        attend_quarter(0, lambda: start_cache(2))
        share(0)
        attend_quarter(1, lambda: start_cache(3))
        share(1)
        attend_quarter(2, lambda: start_all(*c_o, c_g))
        attend_quarter(3, lambda: start_all(c_u))
        own = pl.ds(pl.multiple_of(row * mine, mine), mine)
        for piece in range(2):
            here = pl.ds(pl.multiple_of(row * mine + piece * part_rows, part_rows), part_rows)
            key_own, val_own = kn_ref[here, :], vn_ref[here, :]
            outs, tops, counts = (load_groups(ref, 1, piece * part_rows * 8, part_rows, feat, group) for ref in (o_ref, m_ref, l_ref))
            new_tops = [half_sums(qg_ref[g, here, :] * key_own) * SCALE for g in range(group)]
            shared[piece].wait_recv()
            outs_p, tops_p, counts_p = unpack_partial(rx.at[piece], group)
            for g in range(group):
                merged = merge(((outs[g], tops[g], counts[g]), (outs_p[g], tops_p[g], counts_p[g]), (val_own, new_tops[g], 1.0)))
                att_ref[piece * part_rows:(piece + 1) * part_rows, g * feat:(g + 1) * feat] = merged.astype(jnp.bfloat16)
        for copy in c_o:
            copy.wait()
        pending = list(shared)
        ends = (core, other_core, other_chip)

        def weights_ready():
            c_g.wait()
            c_u.wait()
            start_all(c_d, c_qc)

        use = norm_products(lambda cols, summed: x_ref[own, cols].astype(jnp.float32) + summed, h_ref, square, gm_row, ((wg_ref, gate_acc), (wu_ref, upper_acc)), weights_ready)
        pending += all_reduce(chunk_dot(att_ref, wo_ref, CHUNKS), use, part.at[0], from_core.at[0], chip.at[0], from_chip.at[0], total.at[0], red_sems.at[0], *ends)
        swiglu_hidden(norm_scale(square, width), gate_acc, upper_acc, act_ref)
        c_d.wait()
        use = norm_products(lambda cols, summed: h_ref[:, cols] + summed, h_ref, square, gx_row, ((wqc_ref, query_acc),), c_qc.wait)
        pending += all_reduce(chunk_dot(act_ref, wd_ref, CHUNKS), use, part.at[1], from_core.at[1], chip.at[1], from_chip.at[1], total.at[1], red_sems.at[1], *ends)
        query = query_acc[...] * norm_scale(square, width)
        groups = by_group([query[:, n * feat:(n + 1) * feat] for n in range(qcols // feat)], group)
        gain = jnp.concatenate([gq_ref[...].astype(jnp.float32)] * 2, axis=1)
        groups = [(v * lax.rsqrt(half_sums(v * v) / head_dim + NORM_EPS) * gain).astype(jnp.bfloat16).astype(jnp.float32) for v in groups]
        for g in range(group):
            qtx[g] = groups[g]
        sent = remote(qtx, qrx, pair_sems, (2,), other_row)
        sent.start()
        pending.append(sent)
        store_block_diagonal(qx_ref, groups, (row,))
        sent.wait_recv()
        store_block_diagonal(qx_ref, [qrx[g] for g in range(group)], (1 - row,))
        for copy in pending:
            copy.wait_send()

    bf16, f32 = jnp.bfloat16, jnp.float32
    chunk_shape = (2, CHUNKS, mine, chunk)
    return pl.pallas_call(
        kernel,
        out_shape=(jax.ShapeDtypeStruct((batch, feat), f32), jax.ShapeDtypeStruct((batch, feat), f32),
                   jax.ShapeDtypeStruct((2, mine * 8, feat), f32), jax.ShapeDtypeStruct((mine, width), f32)),
        in_specs=[ANY] * 17,
        out_specs=(VMEM,) * 4,
        scratch_shapes=[pltpu.SMEM(seq_len.shape, seq_len.dtype)] + [pltpu.VMEM(a.shape, a.dtype) for a in (x, *gains, freqs)]
                       + [pltpu.VMEM(wq.shape, bf16), pltpu.VMEM(wk.shape, bf16), pltpu.VMEM(wv.shape, bf16),
                        pltpu.VMEM(keys.shape, bf16), pltpu.VMEM(values.shape, bf16), pltpu.VMEM(wo.shape, bf16),
                        pltpu.VMEM(wg.shape, bf16), pltpu.VMEM(wu.shape, bf16), pltpu.VMEM(wd.shape, bf16), pltpu.VMEM(wqc.shape, bf16),
                        pltpu.VMEM((batch, feat), f32), pltpu.VMEM((group, batch, feat), f32),
                        pltpu.VMEM((batch * 8, feat), f32)] + [pltpu.VMEM((2, mine * 8, feat), f32)] * 3
                       + [pltpu.VMEM((2, group + 1, mine // 2, feat), f32)] * 2
                       + [pltpu.VMEM((mine, group * feat), bf16), pltpu.VMEM((1, width), f32), pltpu.VMEM((1, width), f32), pltpu.VMEM((mine, LANES), f32),
                          pltpu.VMEM((mine, ff), f32), pltpu.VMEM((mine, ff), f32), pltpu.VMEM((mine, qcols), f32), pltpu.VMEM((mine, ff), bf16)]
                       + [pltpu.VMEM((2, CHUNKS, 2, mine, chunk), f32)] + [pltpu.VMEM(chunk_shape, f32)] * 3 + [pltpu.VMEM((2, CHUNKS, 2, mine, chunk), f32)]
                       + [pltpu.VMEM((group, mine, feat), f32)] * 2
                       + [pltpu.SemaphoreType.DMA((7,)), pltpu.SemaphoreType.DMA((7,)), pltpu.SemaphoreType.DMA((loads,)), pltpu.SemaphoreType.DMA((loads,)), pltpu.SemaphoreType.DMA((2 * group,)),
                          pltpu.SemaphoreType.DMA((2, 2, 3, CHUNKS)), pltpu.SemaphoreType.DMA((2, 3))],
        compiler_params=pltpu.CompilerParams(vmem_limit_bytes=53 * 1024 * 1024, collective_id=1, has_side_effects=True),
        cost_estimate=pl.CostEstimate(flops=2 * batch * width * (3 * ff + 3 * qcols), bytes_accessed=50 * 1024 * 1024, transcendentals=batch * 8 * slots),
        name='self_layer',
    )(*in_hbm(seq_len, x, *gains, freqs, keys, values, wq, wk, wv, wo, wg, wu, wd, wqc))


def cross_tail(packed, hidden_in, tile_rows, gates, gain, wo, wg, wu, wd, group):
    mine = hidden_in.shape[0]
    feat = packed.shape[3]
    head_dim = feat // 2
    width, ff = wg.shape
    tiles = tile_rows.shape[0]
    chunk = width // CHUNKS // 2
    last = width // LAST_CHUNKS // 2

    def kernel(tile_hbm, gate_hbm, p_ref, h_ref, gain_hbm, wo_hbm, wg_hbm, wu_hbm, wd_hbm, final,
               tile_ref, gate_ref, gain_ref, wo_ref, wg_ref, wu_ref, wd_ref, on_ref, h3_ref, rx, att_ref, gain_row, square, gate_acc, upper_acc, act_ref,
               part, from_core, chip, from_chip, total, last_part, last_from_core, last_chip, last_from_chip,
               gsem, wsem, osem, red_sems, last_sems, pair_sems, far_sems):
        row, core, other_core, other_chip, other_row = neighbours()
        barrier = pltpu.get_barrier_semaphore()
        greet(barrier, (other_core, other_chip, other_row))
        c_o = load_projection(wo_hbm, wo_ref, osem, group, head_dim)
        small = [pltpu.make_async_copy(src, dst, gsem.at[i]) for i, (src, dst) in enumerate(((tile_hbm, tile_ref), (gate_hbm, gate_ref), (gain_hbm, gain_ref)))]
        for copy in small + c_o:
            copy.start()
        c_w = [pltpu.make_async_copy(src, dst, wsem.at[i]) for i, (src, dst) in enumerate(((wg_hbm, wg_ref), (wu_hbm, wu_ref), (wd_hbm, wd_ref)))]
        for copy in c_w[:2]:
            copy.start()
        pl.semaphore_wait(barrier, 3)
        sent = remote(p_ref.at[1 - row], rx, pair_sems, (0,), other_row)
        sent.start()
        for copy in small:
            copy.wait()
        gain_row[...] = lane_row(gain_ref)
        for r in range(mine):
            seen = tile_ref[0, row * mine + r]
            for t in range(1, tiles):
                seen = jnp.maximum(seen, tile_ref[t, row * mine + r])
            on_ref[r:r + 1, :] = jnp.full((1, LANES), jnp.where(seen != 0, 1.0, 0.0))
        gate_att = jnp.tanh(jnp.full((1, LANES), gate_ref[0]))[:, :1]
        gate_mlp = jnp.tanh(jnp.full((1, LANES), gate_ref[1]))[:, :1]
        outs, tops, counts = unpack_partial(p_ref.at[row], group)
        sent.wait_recv()
        outs_p, tops_p, counts_p = unpack_partial(rx, group)
        for g in range(group):
            merged = merge(((outs[g], tops[g], counts[g]), (outs_p[g], tops_p[g], counts_p[g])))
            att_ref[:, g * feat:(g + 1) * feat] = merged.astype(jnp.bfloat16)
        for copy in c_o:
            copy.wait()
        pending = [sent]
        ends = (core, other_core, other_chip)
        scale_att, scale_mlp = gate_att * on_ref[:, :1], gate_mlp * on_ref[:, :1]

        def weights_ready():
            c_w[0].wait()
            c_w[1].wait()
            c_w[2].start()

        use = norm_products(lambda cols, summed: h_ref[:, cols] + scale_att * summed, h3_ref, square, gain_row, ((wg_ref, gate_acc), (wu_ref, upper_acc)), weights_ready)
        pending += all_reduce(chunk_dot(att_ref, wo_ref, CHUNKS), use, part, from_core, chip, from_chip, total, red_sems, *ends)
        swiglu_hidden(norm_scale(square, width), gate_acc, upper_acc, act_ref)
        c_w[2].wait()
        first, second = reduce_chips(chunk_dot(act_ref, wd_ref, LAST_CHUNKS), last_part, last_from_core, last_chip, last_from_chip, last_sems, *ends)
        pending += first + second
        near, far, relay = [], [], []
        for j in range(LAST_CHUNKS):
            second[j].wait_recv()
            summed = last_chip[j] + last_from_chip[j]
            cols = pl.ds(pl.multiple_of((2 * j + core) * last, last), last)
            place = (pl.ds(pl.multiple_of(row * mine, mine), mine), cols)
            final[place] = (h3_ref[:, cols] + scale_mlp * summed).astype(jnp.bfloat16).astype(jnp.float32)
            piece = final.at[place]
            far.append(remote(piece, piece, far_sems, (0, j), other_row))
            far[j].start()
            near.append(remote(piece, piece, far_sems, (1, j), other_core))
            near[j].start()
        for j in range(LAST_CHUNKS):
            far[j].wait_recv()
            place = (pl.ds(pl.multiple_of((1 - row) * mine, mine), mine), pl.ds(pl.multiple_of((2 * j + core) * last, last), last))
            piece = final.at[place]
            relay.append(remote(piece, piece, far_sems, (2, j), other_core))
            relay[j].start()
        for j in range(LAST_CHUNKS):
            near[j].wait_recv()
        for j in range(LAST_CHUNKS):
            relay[j].wait_recv()
        for copy in pending + near + far + relay:
            copy.wait_send()

    bf16, f32 = jnp.bfloat16, jnp.float32
    chunk_shape, last_shape = (CHUNKS, mine, chunk), (LAST_CHUNKS, mine, last)
    return pl.pallas_call(
        kernel,
        out_shape=jax.ShapeDtypeStruct((2 * mine, width), f32),
        in_specs=[ANY] * 2 + [VMEM] * 2 + [ANY] * 5,
        out_specs=VMEM,
        scratch_shapes=[pltpu.SMEM(tile_rows.shape, tile_rows.dtype), pltpu.SMEM(gates.shape, gates.dtype), pltpu.VMEM(gain.shape, bf16), pltpu.VMEM(wo.shape, bf16), pltpu.VMEM(wg.shape, bf16), pltpu.VMEM(wu.shape, bf16), pltpu.VMEM(wd.shape, bf16),
                        pltpu.VMEM((mine, LANES), f32), pltpu.VMEM((mine, width), f32)]
                       + [pltpu.VMEM((group + 1, mine, feat), f32)]
                       + [pltpu.VMEM((mine, group * feat), bf16), pltpu.VMEM((1, width), f32), pltpu.VMEM((mine, LANES), f32),
                          pltpu.VMEM((mine, ff), f32), pltpu.VMEM((mine, ff), f32), pltpu.VMEM((mine, ff), bf16)]
                       + [pltpu.VMEM((CHUNKS, 2, mine, chunk), f32)] + [pltpu.VMEM(chunk_shape, f32)] * 3 + [pltpu.VMEM((CHUNKS, 2, mine, chunk), f32)]
                       + [pltpu.VMEM((LAST_CHUNKS, 2, mine, last), f32)] + [pltpu.VMEM(last_shape, f32)] * 3
                       + [pltpu.SemaphoreType.DMA((3,)), pltpu.SemaphoreType.DMA((3,)), pltpu.SemaphoreType.DMA((2 * group,)),
                          pltpu.SemaphoreType.DMA((2, 3, CHUNKS)), pltpu.SemaphoreType.DMA((2, 2, LAST_CHUNKS)), pltpu.SemaphoreType.DMA((2, 1)), pltpu.SemaphoreType.DMA((2, 3, LAST_CHUNKS))],
        compiler_params=pltpu.CompilerParams(vmem_limit_bytes=36 * 1024 * 1024, collective_id=2, has_side_effects=True),
        cost_estimate=pl.CostEstimate(flops=4 * mine * width * 3 * ff, bytes_accessed=30 * 1024 * 1024, transcendentals=mine * ff),
        name='cross_tail',
    )(*in_hbm(tile_rows, gates), packed, hidden_in, *in_hbm(gain, wo, wg, wu, wd))


def cross_attention(query_bd, keys, values, tile_rows, key_new, val_new):
    rows, feat, tokens = keys.shape
    tiles = tile_rows.shape[0]
    half_rows = rows // 2
    head_dim = feat // 2
    tile_tok = tokens // 2
    base_one = tile_tok // LANES * LANES
    width = tokens - base_one
    width_zero = min(width, -(-tile_tok // LANES) * LANES)

    def kernel(tile_hbm, q_ref, kin_ref, vin_ref, k_hbm, v_hbm, p_ref, kn_ref, vn_ref,
               tile_ref, list_ref, o_ref, m_ref, l_ref, s_ref, kbuf, vbuf, knb, vnb, tsem, nsem, ksem, vsem):
        kv_index = lax.axis_index('kv')
        first_tile = kv_index * (tiles // 2)

        def collect(tile, count):
            def add(row, count):
                list_ref[count] = row
                return count + jnp.where(tile_ref[first_tile + tile, row] != 0, 1, 0)

            end = lax.fori_loop(0, rows, add, count, unroll=64)
            list_ref[end] = list_ref[jnp.maximum(end - 1, 0)]
            return end

        def copies(index, is_one, hbm, buf, sem):
            slot = lax.rem(index, SLOTS)
            span = pl.ds(base_one, width) if is_one else pl.ds(0, width_zero)
            dest = pl.ds(0, width) if is_one else pl.ds(0, width_zero)
            return [pltpu.make_async_copy(hbm.at[list_ref[2 * index + half], :, span], buf.at[slot, pl.ds(half * feat, feat), dest], sem.at[slot, half])
                    for half in range(2)]

        key_side, val_side = (k_hbm, kbuf, ksem), (v_hbm, vbuf, vsem)

        def start(index, is_one):
            for copy in copies(index, is_one, *key_side) + copies(index, is_one, *val_side):
                copy.start()

        def wait(index, side):
            @pl.when(index < pairs_zero)
            def _():
                for copy in copies(index, False, *side):
                    copy.wait()

            @pl.when((index >= pairs_zero) & (index < pairs))
            def _():
                for copy in copies(index, True, *side):
                    copy.wait()

        tile_copy = pltpu.make_async_copy(tile_hbm, tile_ref, tsem)
        tile_copy.start()
        tile_copy.wait()
        n_zero = collect(0, jnp.int32(0))
        pairs_zero = (n_zero + 1) // 2
        for index in range(SLOTS - 1):
            pl.when(index < pairs_zero)(functools.partial(start, jnp.int32(index), False))
        end_one = collect(1, 2 * pairs_zero)
        pairs = (end_one + 1) // 2
        for index in range(SLOTS - 1):
            pl.when((index >= pairs_zero) & (index < pairs))(functools.partial(start, jnp.int32(index), True))
        o_ref[...] = jnp.zeros_like(o_ref)
        l_ref[...] = jnp.zeros_like(l_ref)
        m_ref[...] = jnp.full_like(m_ref, MASK_VALUE)
        new_copies = []
        for i, (src, dst, out) in enumerate(((kin_ref, knb, kn_ref), (vin_ref, vnb, vn_ref))):
            dst[...] = jnp.stack([src[:, :head_dim], src[:, head_dim:]], axis=1).astype(jnp.bfloat16)
            new_copies.append(pltpu.make_async_copy(dst, out, nsem.at[i]))
            new_copies[i].start()

        def scores_of(index):
            last = jnp.minimum(index, jnp.maximum(pairs - 1, 0))
            q_a, q_b = (q_ref[pl.ds(pl.multiple_of(list_ref[2 * last + half] * 8, 8), 8), :] for half in range(2))
            zero = jnp.zeros_like(q_a)
            q_pair = jnp.concatenate([jnp.concatenate([q_a, zero], axis=1), jnp.concatenate([zero, q_b], axis=1)], axis=0).astype(jnp.bfloat16)
            return jnp.dot(q_pair, kbuf[lax.rem(index, SLOTS)], preferred_element_type=jnp.float32)

        @pl.when(pairs > 0)
        def _():
            wait(jnp.int32(0), key_side)
            s_ref[0] = scores_of(jnp.int32(0))

        def step(index, carry):
            ahead = index + SLOTS - 1
            pl.when(ahead < pairs_zero)(functools.partial(start, ahead, False))
            pl.when((ahead >= pairs_zero) & (ahead < pairs))(functools.partial(start, ahead, True))
            wait(index + 1, key_side)
            wait(index, val_side)
            slot = lax.rem(index, SLOTS)
            is_one = index >= pairs_zero
            low = jnp.where(is_one, tile_tok - base_one, 0)
            high = jnp.where(is_one, width, tile_tok)
            end = jnp.where(is_one, end_one, n_zero)
            high_b = jnp.where(2 * index + 1 == end, 0, high)
            scores = s_ref[lax.rem(index, 2)]
            lane = lax.broadcasted_iota(jnp.int32, scores.shape, 1)
            sub = lax.broadcasted_iota(jnp.int32, scores.shape, 0)
            visible = (lane >= low) & (lane < jnp.where(sub < 8, high, high_b))
            scores = jnp.where(visible, scores, MASK_VALUE)
            top = jnp.max(scores, axis=1, keepdims=True)
            probs = jnp.where(visible, jnp.exp((scores - top) * SCALE), 0.0)
            total = jnp.sum(probs, axis=1, keepdims=True)
            following = scores_of(index + 1)
            lane_v = lax.broadcasted_iota(jnp.int32, (2 * feat, width - width_zero), 1)
            tail = jnp.where(lane_v < jnp.where(is_one, width, 0), vbuf[slot, :, width_zero:], jnp.zeros((), jnp.bfloat16))
            vals = jnp.concatenate([vbuf[slot, :, :width_zero], tail], axis=1)
            out = lax.dot_general(probs.astype(jnp.bfloat16), vals, (((1,), (1,)), ((), ())), preferred_element_type=jnp.float32)
            for half in range(2):
                where = pl.ds(pl.multiple_of(list_ref[2 * index + half] * 8, 8), 8)
                part = out[8 * half:8 * half + 8, feat * half:feat * half + feat]
                top_new = jnp.broadcast_to(top[8 * half:8 * half + 8] * SCALE, (8, feat))
                total_new = jnp.broadcast_to(total[8 * half:8 * half + 8], (8, feat))
                top_old = m_ref[where, :]
                best = jnp.maximum(top_old, top_new)
                w_old = jnp.exp(top_old - best)
                w_new = jnp.exp(top_new - best)
                m_ref[where, :] = best
                l_ref[where, :] = l_ref[where, :] * w_old + total_new * w_new
                o_ref[where, :] = o_ref[where, :] * w_old + part * w_new
            s_ref[lax.rem(index + 1, 2)] = following
            return carry

        lax.fori_loop(0, pairs, step, 0)
        low_half = half_lane((half_rows, feat))
        for half in range(2):
            def groups(ref):
                at = half * half_rows * 8
                return [jnp.where(low_half, ref[pl.ds(at + g, half_rows, stride=8), :], ref[pl.ds(at + 4 + g, half_rows, stride=8), :]) for g in range(4)]

            pack_partial(p_ref.at[half], groups(o_ref), groups(m_ref), groups(l_ref))
        for copy in new_copies:
            copy.wait()

    state = pltpu.VMEM((rows * 8, feat), jnp.float32)
    heads = jax.ShapeDtypeStruct((rows, 2, head_dim), jnp.bfloat16)
    return pl.pallas_call(
        kernel,
        out_shape=(jax.ShapeDtypeStruct((2, 5, half_rows, feat), jnp.float32), heads, heads),
        in_specs=[ANY, VMEM, VMEM, VMEM, ANY, ANY],
        out_specs=(VMEM, ANY, ANY),
        scratch_shapes=[pltpu.SMEM(tile_rows.shape, jnp.int32), pltpu.SMEM((2 * rows + 8,), jnp.int32), state, state, state,
                        pltpu.VMEM((2, 16, width), jnp.float32),
                        pltpu.VMEM((SLOTS, 2 * feat, width), jnp.bfloat16),
                        pltpu.VMEM((SLOTS, 2 * feat, width), jnp.bfloat16),
                        pltpu.VMEM(heads.shape, heads.dtype), pltpu.VMEM(heads.shape, heads.dtype),
                        pltpu.SemaphoreType.DMA, pltpu.SemaphoreType.DMA((2,)), pltpu.SemaphoreType.DMA((SLOTS, 2)), pltpu.SemaphoreType.DMA((SLOTS, 2))],
        compiler_params=pltpu.CompilerParams(vmem_limit_bytes=30 * 1024 * 1024),
        cost_estimate=pl.CostEstimate(flops=4 * 8 * feat * tokens * rows, bytes_accessed=2 * feat * tokens * rows, transcendentals=8 * tokens * rows),
        name='cross_attention',
    )(*in_hbm(tile_rows), query_bd.reshape(rows * 8, feat), key_new, val_new, *in_hbm(keys, values))


def solution(mesh):
    rows_spec = P('dp', None)
    cache_spec = P('dp', 'tp', 'kv', None)
    new_spec = P('dp', 'tp', None)
    col_spec = P(None, 'tp')
    row_spec = P('tp', None)
    vec_spec = P(None)
    in_specs = (rows_spec, cache_spec, cache_spec, P('dp'), cache_spec, cache_spec, rows_spec,
                vec_spec, col_spec, col_spec, col_spec, row_spec, vec_spec, col_spec, col_spec, row_spec,
                vec_spec, col_spec, vec_spec, row_spec, vec_spec, vec_spec, col_spec, col_spec, row_spec)
    out_specs = (rows_spec, new_spec, new_spec)

    def device_step(x, ks_cache, vs_cache, seq_len, kx_cache, vx_cache, tile_vis, attn_norm, wq_self, wk_self, wv_self, wo_self, mlp_norm, wg_self, wu_self, wd_self, xattn_norm, wq_cross, q_norm, wo_cross, cross_gates, xmlp_norm, wg_cross, wu_cross, wd_cross):
        batch, width = x.shape
        kv_local, slots, head_dim = ks_cache.shape[1:]
        feat = kv_local * head_dim
        group = wq_self.shape[1] // feat
        tokens = kx_cache.shape[2]
        freqs = jnp.asarray(np.tile(rope_freqs(head_dim), 2 * feat // head_dim)[None])

        def lane_rows(gain):
            return gain.reshape(-1, LANES)

        def token_minor(cache):
            return jnp.swapaxes(cache, 2, 3).reshape(batch, feat, cache.shape[2])

        key_new, val_new, query_x, h_two = self_layer(
            x, token_minor(ks_cache).reshape(batch * feat, slots), token_minor(vs_cache).reshape(batch * feat, slots), seq_len,
            [lane_rows(attn_norm), lane_rows(mlp_norm), lane_rows(xattn_norm), q_norm[None]], freqs,
            wq_self, wk_self, wv_self, wo_self, wg_self, wu_self, wd_self, wq_cross, group)
        tile_rows = tile_vis.T
        packed, key_new, val_new = cross_attention(query_x, token_minor(kx_cache), token_minor(vx_cache), tile_rows, key_new, val_new)
        h_four = cross_tail(packed, h_two, tile_rows, cross_gates, lane_rows(xmlp_norm), wo_cross, wg_cross, wu_cross, wd_cross, group)
        return h_four.astype(jnp.bfloat16), key_new, val_new

    return jax.shard_map(device_step, mesh=mesh, in_specs=in_specs, out_specs=out_specs, check_vma=False)
```
